8 devices in a mesh: dp: 1 (over z), col: 2 (over y), row: 4 (over x, core).
Axes of the slice: x: 2, y: 2, z: 1, core: 2. Of those that a mesh axis runs over, the one named last changes fastest.
Arguments:
- h_first: bfloat16 [128, 768], P(('dp', 'col', 'row'))
- h_second: bfloat16 [128, 768], P(('dp', 'col', 'row'))
- start_pos: int32 [128], P(('dp', 'col', 'row'))
- enc_lens: int32 [128], P(('dp', 'col', 'row'))
- dec_bias: float32 [32, 12], replicated
- norm_self: bfloat16 [2, 768], replicated
- norm_cross: bfloat16 [2, 768], replicated
- norm_mlp: bfloat16 [2, 768], replicated
- w_query: bfloat16 [2, 768, 768], P(None, 'row', 'col')
- w_key: bfloat16 [2, 768, 768], P(None, 'row', 'col')
- w_value: bfloat16 [2, 768, 768], P(None, 'row', 'col')
- w_out: bfloat16 [2, 768, 768], P(None, 'row', 'col')
- w_cquery: bfloat16 [2, 768, 768], P(None, 'row', 'col')
- w_cout: bfloat16 [2, 768, 768], P(None, 'row', 'col')
- w_gate: bfloat16 [2, 768, 2048], P(None, 'row', 'col')
- w_up: bfloat16 [2, 768, 2048], P(None, 'row', 'col')
- w_down: bfloat16 [2, 2048, 768], P(None, 'row', 'col')
- self_k: bfloat16 [2, 128, 512, 12, 64], P(None, ('dp', 'col', 'row'))
- self_v: bfloat16 [2, 128, 512, 12, 64], P(None, ('dp', 'col', 'row'))
- cross_k: bfloat16 [2, 128, 512, 12, 64], P(None, ('dp', 'col', 'row'))
- cross_v: bfloat16 [2, 128, 512, 12, 64], P(None, ('dp', 'col', 'row'))
Outputs:
- output 1: bfloat16 [2, 128, 768], P(None, ('dp', 'col', 'row'))
- output 2: bfloat16 [2, 128, 512, 12, 64], P(None, ('dp', 'col', 'row'))
- output 3: bfloat16 [2, 128, 512, 12, 64], P(None, ('dp', 'col', 'row'))
All inputs are finite; a program needn't handle non-finite values.
Results may differ from the reference program's by a relative error of at most 0.0181874.
Values are sent between devices in bfloat16 or wider.
A program may use at most 1 GiB of HBM per device.

```python
import jax
import jax.numpy as jnp
from jax import lax

D_MODEL = 768
HEADS = 12
HEAD_DIM = 64
D_FF = 2048
BATCH_SIZE = 128
CACHE_LEN = 512
ENC_LEN = 512
NUM_LAYERS = 2
NUM_BUCKETS = 32

INNER_DIM = HEADS * HEAD_DIM
NORM_EPS = 1e-6
BUCKET_EDGES = (16, 19, 21, 24, 27, 31, 35, 40, 46, 52, 59, 67, 77, 87, 99, 113)


def setup_inputs(seed: int = 0, part: int = 0) -> dict:
    part_keys = jax.random.split(jax.random.fold_in(jax.random.key(seed), part), 8)
    shared_keys = jax.random.split(jax.random.key(seed + 1), 13)

    def normal_bf16(key, shape, scale):
        return (jax.random.normal(key, shape, jnp.float32) * scale).astype(jnp.bfloat16)

    def gain_draw(key):
        return jax.random.uniform(key, (NUM_LAYERS, D_MODEL), jnp.float32, 0.5, 1.5).astype(jnp.bfloat16)

    start_pos = jax.random.randint(part_keys[2], (BATCH_SIZE,), 0, CACHE_LEN - 1, jnp.int32)
    start_pos = start_pos.at[0].set(CACHE_LEN - 2).at[1].set(0)
    enc_lens = jax.random.randint(part_keys[3], (BATCH_SIZE,), 1, ENC_LEN + 1, jnp.int32)
    enc_lens = enc_lens.at[0].set(ENC_LEN).at[1].set(1)
    self_shape = (NUM_LAYERS, BATCH_SIZE, CACHE_LEN, HEADS, HEAD_DIM)
    cross_shape = (NUM_LAYERS, BATCH_SIZE, ENC_LEN, HEADS, HEAD_DIM)
    in_shape = (NUM_LAYERS, D_MODEL, INNER_DIM)
    out_shape = (NUM_LAYERS, INNER_DIM, D_MODEL)
    ff_shape = (NUM_LAYERS, D_MODEL, D_FF)
    down_shape = (NUM_LAYERS, D_FF, D_MODEL)
    query_scale = 1.5 * (D_MODEL * HEAD_DIM) ** -0.5
    model_scale = D_MODEL ** -0.5
    inner_scale = 2.0 * INNER_DIM ** -0.5
    return dict(
        h_first=normal_bf16(part_keys[0], (BATCH_SIZE, D_MODEL), 1.0),
        h_second=normal_bf16(part_keys[1], (BATCH_SIZE, D_MODEL), 1.0),
        start_pos=start_pos,
        enc_lens=enc_lens,
        dec_bias=jax.random.normal(shared_keys[0], (NUM_BUCKETS, HEADS), jnp.float32),
        norm_self=gain_draw(shared_keys[1]),
        norm_cross=gain_draw(shared_keys[2]),
        norm_mlp=gain_draw(shared_keys[3]),
        w_query=normal_bf16(shared_keys[4], in_shape, query_scale),
        w_key=normal_bf16(shared_keys[5], in_shape, model_scale),
        w_value=normal_bf16(shared_keys[6], in_shape, model_scale),
        w_out=normal_bf16(shared_keys[7], out_shape, inner_scale),
        w_cquery=normal_bf16(shared_keys[8], in_shape, query_scale),
        w_cout=normal_bf16(shared_keys[9], out_shape, inner_scale),
        w_gate=normal_bf16(shared_keys[10], ff_shape, model_scale),
        w_up=normal_bf16(shared_keys[11], ff_shape, model_scale),
        w_down=normal_bf16(shared_keys[12], down_shape, 1.5 * D_FF ** -0.5),
        self_k=normal_bf16(part_keys[4], self_shape, 1.0),
        self_v=normal_bf16(part_keys[5], self_shape, 1.0),
        cross_k=normal_bf16(part_keys[6], cross_shape, 1.0),
        cross_v=normal_bf16(part_keys[7], cross_shape, 1.0),
    )


def rms_norm(hidden, gain):
    mean_sq = jnp.mean(hidden * hidden, axis=-1, keepdims=True)
    return (hidden * lax.rsqrt(mean_sq + NORM_EPS) * gain.astype(jnp.float32)).astype(jnp.bfloat16)


def project(act, weight):
    return jnp.dot(act, weight, preferred_element_type=jnp.float32).astype(jnp.bfloat16)


def attend(query_vec, keys, values, bias):
    scores = jnp.einsum('bhd,bthd->bth', query_vec.astype(jnp.float32), keys.astype(jnp.float32)) + bias
    attn_probs = jax.nn.softmax(scores, axis=1).astype(jnp.bfloat16)
    mixed = jnp.einsum('bth,bthd->bhd', attn_probs.astype(jnp.float32), values.astype(jnp.float32))
    return mixed.astype(jnp.bfloat16).reshape(query_vec.shape[0], -1)


def position_bias(dec_bias, pos):
    offset = pos[:, None] - jnp.arange(CACHE_LEN, dtype=jnp.int32)[None, :]
    distance = jnp.maximum(offset, 0)
    bucket_edges = jnp.array(BUCKET_EDGES, dtype=jnp.int32)
    far_bucket = BUCKET_EDGES[0] - 1 + jnp.sum((distance[:, :, None] >= bucket_edges).astype(jnp.int32), axis=-1)
    bucket = jnp.where(distance < BUCKET_EDGES[0], distance, far_bucket)
    return jnp.where((offset >= 0)[:, :, None], dec_bias[bucket], -jnp.inf)


def cross_bias(enc_lens):
    in_range = jnp.arange(ENC_LEN, dtype=jnp.int32)[None, :, None] < enc_lens[:, None, None]
    return jnp.where(in_range, 0.0, -jnp.inf)


def decode_step(hidden, pos, enc_lens, dec_bias, layer_params):
    self_mask = position_bias(dec_bias, pos)
    cross_mask = cross_bias(enc_lens)
    write_mask = (jnp.arange(CACHE_LEN, dtype=jnp.int32)[None, :] == pos[:, None])[:, :, None, None]

    def layer_body(residual, params):
        (g_self, g_cross, g_mlp, w_query, w_key, w_value, w_out, w_cquery, w_cout,
         w_gate, w_up, w_down, keys_self, vals_self, keys_cross, vals_cross) = params
        normed = rms_norm(residual, g_self)
        query_vec = project(normed, w_query).reshape(-1, HEADS, HEAD_DIM)
        key_row = project(normed, w_key).reshape(-1, 1, HEADS, HEAD_DIM)
        val_row = project(normed, w_value).reshape(-1, 1, HEADS, HEAD_DIM)
        keys_self = jnp.where(write_mask, key_row, keys_self)
        vals_self = jnp.where(write_mask, val_row, vals_self)
        attn_out = attend(query_vec, keys_self, vals_self, self_mask)
        residual = residual + project(attn_out, w_out).astype(jnp.float32)
        normed = rms_norm(residual, g_cross)
        query_vec = project(normed, w_cquery).reshape(-1, HEADS, HEAD_DIM)
        attn_out = attend(query_vec, keys_cross, vals_cross, cross_mask)
        residual = residual + project(attn_out, w_cout).astype(jnp.float32)
        normed = rms_norm(residual, g_mlp)
        gate_val = project(normed, w_gate)
        up_val = project(normed, w_up)
        mlp_act = (jax.nn.silu(gate_val.astype(jnp.float32)) * up_val.astype(jnp.float32)).astype(jnp.bfloat16)
        residual = residual + project(mlp_act, w_down).astype(jnp.float32)
        return residual, (keys_self, vals_self)

    residual, (keys_all, vals_all) = lax.scan(layer_body, hidden.astype(jnp.float32), layer_params)
    return residual.astype(jnp.bfloat16), keys_all, vals_all


def reference(h_first, h_second, start_pos, enc_lens, dec_bias, norm_self, norm_cross, norm_mlp,
              w_query, w_key, w_value, w_out, w_cquery, w_cout, w_gate, w_up, w_down,
              self_k, self_v, cross_k, cross_v):
    shared = (norm_self, norm_cross, norm_mlp, w_query, w_key, w_value, w_out, w_cquery, w_cout,
              w_gate, w_up, w_down)
    first_out, keys_one, vals_one = decode_step(h_first, start_pos, enc_lens, dec_bias,
                                                shared + (self_k, self_v, cross_k, cross_v))
    second_out, keys_two, vals_two = decode_step(h_second, start_pos + 1, enc_lens, dec_bias,
                                                 shared + (keys_one, vals_one, cross_k, cross_v))
    return (jnp.stack([first_out, second_out]), keys_two, vals_two)
```

```python
import functools

import jax
import jax.numpy as jnp
import numpy as np
from jax import lax
from jax.experimental import pallas as pl
from jax.experimental.pallas import tpu as pltpu
from jax.sharding import PartitionSpec as P

NORM_EPS = 1e-6
BUCKET_EDGES = (16, 19, 21, 24, 27, 31, 35, 40, 46, 52, 59, 67, 77, 87, 99, 113)
HEADS = 12
HEAD_DIM = 64
D = HEADS * HEAD_DIM
TOKENS = 2
LANES = 128
HROWS = 16
NEG = -1e30
SEQ_BLOCK = 2
MESH = pl.DeviceIdType.MESH
F32 = jnp.float32
BF16 = jnp.bfloat16
VMEM_LIMIT = 56 << 20


def dot32(a, b):
    return jnp.dot(a, b, preferred_element_type=F32)


def head_mask():
    row = lax.broadcasted_iota(jnp.int32, (HROWS, D), 0)
    col = lax.broadcasted_iota(jnp.int32, (HROWS, D), 1)
    return (col >= row * HEAD_DIM) & (col < (row + 1) * HEAD_DIM)


def spread_query(q_ref, b, seqs, hmask):
    rows = []
    for s in range(TOKENS):
        at = pl.ds(s * seqs + b, 1)
        row = jnp.concatenate([q_ref[0, at, 0:D // 2], q_ref[1, at, 0:D // 2]], axis=1)
        rows.append(jnp.where(hmask, jnp.broadcast_to(row, (HROWS, D)), 0.0))
    return jnp.concatenate(rows, axis=0).astype(BF16)


def softmax_rows(sc):
    top = jnp.max(sc, axis=1, keepdims=True)
    e = jnp.exp(sc - top)
    return (e / jnp.sum(e, axis=1, keepdims=True)).astype(BF16)


def mix_values(probs, vals, hmask, o_ref, b):
    mixed = lax.dot_general(probs, vals, (((1,), (1,)), ((), ())), preferred_element_type=F32)
    for s in range(TOKENS):
        part = jnp.where(hmask, mixed[s * HROWS:(s + 1) * HROWS], 0.0)
        row = jnp.sum(part, axis=0, keepdims=True)
        o_ref[s, pl.ds(b, 1), :] = row.astype(BF16).astype(F32)


def self_kernel(seqs, pos_ref, qkv_ref, tab_ref, k_ref, v_ref, *rest):
    ko_ref, vo_ref, o_ref, kvt = rest[-4:]
    i = pl.program_id(0)
    half = D // 2

    @pl.when(i == 0)
    def _():
        for which in range(2):
            for cb in range(2):
                lo = (which + 1) * half
                kvt[which, pl.ds(cb * half, half), :] = qkv_ref[cb, :, lo:lo + half].T.astype(BF16)

    hmask = head_mask()
    row_id = lax.broadcasted_iota(jnp.int32, (TOKENS * seqs, LANES), 0)
    lane_id = lax.broadcasted_iota(jnp.int32, (TOKENS * seqs, LANES), 1)
    lane_row = lax.broadcasted_iota(jnp.int32, (D, LANES), 1)
    cache_len = k_ref.shape[-1]
    t_id = lax.broadcasted_iota(jnp.int32, (HROWS, cache_len), 1)
    for j in range(SEQ_BLOCK):
        b = i * SEQ_BLOCK + j
        p = pos_ref[b]
        ko_ref[0, j] = k_ref[0, j]
        vo_ref[0, j] = v_ref[0, j]
        for s in range(TOKENS):
            t = p + s
            off = pl.multiple_of((t // LANES) * LANES, LANES)
            lane = t - off
            sel = jnp.where((row_id == s * seqs + b) & (lane_id == lane), 1.0, 0.0).astype(BF16)
            here = lane_row == lane
            for which, ref in ((0, ko_ref), (1, vo_ref)):
                ins = dot32(kvt[which], sel)
                old = ref[0, j, :, pl.ds(off, LANES)].astype(F32)
                ref[0, j, :, pl.ds(off, LANES)] = jnp.where(here, ins, old).astype(BF16)
        qbd = spread_query(qkv_ref, b, seqs, hmask)
        sc = dot32(qbd, ko_ref[0, j])
        parts = []
        for s in range(TOKENS):
            t = p + s
            bias = pltpu.roll(tab_ref[...], lax.rem(t + 1, cache_len), 1)
            parts.append(jnp.where(t_id <= t, sc[s * HROWS:(s + 1) * HROWS] + bias, NEG))
        probs = softmax_rows(jnp.concatenate(parts, axis=0))
        mix_values(probs, vo_ref[0, j], hmask, o_ref, b)


def self_attention(layer, pos, qkv, table, cache_k, cache_v, outs):
    layers, seqs, _, cache_len = cache_k.shape
    cache_spec = pl.BlockSpec((1, SEQ_BLOCK, D, cache_len), lambda i, pos: (layer, i, 0, 0))
    whole3 = pl.BlockSpec(qkv.shape, lambda i, pos: (0, 0, 0))
    in_specs = [whole3, pl.BlockSpec(table.shape, lambda i, pos: (0, 0)), cache_spec, cache_spec]
    args = [pos, qkv, table, cache_k, cache_v]
    aliases = {}
    if outs is not None:
        in_specs += [pl.BlockSpec(memory_space=pl.ANY)] * 2
        args += list(outs)
        aliases = {5: 0, 6: 1}
    nbytes = 4 * seqs * D * cache_len * 2
    return pl.pallas_call(
        functools.partial(self_kernel, seqs),
        out_shape=(jax.ShapeDtypeStruct(cache_k.shape, BF16), jax.ShapeDtypeStruct(cache_v.shape, BF16),
                   jax.ShapeDtypeStruct((TOKENS, seqs, D), F32)),
        grid_spec=pltpu.PrefetchScalarGridSpec(
            num_scalar_prefetch=1, grid=(seqs // SEQ_BLOCK,), in_specs=in_specs,
            out_specs=[cache_spec, cache_spec, pl.BlockSpec((TOKENS, seqs, D), lambda i, pos: (0, 0, 0))],
            scratch_shapes=[pltpu.VMEM((2, D, TOKENS * seqs), BF16)]),
        input_output_aliases=aliases,
        cost_estimate=pl.CostEstimate(flops=20_000_000_000, bytes_accessed=nbytes, transcendentals=0),
        compiler_params=pltpu.CompilerParams(dimension_semantics=("arbitrary",), vmem_limit_bytes=VMEM_LIMIT),
        name="self_attn",
    )(*args)


def cross_kernel(seqs, len_ref, q_ref, k_ref, v_ref, o_ref):
    i = pl.program_id(0)
    hmask = head_mask()
    t_id = lax.broadcasted_iota(jnp.int32, (TOKENS * HROWS, k_ref.shape[-1]), 1)
    for j in range(SEQ_BLOCK):
        b = i * SEQ_BLOCK + j
        qbd = spread_query(q_ref, b, seqs, hmask)
        sc = jnp.where(t_id < len_ref[b], dot32(qbd, k_ref[0, j]), NEG)
        mix_values(softmax_rows(sc), v_ref[0, j], hmask, o_ref, b)


def cross_attention(layer, lens, q, cache_k, cache_v):
    layers, seqs, _, enc_len = cache_k.shape
    cache_spec = pl.BlockSpec((1, SEQ_BLOCK, D, enc_len), lambda i, n: (layer, i, 0, 0))
    nbytes = 2 * seqs * D * enc_len * 2
    return pl.pallas_call(
        functools.partial(cross_kernel, seqs),
        out_shape=jax.ShapeDtypeStruct((TOKENS, seqs, D), F32),
        grid_spec=pltpu.PrefetchScalarGridSpec(
            num_scalar_prefetch=1, grid=(seqs // SEQ_BLOCK,),
            in_specs=[pl.BlockSpec(q.shape, lambda i, n: (0, 0, 0)), cache_spec, cache_spec],
            out_specs=pl.BlockSpec((TOKENS, seqs, D), lambda i, n: (0, 0, 0))),
        cost_estimate=pl.CostEstimate(flops=10_000_000_000, bytes_accessed=nbytes, transcendentals=0),
        compiler_params=pltpu.CompilerParams(dimension_semantics=("arbitrary",), vmem_limit_bytes=VMEM_LIMIT),
        name="cross_attn",
    )(lens, q, cache_k, cache_v)


def rms(res, gain):
    mean_sq = jnp.mean(res * res, axis=-1, keepdims=True)
    return (res * lax.rsqrt(mean_sq + NORM_EPS) * gain.astype(F32)).astype(BF16)


class Stage:
    def __init__(self):
        self.c = lax.axis_index("col")
        r = lax.axis_index("row")
        partner = r + 1 - 2 * (r % 2)
        self.owners = (r, partner, (r + 2) % 4)
        self.peer = (lax.axis_index("dp"), 1 - self.c, r)
        self.partner = (lax.axis_index("dp"), self.c, partner)

    def fetch(self, pieces, dst, sems):
        depth = pieces[0].shape[0]
        copies = []
        for n, piece in enumerate(pieces):
            copy = pltpu.make_async_copy(piece, dst.at[self.rows_of(n, depth), :], sems.at[n])
            copy.start()
            copies.append(copy)
        return copies

    def rows_of(self, n, depth):
        return pl.ds(pl.multiple_of(self.owners[n] * depth, depth), depth)

    def relay(self, pieces, dst, sems):
        at = self.rows_of(2, pieces[2].shape[0])
        copy = pltpu.make_async_remote_copy(src_ref=pieces[2], dst_ref=dst.at[at, :], send_sem=sems.at[3],
                                            recv_sem=sems.at[4], device_id=self.partner, device_id_type=MESH)
        copy.start()
        return copy

    def greet(self):
        barrier = pltpu.get_barrier_semaphore()
        for other in (self.peer, self.partner):
            pl.semaphore_signal(barrier, inc=1, device_id=other, device_id_type=MESH)
        pl.semaphore_wait(barrier, 2)

    def send(self, src, dst, sems):
        copy = pltpu.make_async_remote_copy(src_ref=src, dst_ref=dst, send_sem=sems.at[0], recv_sem=sems.at[1],
                                            device_id=self.peer, device_id_type=MESH)
        copy.start()
        return copy

    def trade_rows(self, own, buf, sems):
        buf[0] = own
        self.send(buf.at[0], buf.at[1], sems).wait()
        rows, width = own.shape
        return buf[...].reshape(2 * rows, width)

    def trade_columns(self, mine, buf, sems):
        rows, width = mine.shape[0] // 2, mine.shape[1]
        c = self.c
        buf[c] = mine.astype(BF16).reshape(2, rows, width)
        first = self.send(buf.at[c, 0], buf.at[c, 1], sems.at[0])
        second = self.send(buf.at[c, 1], buf.at[c, 0], sems.at[1])
        first.wait()
        second.wait()
        return jnp.concatenate([buf[0].reshape(2 * rows, width), buf[1].reshape(2 * rows, width)], axis=1)

    def give_rows(self, mine, buf, sems, out_ref):
        rows = mine.shape[0] // 2
        c = self.c
        mine = mine.astype(BF16)
        buf[0] = mine[rows:]
        copy = self.send(buf.at[0], buf.at[1], sems)
        out_ref[c] = mine[:rows].astype(F32)
        copy.wait()
        out_ref[1 - c] = buf[1].astype(F32)


def start_kernel(h_ref, gain_ref, w0, w1, w2, x_ref, qkv_ref, hbuf, wq, qbuf, fsem, sem):
    st = Stage()
    fetched = st.fetch((w0, w1, w2), wq, fsem)
    st.greet()
    fetched.append(st.relay((w0, w1, w2), wq, fsem))
    res = st.trade_rows(h_ref[...], hbuf, sem.at[0]).astype(F32)
    x_ref[...] = res
    normed = rms(res, gain_ref[...])
    for copy in fetched:
        copy.wait()
    st.give_rows(dot32(normed, wq[...]), qbuf, sem.at[1], qkv_ref)


def middle_kernel(o_ref, x_ref, gain_ref, w0, w1, w2, xo_ref, q_ref, obuf, w, ybuf, qbuf, fsem, sem, sem2):
    st = Stage()
    fetched = st.fetch((w0, w1, w2), w, fsem)
    st.greet()
    fetched.append(st.relay((w0, w1, w2), w, fsem))
    mixed = st.trade_rows(o_ref[...].astype(BF16), obuf, sem.at[0])
    for copy in fetched:
        copy.wait()
    half = D // 2
    y = st.trade_columns(dot32(mixed, w[:, 0:half]), ybuf, sem2)
    res = x_ref[...] + y.astype(F32)
    xo_ref[...] = res
    normed = rms(res, gain_ref[...])
    st.give_rows(dot32(normed, w[:, half:D]), qbuf, sem.at[1], q_ref)


def tail_kernel(last, o_ref, x_ref, gain_ref, *refs):
    st = Stage()
    half = D // 2
    nw = 6 if last else 9
    weights, refs = refs[:nw], refs[nw:]
    if last:
        (hid_ref, obuf, w, wd, ybuf, ubuf, zbuf, fsem, sem, sem2) = refs
    else:
        gain_next, x_out, qkv_ref, obuf, w, wd, ybuf, ubuf, zbuf, wq, qbuf, fsem, sem, sem2 = refs
    places = (w, wd) if last else (w, wd, wq)
    fetched = [st.fetch(weights[3 * n:3 * n + 3], dst, fsem.at[n]) for n, dst in enumerate(places)]
    st.greet()
    for n, dst in enumerate(places):
        fetched[n].append(st.relay(weights[3 * n:3 * n + 3], dst, fsem.at[n]))
    mixed = st.trade_rows(o_ref[...].astype(BF16), obuf, sem.at[0])
    for copy in fetched[0]:
        copy.wait()
    y = st.trade_columns(dot32(mixed, w[:, 0:half]), ybuf, sem2.at[0])
    res = x_ref[...] + y.astype(F32)
    normed = rms(res, gain_ref[...])
    ff = (w.shape[1] - half) // 2
    gate = dot32(normed, w[:, half:half + ff]).astype(BF16).astype(F32)
    up = dot32(normed, w[:, half + ff:half + 2 * ff]).astype(BF16).astype(F32)
    act = st.trade_columns(gate * jax.nn.sigmoid(gate) * up, ubuf, sem2.at[1])
    for copy in fetched[1]:
        copy.wait()
    z = st.trade_columns(dot32(act, wd[...]), zbuf, sem2.at[2])
    res = res + z.astype(F32)
    rows = o_ref.shape[0]
    if last:
        hid_ref[...] = res[:rows].astype(BF16)
    else:
        x_out[...] = res
        normed = rms(res, gain_next[...])
        for copy in fetched[2]:
            copy.wait()
        st.give_rows(dot32(normed, wq[...]), qbuf, sem.at[1], qkv_ref)


def exchange_call(kernel, cid, name, vmem_args, hbm_args, extra_vmem, out_shape, scratch, flops):
    vm = pl.BlockSpec(memory_space=pltpu.VMEM)
    hb = pl.BlockSpec(memory_space=pl.ANY)
    return pl.pallas_call(
        kernel,
        out_shape=out_shape,
        in_specs=[vm] * len(vmem_args) + [hb] * len(hbm_args) + [vm] * len(extra_vmem),
        out_specs=jax.tree.map(lambda _: vm, out_shape),
        scratch_shapes=scratch,
        cost_estimate=pl.CostEstimate(flops=flops, bytes_accessed=8 << 20, transcendentals=0),
        compiler_params=pltpu.CompilerParams(collective_id=cid, has_side_effects=True, vmem_limit_bytes=VMEM_LIMIT),
        name=name,
    )(*vmem_args, *hbm_args, *extra_vmem)


def spread_weight(shard):
    across = [(r, (r + 2) % 4) for r in range(4)]
    swap = [(r, r + 1 - 2 * (r % 2)) for r in range(4)]
    from_x = lax.ppermute(shard, "row", across)
    from_core = lax.ppermute(shard, "row", swap)
    return (shard, from_core, from_x)


def bias_table(dec_bias, cache_len):
    dist = np.arange(cache_len)[::-1]
    far = BUCKET_EDGES[0] - 1 + np.sum(dist[:, None] >= np.array(BUCKET_EDGES)[None, :], axis=1)
    bucket = np.where(dist < BUCKET_EDGES[0], dist, far)
    onehot = (np.arange(dec_bias.shape[0])[:, None] == bucket[None, :]).astype(np.float32)
    padded = jnp.pad(dec_bias, ((0, 0), (0, HROWS - dec_bias.shape[1])))
    return lax.dot_general(padded, jnp.asarray(onehot), (((0,), (0,)), ((), ())),
                           precision=lax.Precision.HIGHEST, preferred_element_type=F32)


def solution(mesh):
    batch_axes = ('dp', 'col', 'row')

    def local_step(h_first, h_second, start_pos, enc_lens, dec_bias, norm_self, norm_cross, norm_mlp,
                   w_query, w_key, w_value, w_out, w_cquery, w_cout, w_gate, w_up, w_down,
                   self_k, self_v, cross_k, cross_v):
        layers, seqs, cache_len = self_k.shape[:3]
        rows = TOKENS * seqs
        half = D // 2
        ffc = w_gate.shape[2]
        depth = 4 * w_query.shape[1]
        fdepth = 4 * w_down.shape[1]

        def flat(cache):
            return jnp.transpose(cache, (0, 1, 3, 4, 2)).reshape(layers, seqs, D, cache.shape[2])

        caches = [flat(a) for a in (self_k, self_v, cross_k, cross_v)]
        cat = lambda *ws: jnp.concatenate(ws, axis=1)
        wqkv = [spread_weight(cat(w_query[l], w_key[l], w_value[l])) for l in range(layers)]
        wmid = [spread_weight(cat(w_out[l], w_cquery[l])) for l in range(layers)]
        wtail = [spread_weight(cat(w_cout[l], w_gate[l], w_up[l])) for l in range(layers)]
        wdown = [spread_weight(w_down[l]) for l in range(layers)]
        table = bias_table(dec_bias, cache_len)

        vm = lambda shape, dt=BF16: pltpu.VMEM(shape, dt)
        dma = lambda *shape: pltpu.SemaphoreType.DMA(shape)
        rowbuf = lambda width: vm((2, rows, width))
        colbuf = lambda width: vm((2, 2, rows, width))
        res_t = jax.ShapeDtypeStruct((2 * rows, D), F32)
        qkv_t = jax.ShapeDtypeStruct((2, rows, 3 * half), F32)
        q_t = jax.ShapeDtypeStruct((2, rows, half), F32)
        gain = lambda g, l: g[l][None, :]

        hidden = jnp.concatenate([h_first, h_second], axis=0)
        res, qkv = exchange_call(
            start_kernel, 0, "start", [hidden, gain(norm_self, 0)], wqkv[0], [], (res_t, qkv_t),
            [rowbuf(D), vm((depth, 3 * half)), rowbuf(3 * half), dma(5), dma(2, 2)], 3_000_000_000)
        outs = None
        for l in range(layers):
            k_out, v_out, mixed = self_attention(l, start_pos, qkv, table, caches[0], caches[1], outs)
            outs = (k_out, v_out)
            res, q = exchange_call(
                middle_kernel, 1, "middle", [mixed.reshape(rows, D), res, gain(norm_cross, l)], wmid[l], [],
                (res_t, q_t),
                [rowbuf(D), vm((depth, D)), colbuf(half), rowbuf(half), dma(5), dma(2, 2), dma(2, 2)],
                6_000_000_000)
            mixed = cross_attention(l, enc_lens, q, caches[2], caches[3])
            last = l == layers - 1
            scratch = [rowbuf(D), vm((depth, half + 2 * ffc)), vm((fdepth, half)), colbuf(half), colbuf(ffc),
                       colbuf(half)]
            if not last:
                scratch += [vm((depth, 3 * half)), rowbuf(3 * half)]
            scratch += [dma(3, 5), dma(2, 2), dma(3, 2, 2)]
            weights = wtail[l] + wdown[l] + (() if last else wqkv[l + 1])
            out_t = jax.ShapeDtypeStruct((rows, D), BF16) if last else (res_t, qkv_t)
            got = exchange_call(
                functools.partial(tail_kernel, last), 3 if last else 2, "last" if last else "tail",
                [mixed.reshape(rows, D), res, gain(norm_mlp, l)], weights,
                [] if last else [gain(norm_self, l + 1)], out_t, scratch, 10_000_000_000)
            if last:
                hid = got
            else:
                res, qkv = got

        def unflat(cache):
            return jnp.transpose(cache.reshape(layers, seqs, HEADS, HEAD_DIM, cache_len), (0, 1, 4, 2, 3))

        return hid.reshape(TOKENS, seqs, D), unflat(outs[0]), unflat(outs[1])

    row_spec = P(batch_axes, None)
    seq_spec = P(batch_axes)
    weight_spec = P(None, 'row', 'col')
    cache_spec = P(None, batch_axes)
    in_specs = (row_spec, row_spec, seq_spec, seq_spec, P(), P(), P(), P()) + (weight_spec,) * 9 + (cache_spec,) * 4
    out_specs = (P(None, batch_axes), cache_spec, cache_spec)
    return jax.shard_map(local_step, mesh=mesh, in_specs=in_specs, out_specs=out_specs, check_vma=False)
```

```python
import functools

import jax
import jax.numpy as jnp
import numpy as np
from jax import lax
from jax.experimental import pallas as pl
from jax.experimental.pallas import tpu as pltpu
from jax.sharding import PartitionSpec as P

NORM_EPS = 1e-6
BUCKET_EDGES = (16, 19, 21, 24, 27, 31, 35, 40, 46, 52, 59, 67, 77, 87, 99, 113)
HEADS = 12
HEAD_DIM = 64
D = HEADS * HEAD_DIM
TOKENS = 2
LANES = 128
HROWS = 16
NEG = -1e30
SEQ_BLOCK = 2
AHEAD = 6
MESH = pl.DeviceIdType.MESH
F32 = jnp.float32
BF16 = jnp.bfloat16
VMEM_LIMIT = 56 << 20


def dot32(a, b):
    return jnp.dot(a, b, preferred_element_type=F32)


def head_mask():
    row = lax.broadcasted_iota(jnp.int32, (HROWS, D), 0)
    col = lax.broadcasted_iota(jnp.int32, (HROWS, D), 1)
    return (col >= row * HEAD_DIM) & (col < (row + 1) * HEAD_DIM)


def spread_query(q_ref, b, seqs, hmask):
    rows = []
    for s in range(TOKENS):
        at = pl.ds(s * seqs + b, 1)
        row = jnp.concatenate([q_ref[0, at, 0:D // 2], q_ref[1, at, 0:D // 2]], axis=1)
        rows.append(jnp.where(hmask, jnp.broadcast_to(row, (HROWS, D)), 0.0))
    return jnp.concatenate(rows, axis=0).astype(BF16)


def softmax_rows(sc):
    top = jnp.max(sc, axis=1, keepdims=True)
    e = jnp.exp(sc - top)
    return (e / jnp.sum(e, axis=1, keepdims=True)).astype(BF16)


def mix_values(probs, vals, hmask, o_ref, b):
    mixed = lax.dot_general(probs, vals, (((1,), (1,)), ((), ())), preferred_element_type=F32)
    for s in range(TOKENS):
        part = jnp.where(hmask, mixed[s * HROWS:(s + 1) * HROWS], 0.0)
        row = jnp.sum(part, axis=0, keepdims=True)
        o_ref[s, pl.ds(b, 1), :] = row.astype(BF16).astype(F32)


def self_kernel(layer, seqs, aliased, pos_ref, qkv_ref, tab_ref, k_in, v_in, *rest):
    k_out, v_out, o_ref, kbuf, vbuf, kvt, in_sem, out_sem = rest[2 if aliased else 0:]
    half = D // 2
    cache_len = kbuf.shape[-1]
    sides = ((0, k_in, k_out, kbuf), (1, v_in, v_out, vbuf))

    def loads(b):
        return [pltpu.make_async_copy(src.at[layer, b], buf.at[b], in_sem.at[n, b]) for n, src, _, buf in sides]

    def stores(b):
        return [pltpu.make_async_copy(buf.at[b], dst.at[layer, b], out_sem.at[n, b]) for n, _, dst, buf in sides]

    for b in range(AHEAD):
        for copy in loads(b):
            copy.start()
    for which in range(2):
        for cb in range(2):
            lo = (which + 1) * half
            kvt[which, pl.ds(cb * half, half), :] = qkv_ref[cb, :, lo:lo + half].T.astype(BF16)

    def step(i, carry):
        hmask = head_mask()
        row_id = lax.broadcasted_iota(jnp.int32, (TOKENS * seqs, LANES), 0)
        lane_id = lax.broadcasted_iota(jnp.int32, (TOKENS * seqs, LANES), 1)
        lane_row = lax.broadcasted_iota(jnp.int32, (D, LANES), 1)
        t_id = lax.broadcasted_iota(jnp.int32, (HROWS, cache_len), 1)
        for j in range(SEQ_BLOCK):
            ahead = i * SEQ_BLOCK + j + AHEAD

            @pl.when(ahead < seqs)
            def _():
                for copy in loads(ahead):
                    copy.start()
        for j in range(SEQ_BLOCK):
            b = i * SEQ_BLOCK + j
            p = pos_ref[b]
            for copy in loads(b):
                copy.wait()
            for s in range(TOKENS):
                t = p + s
                off = pl.multiple_of((t // LANES) * LANES, LANES)
                lane = t - off
                sel = jnp.where((row_id == s * seqs + b) & (lane_id == lane), 1.0, 0.0).astype(BF16)
                here = lane_row == lane
                for n, _, _, buf in sides:
                    ins = dot32(kvt[n], sel)
                    old = buf[b, :, pl.ds(off, LANES)].astype(F32)
                    buf[b, :, pl.ds(off, LANES)] = jnp.where(here, ins, old).astype(BF16)
            for copy in stores(b):
                copy.start()
            qbd = spread_query(qkv_ref, b, seqs, hmask)
            sc = dot32(qbd, kbuf[b])
            parts = []
            for s in range(TOKENS):
                t = p + s
                bias = pltpu.roll(tab_ref[...], lax.rem(t + 1, cache_len), 1)
                parts.append(jnp.where(t_id <= t, sc[s * HROWS:(s + 1) * HROWS] + bias, NEG))
            probs = softmax_rows(jnp.concatenate(parts, axis=0))
            mix_values(probs, vbuf[b], hmask, o_ref, b)
        return carry

    lax.fori_loop(0, seqs // SEQ_BLOCK, step, 0)
    for b in range(seqs):
        for copy in stores(b):
            copy.wait()


def self_attention(layer, pos, qkv, table, cache_k, cache_v, outs):
    layers, seqs, _, cache_len = cache_k.shape
    vm = pl.BlockSpec(memory_space=pltpu.VMEM)
    hb = pl.BlockSpec(memory_space=pl.ANY)
    in_specs = [pl.BlockSpec(memory_space=pltpu.SMEM), vm, vm, hb, hb]
    args = [pos, qkv, table, cache_k, cache_v]
    aliases = {}
    if outs is not None:
        in_specs += [hb, hb]
        args += list(outs)
        aliases = {5: 0, 6: 1}
    buf = pltpu.VMEM((seqs, D, cache_len), BF16)
    return pl.pallas_call(
        functools.partial(self_kernel, layer, seqs, outs is not None),
        out_shape=(jax.ShapeDtypeStruct(cache_k.shape, BF16), jax.ShapeDtypeStruct(cache_v.shape, BF16),
                   jax.ShapeDtypeStruct((TOKENS, seqs, D), F32)),
        in_specs=in_specs,
        out_specs=[hb, hb, vm],
        scratch_shapes=[buf, buf, pltpu.VMEM((2, D, TOKENS * seqs), BF16),
                        pltpu.SemaphoreType.DMA((2, seqs)), pltpu.SemaphoreType.DMA((2, seqs))],
        input_output_aliases=aliases,
        cost_estimate=pl.CostEstimate(flops=20_000_000_000, bytes_accessed=4 * seqs * D * cache_len * 2,
                                      transcendentals=0),
        compiler_params=pltpu.CompilerParams(vmem_limit_bytes=VMEM_LIMIT),
        name="self_attn",
    )(*args)


def rms(res, gain):
    mean_sq = jnp.mean(res * res, axis=-1, keepdims=True)
    return (res * lax.rsqrt(mean_sq + NORM_EPS) * gain.astype(F32)).astype(BF16)


class Stage:
    def __init__(self):
        dp, self.c, self.r = lax.axis_index("dp"), lax.axis_index("col"), lax.axis_index("row")
        self.across = (self.r + 2) % 4
        core = self.r + 1 - 2 * (self.r % 2)
        self.peer = (dp, 1 - self.c, self.r)
        self.partner = (dp, self.c, core)
        self.xpeer = (dp, self.c, self.across)

    def greet(self):
        barrier = pltpu.get_barrier_semaphore()
        for other in (self.peer, self.partner, self.xpeer):
            pl.semaphore_signal(barrier, inc=1, device_id=other, device_id_type=MESH)
        pl.semaphore_wait(barrier, 3)

    def remote(self, src, dst, send_sem, recv_sem, to):
        return pltpu.make_async_remote_copy(src_ref=src, dst_ref=dst, send_sem=send_sem, recv_sem=recv_sem,
                                            device_id=to, device_id_type=MESH)

    def send(self, src, dst, sems):
        copy = self.remote(src, dst, sems.at[0], sems.at[1], self.peer)
        copy.start()
        return copy

    def trade_rows(self, own, buf, sems):
        buf[0] = own
        self.send(buf.at[0], buf.at[1], sems).wait()
        rows, width = own.shape
        return buf[...].reshape(2 * rows, width)

    def trade_columns(self, mine, buf, sems):
        rows, width = mine.shape[0] // 2, mine.shape[1]
        c = self.c
        buf[c] = mine.astype(BF16).reshape(2, rows, width)
        first = self.send(buf.at[c, 0], buf.at[c, 1], sems.at[0])
        second = self.send(buf.at[c, 1], buf.at[c, 0], sems.at[1])
        first.wait()
        second.wait()
        return jnp.concatenate([buf[0].reshape(2 * rows, width), buf[1].reshape(2 * rows, width)], axis=1)

    def give_rows(self, mine, buf, sems, out_ref):
        rows = mine.shape[0] // 2
        c = self.c
        mine = mine.astype(BF16)
        buf[0] = mine[rows:]
        copy = self.send(buf.at[0], buf.at[1], sems)
        out_ref[c] = mine[:rows].astype(F32)
        copy.wait()
        out_ref[1 - c] = buf[1].astype(F32)


class Weight:
    def __init__(self, st, own, dst, col, sems, crossed=None):
        depth, width = own.shape
        self.st, self.crossed = st, crossed

        def place(owner):
            return dst.at[pl.ds(pl.multiple_of(owner * depth, depth), depth), pl.ds(col, width)]

        mine, theirs = place(st.r), place(st.across)
        self.local = pltpu.make_async_copy(own, mine, sems.at[0])
        self.share = st.remote(own, mine, sems.at[1], sems.at[2], st.partner)
        if crossed is None:
            self.cross = st.remote(own, mine, sems.at[3], sems.at[4], st.xpeer)
            self.pass_on = st.remote(theirs, theirs, sems.at[5], sems.at[6], st.partner)
        else:
            self.cross = pltpu.make_async_copy(crossed, theirs, sems.at[3])
            self.pass_on = st.remote(crossed, theirs, sems.at[5], sems.at[6], st.partner)

    def open_local(self):
        self.local.start()
        if self.crossed is not None:
            self.cross.start()

    def open_cross(self):
        if self.crossed is None:
            self.cross.start()

    def open_share(self):
        self.share.start()
        if self.crossed is not None:
            self.pass_on.start()

    def relay(self):
        if self.crossed is None:
            self.cross.wait_recv()
            self.pass_on.start()

    def finish(self):
        self.local.wait()
        self.share.wait()
        if self.crossed is None:
            self.cross.wait_send()
        else:
            self.cross.wait()
        self.pass_on.wait()


def each(items, name):
    for item in items:
        getattr(item, name)()


def weights_of(st, refs, layer, dst, sems, crossed=None):
    col, found = 0, []
    for n, ref in enumerate(refs):
        width = ref.shape[2]
        given = None if crossed is None else crossed.at[:, pl.ds(col, width)]
        found.append(Weight(st, ref.at[layer], dst, col, sems.at[n], given))
        col += width
    return found


def forward(st, refs, layer, dst, sems):
    col, copies = 0, []
    for n, ref in enumerate(refs):
        width = ref.shape[2]
        copies.append(st.remote(ref.at[layer], dst.at[:, pl.ds(col, width)], sems.at[n, 0], sems.at[n, 1], st.xpeer))
        col += width
    return copies


def collect(refs, layer, dst, sems):
    col, copies = 0, []
    for n, ref in enumerate(refs):
        width = ref.shape[2]
        copies.append(pltpu.make_async_copy(ref.at[layer], dst.at[:, pl.ds(col, width)], sems.at[n]))
        col += width
    return copies


def start_kernel(h_ref, gain_ref, wq_r, wk_r, wv_r, wo_r, wc_r, wco_r, wg_r, wu_r,
                 x_ref, qkv_ref, xmid_ref, tail_ref, hbuf, wqkv, qbuf, tbuf, wsem, xsem, tsem, sem):
    st = Stage()
    weights = weights_of(st, (wq_r, wk_r, wv_r), 0, wqkv, wsem)
    middle = forward(st, (wo_r, wc_r), 0, xmid_ref, xsem)
    tail = collect((wco_r, wg_r, wu_r), 0, tbuf, tsem)
    each(weights, "open_local")
    each(tail, "start")
    st.greet()
    each(weights, "open_cross")
    each(middle, "start")
    each(weights, "open_share")
    res = st.trade_rows(h_ref[...], hbuf, sem.at[0]).astype(F32)
    x_ref[...] = res
    normed = rms(res, gain_ref[...])
    each(tail, "wait")
    tail_out = pltpu.make_async_copy(tbuf, tail_ref, tsem.at[3])
    tail_out.start()
    each(weights, "relay")
    each(weights, "finish")
    st.give_rows(dot32(normed, wqkv[...]), qbuf, sem.at[1], qkv_ref)
    tail_out.wait()
    each(middle, "wait")


def layer_kernel(layer, last, seqs, len_ref, o_ref, x_ref, gcross_ref, gmlp_ref, *refs):
    if last:
        (ck, cv, xmid_in, xtail_in, wo_r, wc_r, wco_r, wg_r, wu_r, wd_r, hid_ref,
         kbuf, vbuf, wmid, wtail, wdown, qs, os, obuf, ybuf, qbuf, obuf2, ybuf2, ubuf, zbuf,
         kvsem, msem, wtsem, dsem, sem, sem2) = refs
    else:
        (gself_ref, ck, cv, xmid_in, xtail_in, wo_r, wc_r, wco_r, wg_r, wu_r, wd_r, wq_r, wk_r, wv_r,
         x_out, qkv_ref, xmid_ref, tail_ref,
         kbuf, vbuf, wmid, wtail, wdown, qs, os, obuf, ybuf, qbuf, obuf2, ybuf2, ubuf, zbuf,
         kvsem, msem, wtsem, dsem, sem, sem2, wqkv, qkvbuf, tbuf, wsem, xsem, tsem) = refs
    st = Stage()
    half = D // 2
    rows = o_ref.shape[0]
    mid = weights_of(st, (wo_r, wc_r), layer, wmid, msem, xmid_in)
    tail = weights_of(st, (wco_r, wg_r, wu_r), layer, wtail, wtsem, xtail_in)
    down = weights_of(st, (wd_r,), layer, wdown, dsem)
    each(mid, "open_local")

    def caches(b):
        return [pltpu.make_async_copy(src.at[layer, b], buf.at[b], kvsem.at[n, b])
                for n, (src, buf) in enumerate(((ck, kbuf), (cv, vbuf)))]

    def fetch_caches(b, carry):
        each(caches(b), "start")
        return carry

    lax.fori_loop(0, seqs, fetch_caches, 0)
    each(tail, "open_local")
    each(down, "open_local")
    if not last:
        ahead = weights_of(st, (wq_r, wk_r, wv_r), layer + 1, wqkv, wsem)
        nextmid = forward(st, (wo_r, wc_r), layer + 1, xmid_ref, xsem)
        nexttail = collect((wco_r, wg_r, wu_r), layer + 1, tbuf, tsem)
        each(ahead, "open_local")
        each(nexttail, "start")
    st.greet()
    each(mid, "open_share")
    each(down, "open_cross")
    if not last:
        each(ahead, "open_cross")
        each(nextmid, "start")
    mixed = st.trade_rows(o_ref[...].astype(BF16), obuf, sem.at[0])
    each(mid, "finish")
    y = st.trade_columns(dot32(mixed, wmid[:, 0:half]), ybuf, sem2.at[0])
    res = x_ref[...] + y.astype(F32)
    normed = rms(res, gcross_ref[...])
    st.give_rows(dot32(normed, wmid[:, half:D]), qbuf, sem.at[1], qs)
    each(tail, "open_share")
    each(down, "open_share")
    if not last:
        each(ahead, "open_share")
        each(nexttail, "wait")
        tail_out = pltpu.make_async_copy(tbuf, tail_ref, tsem.at[3])
        tail_out.start()

    def cross_step(i, carry):
        hmask = head_mask()
        t_id = lax.broadcasted_iota(jnp.int32, (TOKENS * HROWS, kbuf.shape[-1]), 1)
        for j in range(SEQ_BLOCK):
            b = i * SEQ_BLOCK + j
            each(caches(b), "wait")
            qbd = spread_query(qs, b, seqs, hmask)
            sc = jnp.where(t_id < len_ref[b], dot32(qbd, kbuf[b]), NEG)
            mix_values(softmax_rows(sc), vbuf[b], hmask, os, b)
        return carry

    lax.fori_loop(0, seqs // SEQ_BLOCK, cross_step, 0)
    each(down, "relay")
    mixed = st.trade_rows(os[...].reshape(rows, D).astype(BF16), obuf2, sem.at[2])
    each(tail, "finish")
    y = st.trade_columns(dot32(mixed, wtail[:, 0:half]), ybuf2, sem2.at[1])
    res = res + y.astype(F32)
    normed = rms(res, gmlp_ref[...])
    ff = (wtail.shape[1] - half) // 2
    gate = dot32(normed, wtail[:, half:half + ff]).astype(BF16).astype(F32)
    up = dot32(normed, wtail[:, half + ff:half + 2 * ff]).astype(BF16).astype(F32)
    act = st.trade_columns(gate * jax.nn.sigmoid(gate) * up, ubuf, sem2.at[2])
    if not last:
        each(ahead, "relay")
    each(down, "finish")
    z = st.trade_columns(dot32(act, wdown[...]), zbuf, sem2.at[3])
    res = res + z.astype(F32)
    if last:
        hid_ref[...] = res[:rows].astype(BF16)
    else:
        x_out[...] = res
        normed = rms(res, gself_ref[...])
        each(ahead, "finish")
        st.give_rows(dot32(normed, wqkv[...]), qkvbuf, sem.at[3], qkv_ref)
        tail_out.wait()
        each(nextmid, "wait")


def exchange_call(kernel, cid, name, specs, args, outs, scratch, flops):
    spaces = {"s": pltpu.SMEM, "v": pltpu.VMEM, "h": pl.ANY}
    spec = lambda letters: [pl.BlockSpec(memory_space=spaces[x]) for x in letters]
    return pl.pallas_call(
        kernel,
        out_shape=tuple(t for _, t in outs),
        in_specs=spec(specs),
        out_specs=tuple(spec(x for x, _ in outs)),
        scratch_shapes=scratch,
        cost_estimate=pl.CostEstimate(flops=flops, bytes_accessed=8 << 20, transcendentals=0),
        compiler_params=pltpu.CompilerParams(collective_id=cid, has_side_effects=True, vmem_limit_bytes=VMEM_LIMIT),
        name=name,
    )(*args)


def bias_table(dec_bias, cache_len):
    dist = np.arange(cache_len)[::-1]
    far = BUCKET_EDGES[0] - 1 + np.sum(dist[:, None] >= np.array(BUCKET_EDGES)[None, :], axis=1)
    bucket = np.where(dist < BUCKET_EDGES[0], dist, far)
    onehot = (np.arange(dec_bias.shape[0])[:, None] == bucket[None, :]).astype(np.float32)
    padded = jnp.pad(dec_bias, ((0, 0), (0, HROWS - dec_bias.shape[1])))
    return lax.dot_general(padded, jnp.asarray(onehot), (((0,), (0,)), ((), ())),
                           precision=lax.Precision.HIGHEST, preferred_element_type=F32)


def solution(mesh):
    batch_axes = ('dp', 'col', 'row')

    def local_step(h_first, h_second, start_pos, enc_lens, dec_bias, norm_self, norm_cross, norm_mlp,
                   w_query, w_key, w_value, w_out, w_cquery, w_cout, w_gate, w_up, w_down,
                   self_k, self_v, cross_k, cross_v):
        layers, seqs, cache_len = self_k.shape[:3]
        rows = TOKENS * seqs
        half = D // 2
        ffc = w_gate.shape[2]
        depth = 4 * w_query.shape[1]
        fdepth = 4 * w_down.shape[1]

        def flat(cache):
            return jnp.transpose(cache, (0, 1, 3, 4, 2)).reshape(layers, seqs, D, cache.shape[2])

        caches = [flat(a) for a in (self_k, self_v, cross_k, cross_v)]
        table = bias_table(dec_bias, cache_len)
        tail_width = half + 2 * ffc
        block = w_query.shape[1]

        vm = lambda shape, dt=BF16: pltpu.VMEM(shape, dt)
        dma = lambda *shape: pltpu.SemaphoreType.DMA(shape)
        rowbuf = lambda width: vm((2, rows, width))
        colbuf = lambda width: vm((2, 2, rows, width))
        res_t = ("v", jax.ShapeDtypeStruct((2 * rows, D), F32))
        qkv_t = ("v", jax.ShapeDtypeStruct((2, rows, 3 * half), F32))
        mid_t = ("h", jax.ShapeDtypeStruct((block, D), BF16))
        tail_t = ("h", jax.ShapeDtypeStruct((block, tail_width), BF16))
        gain = lambda g, l: g[l][None, :]
        across = [(r, (r + 2) % 4) for r in range(4)]

        hidden = jnp.concatenate([h_first, h_second], axis=0)
        res, qkv, xmid, tail_own = exchange_call(
            start_kernel, 0, "start", "vv" + "h" * 8,
            [hidden, gain(norm_self, 0), w_query, w_key, w_value, w_out, w_cquery, w_cout, w_gate, w_up],
            [res_t, qkv_t, mid_t, tail_t],
            [rowbuf(D), vm((depth, 3 * half)), rowbuf(3 * half), vm((block, tail_width)),
             dma(3, 7), dma(2, 2), dma(4), dma(2, 2)], 3_000_000_000)
        outs = None
        for l in range(layers):
            last = l == layers - 1
            xtail = lax.ppermute(tail_own, "row", across)
            k_out, v_out, mixed = self_attention(l, start_pos, qkv, table, caches[0], caches[1], outs)
            outs = (k_out, v_out)
            cache_buf = vm((seqs, D, cross_k.shape[2]))
            scratch = [cache_buf, cache_buf, vm((depth, D)), vm((depth, tail_width)), vm((fdepth, half)),
                       vm((2, rows, half), F32), vm((TOKENS, seqs, D), F32), rowbuf(D), colbuf(half), rowbuf(half),
                       rowbuf(D), colbuf(half), colbuf(ffc), colbuf(half),
                       dma(2, seqs), dma(2, 7), dma(3, 7), dma(1, 7), dma(4, 2), dma(4, 2, 2)]
            args = [enc_lens, mixed.reshape(rows, D), res, gain(norm_cross, l), gain(norm_mlp, l)]
            weights = [caches[2], caches[3], xmid, xtail, w_out, w_cquery, w_cout, w_gate, w_up, w_down]
            if last:
                hid, = exchange_call(
                    functools.partial(layer_kernel, l, True, seqs), 1 + l, "last", "svvvv" + "h" * 10,
                    args + weights, [("v", jax.ShapeDtypeStruct((rows, D), BF16))], scratch, 20_000_000_000)
            else:
                scratch += [vm((depth, 3 * half)), rowbuf(3 * half), vm((block, tail_width)),
                            dma(3, 7), dma(2, 2), dma(4)]
                res, qkv, xmid, tail_own = exchange_call(
                    functools.partial(layer_kernel, l, False, seqs), 1 + l, "layer", "svvvvv" + "h" * 13,
                    args + [gain(norm_self, l + 1)] + weights + [w_query, w_key, w_value],
                    [res_t, qkv_t, mid_t, tail_t], scratch, 20_000_000_000)

        def unflat(cache):
            return jnp.transpose(cache.reshape(layers, seqs, HEADS, HEAD_DIM, cache_len), (0, 1, 4, 2, 3))

        return hid.reshape(TOKENS, seqs, D), unflat(outs[0]), unflat(outs[1])

    row_spec = P(batch_axes, None)
    seq_spec = P(batch_axes)
    weight_spec = P(None, 'row', 'col')
    cache_spec = P(None, batch_axes)
    in_specs = (row_spec, row_spec, seq_spec, seq_spec, P(), P(), P(), P()) + (weight_spec,) * 9 + (cache_spec,) * 4
    out_specs = (P(None, batch_axes), cache_spec, cache_spec)
    return jax.shard_map(local_step, mesh=mesh, in_specs=in_specs, out_specs=out_specs, check_vma=False)
```

```python
import functools

import jax
import jax.numpy as jnp
import numpy as np
from jax import lax
from jax.experimental import pallas as pl
from jax.experimental.pallas import tpu as pltpu
from jax.sharding import PartitionSpec as P

NORM_EPS = 1e-6
BUCKET_EDGES = (16, 19, 21, 24, 27, 31, 35, 40, 46, 52, 59, 67, 77, 87, 99, 113)
HEADS = 12
HEAD_DIM = 64
D = HEADS * HEAD_DIM
TOKENS = 2
LANES = 128
HROWS = 16
NEG = -1e30
SEQ_BLOCK = 4
AHEAD = 8
MESH = pl.DeviceIdType.MESH
F32 = jnp.float32
BF16 = jnp.bfloat16
VMEM_LIMIT = 67_043_328


def dot32(a, b):
    return jnp.dot(a, b, preferred_element_type=F32)


def head_mask():
    row = lax.broadcasted_iota(jnp.int32, (HROWS, D), 0)
    col = lax.broadcasted_iota(jnp.int32, (HROWS, D), 1)
    return (col >= row * HEAD_DIM) & (col < (row + 1) * HEAD_DIM)


def spread_query(q_ref, b, seqs, hmask):
    rows = []
    for s in range(TOKENS):
        at = pl.ds(s * seqs + b, 1)
        row = jnp.concatenate([q_ref[0, at, 0:D // 2], q_ref[1, at, 0:D // 2]], axis=1)
        rows.append(jnp.where(hmask, jnp.broadcast_to(row, (HROWS, D)), 0.0))
    return jnp.concatenate(rows, axis=0).astype(BF16)


def softmax_rows(sc):
    top = jnp.max(sc, axis=1, keepdims=True)
    e = jnp.exp(sc - top)
    return (e / jnp.sum(e, axis=1, keepdims=True)).astype(BF16)


def mix_values(probs, values, seqids, hmask, o_ref):
    group = TOKENS * HROWS
    mixes = [lax.dot_general(probs[n * group:(n + 1) * group], values[b], (((1,), (1,)), ((), ())),
                             preferred_element_type=F32) for n, b in enumerate(seqids)]
    for b, mixed in zip(seqids, mixes):
        for s in range(TOKENS):
            part = jnp.where(hmask, mixed[s * HROWS:(s + 1) * HROWS], 0.0)
            row = jnp.sum(part, axis=0, keepdims=True)
            o_ref[s, pl.ds(b, 1), :] = row.astype(BF16).astype(F32)


def self_kernel(layer, seqs, aliased, pos_ref, qkv_ref, tab_ref, k_in, v_in, *rest):
    k_out, v_out, o_ref, kbuf, vbuf, kvt, in_sem, out_sem = rest[2 if aliased else 0:]
    half = D // 2
    cache_len = kbuf.shape[-1]
    sides = ((0, k_in, k_out, kbuf), (1, v_in, v_out, vbuf))

    def loads(b):
        return [pltpu.make_async_copy(src.at[layer, b], buf.at[b], in_sem.at[n, b]) for n, src, _, buf in sides]

    def stores(b):
        return [pltpu.make_async_copy(buf.at[b], dst.at[layer, b], out_sem.at[n, b]) for n, _, dst, buf in sides]

    for b in range(AHEAD):
        for copy in loads(b):
            copy.start()
    for which in range(2):
        for cb in range(2):
            lo = (which + 1) * half
            kvt[which, pl.ds(cb * half, half), :] = qkv_ref[cb, :, lo:lo + half].T.astype(BF16)

    def step(i, carry):
        hmask = head_mask()
        wide = 2 * LANES
        row_id = lax.broadcasted_iota(jnp.int32, (TOKENS * seqs, wide), 0)
        lane_id = lax.broadcasted_iota(jnp.int32, (TOKENS * seqs, wide), 1)
        lane_row = lax.broadcasted_iota(jnp.int32, (D, wide), 1)
        t_id = lax.broadcasted_iota(jnp.int32, (HROWS, cache_len), 1)
        seqids = [i * SEQ_BLOCK + j for j in range(SEQ_BLOCK)]
        for b in seqids:
            ahead = b + AHEAD

            @pl.when(ahead < seqs)
            def _():
                for copy in loads(ahead):
                    copy.start()
        for b in seqids:
            for copy in loads(b):
                copy.wait()
        for b in seqids:
            p = pos_ref[b]
            off = pl.multiple_of(jnp.minimum(p // LANES, cache_len // LANES - 2) * LANES, LANES)
            lane = p - off
            sel = ((row_id == b) & (lane_id == lane)) | ((row_id == seqs + b) & (lane_id == lane + 1))
            sel = jnp.where(sel, 1.0, 0.0).astype(BF16)
            here = (lane_row == lane) | (lane_row == lane + 1)
            for n, _, _, buf in sides:
                ins = dot32(kvt[n], sel)
                old = buf[b, :, pl.ds(off, wide)].astype(F32)
                buf[b, :, pl.ds(off, wide)] = jnp.where(here, ins, old).astype(BF16)
            for copy in stores(b):
                copy.start()
        queries = [spread_query(qkv_ref, b, seqs, hmask) for b in seqids]
        scores = [dot32(q, kbuf[b]) for q, b in zip(queries, seqids)]
        parts = []
        for b, sc in zip(seqids, scores):
            for s in range(TOKENS):
                t = pos_ref[b] + s
                bias = pltpu.roll(tab_ref[...], lax.rem(t + 1, cache_len), 1)
                parts.append(jnp.where(t_id <= t, sc[s * HROWS:(s + 1) * HROWS] + bias, NEG))
        mix_values(softmax_rows(jnp.concatenate(parts, axis=0)), vbuf, seqids, hmask, o_ref)
        return carry

    lax.fori_loop(0, seqs // SEQ_BLOCK, step, 0)
    for b in range(seqs):
        for copy in stores(b):
            copy.wait()


def self_attention(layer, pos, qkv, table, cache_k, cache_v, outs):
    layers, seqs, _, cache_len = cache_k.shape
    vm = pl.BlockSpec(memory_space=pltpu.VMEM)
    hb = pl.BlockSpec(memory_space=pl.ANY)
    in_specs = [pl.BlockSpec(memory_space=pltpu.SMEM), vm, vm, hb, hb]
    args = [pos, qkv, table, cache_k, cache_v]
    aliases = {}
    if outs is not None:
        in_specs += [hb, hb]
        args += list(outs)
        aliases = {5: 0, 6: 1}
    buf = pltpu.VMEM((seqs, D, cache_len), BF16)
    return pl.pallas_call(
        functools.partial(self_kernel, layer, seqs, outs is not None),
        out_shape=(jax.ShapeDtypeStruct(cache_k.shape, BF16), jax.ShapeDtypeStruct(cache_v.shape, BF16),
                   jax.ShapeDtypeStruct((TOKENS, seqs, D), F32)),
        in_specs=in_specs,
        out_specs=[hb, hb, vm],
        scratch_shapes=[buf, buf, pltpu.VMEM((2, D, TOKENS * seqs), BF16),
                        pltpu.SemaphoreType.DMA((2, seqs)), pltpu.SemaphoreType.DMA((2, seqs))],
        input_output_aliases=aliases,
        cost_estimate=pl.CostEstimate(flops=20_000_000_000, bytes_accessed=4 * seqs * D * cache_len * 2,
                                      transcendentals=0),
        compiler_params=pltpu.CompilerParams(vmem_limit_bytes=VMEM_LIMIT),
        name="self_attn",
    )(*args)


def rms(res, gain):
    mean_sq = jnp.mean(res * res, axis=-1, keepdims=True)
    return (res * lax.rsqrt(mean_sq + NORM_EPS) * gain.astype(F32)).astype(BF16)


class Stage:
    def __init__(self):
        dp, self.c, self.r = lax.axis_index("dp"), lax.axis_index("col"), lax.axis_index("row")
        self.across = (self.r + 2) % 4
        core = self.r + 1 - 2 * (self.r % 2)
        self.peer = (dp, 1 - self.c, self.r)
        self.partner = (dp, self.c, core)
        self.xpeer = (dp, self.c, self.across)

    def greet(self):
        barrier = pltpu.get_barrier_semaphore()
        for other in (self.peer, self.partner, self.xpeer):
            pl.semaphore_signal(barrier, inc=1, device_id=other, device_id_type=MESH)
        pl.semaphore_wait(barrier, 3)

    def remote(self, src, dst, send_sem, recv_sem, to):
        return pltpu.make_async_remote_copy(src_ref=src, dst_ref=dst, send_sem=send_sem, recv_sem=recv_sem,
                                            device_id=to, device_id_type=MESH)

    def send(self, src, dst, sems):
        copy = self.remote(src, dst, sems.at[0], sems.at[1], self.peer)
        copy.start()
        return copy

    def trade_rows(self, own, buf, sems):
        buf[0] = own
        self.send(buf.at[0], buf.at[1], sems).wait()
        return jnp.concatenate([buf[0], buf[1]], axis=0)

    def trade_columns(self, mine, buf, sems):
        rows, width = mine.shape[0] // 2, mine.shape[1]
        c = self.c
        buf[c] = mine.astype(BF16).reshape(2, rows, width)
        first = self.send(buf.at[c, 0], buf.at[c, 1], sems.at[0])
        second = self.send(buf.at[c, 1], buf.at[c, 0], sems.at[1])
        first.wait()
        second.wait()
        return jnp.concatenate([buf[0].reshape(2 * rows, width), buf[1].reshape(2 * rows, width)], axis=1)

    def give_rows(self, mine, buf, sems, out_ref):
        rows = mine.shape[0] // 2
        c = self.c
        mine = mine.astype(BF16)
        buf[0] = mine[rows:]
        copy = self.send(buf.at[0], buf.at[1], sems)
        out_ref[c] = mine[:rows].astype(F32)
        copy.wait()
        out_ref[1 - c] = buf[1].astype(F32)


class Weight:
    def __init__(self, st, own, dst, col, sems, crossed=None):
        depth, width = own.shape
        self.st, self.crossed = st, crossed

        def place(owner):
            return dst.at[pl.ds(pl.multiple_of(owner * depth, depth), depth), pl.ds(col, width)]

        mine, theirs = place(st.r), place(st.across)
        self.local = pltpu.make_async_copy(own, mine, sems.at[0])
        self.share = st.remote(own, mine, sems.at[1], sems.at[2], st.partner)
        if crossed is None:
            self.cross = st.remote(own, mine, sems.at[3], sems.at[4], st.xpeer)
            self.pass_on = st.remote(theirs, theirs, sems.at[5], sems.at[6], st.partner)
        else:
            self.cross = pltpu.make_async_copy(crossed, theirs, sems.at[3])
            self.pass_on = st.remote(crossed, theirs, sems.at[5], sems.at[6], st.partner)

    def open_local(self):
        self.local.start()
        if self.crossed is not None:
            self.cross.start()

    def open_cross(self):
        if self.crossed is None:
            self.cross.start()

    def open_share(self):
        self.share.start()
        if self.crossed is not None:
            self.pass_on.start()

    def relay(self):
        if self.crossed is None:
            self.cross.wait_recv()
            self.pass_on.start()

    def finish(self):
        self.local.wait()
        self.share.wait()
        if self.crossed is None:
            self.cross.wait_send()
        else:
            self.cross.wait()
        self.pass_on.wait()


def each(items, name):
    for item in items:
        getattr(item, name)()


def weights_of(st, refs, layer, dst, sems, crossed=None):
    col, found = 0, []
    for n, ref in enumerate(refs):
        width = ref.shape[2]
        given = None if crossed is None else crossed.at[:, pl.ds(col, width)]
        found.append(Weight(st, ref.at[layer], dst, col, sems.at[n], given))
        col += width
    return found


def forward(st, refs, layer, dst, sems):
    col, copies = 0, []
    for n, ref in enumerate(refs):
        width = ref.shape[2]
        copies.append(st.remote(ref.at[layer], dst.at[:, pl.ds(col, width)], sems.at[n, 0], sems.at[n, 1], st.xpeer))
        col += width
    return copies


def collect(refs, layer, dst, sems):
    col, copies = 0, []
    for n, ref in enumerate(refs):
        width = ref.shape[2]
        copies.append(pltpu.make_async_copy(ref.at[layer], dst.at[:, pl.ds(col, width)], sems.at[n]))
        col += width
    return copies


class Whole:
    def __init__(self, st, packs, dst, sems):
        block = packs[0].shape[1]
        self.locals, self.shares = [], []
        for n, (pack, cb) in enumerate(zip(packs, (st.c, 1 - st.c))):
            for m, owner in enumerate((st.r, st.across)):
                place = dst.at[cb, pl.ds(pl.multiple_of(owner * block, block), block), :]
                self.locals.append(pltpu.make_async_copy(pack.at[m], place, sems.at[n, m, 0]))
                self.shares.append(st.remote(pack.at[m], place, sems.at[n, m, 1], sems.at[n, m, 2], st.partner))

    def open_local(self):
        each(self.locals, "start")

    def open_share(self):
        each(self.shares, "start")

    def finish(self):
        each(self.locals, "wait")
        each(self.shares, "wait")


class NextLayer:
    def __init__(self, st, attn, mlp, layer, pack_ref, tail_ref, pbuf, tbuf, sems, xsems):
        self.loads = collect(attn, layer, pbuf, sems.at[0]) + collect(mlp, layer, tbuf, sems.at[1])
        self.sends = forward(st, attn, layer, pack_ref.at[1], xsems)
        self.stores = [pltpu.make_async_copy(pbuf, pack_ref.at[0], sems.at[2, 0]),
                       pltpu.make_async_copy(tbuf, tail_ref, sems.at[2, 1])]

    def store(self):
        each(self.loads, "wait")
        each(self.stores, "start")

    def finish(self):
        each(self.stores, "wait")
        each(self.sends, "wait")


def start_kernel(h_ref, gain_ref, wq_r, wk_r, wv_r, wo_r, wc_r, wco_r, wg_r, wu_r,
                 x_ref, qkv_ref, pack_ref, tail_ref, hbuf, wqkv, qbuf, pbuf, tbuf, wsem, nsem, xsem, sem):
    st = Stage()
    weights = weights_of(st, (wq_r, wk_r, wv_r), 0, wqkv, wsem)
    coming = NextLayer(st, (wo_r, wc_r, wco_r), (wg_r, wu_r), 0, pack_ref, tail_ref, pbuf, tbuf, nsem, xsem)
    each(weights, "open_local")
    each(coming.loads, "start")
    st.greet()
    each(weights, "open_cross")
    each(coming.sends, "start")
    each(weights, "open_share")
    res = st.trade_rows(h_ref[...], hbuf, sem.at[0]).astype(F32)
    x_ref[...] = res[:h_ref.shape[0]]
    normed = rms(res, gain_ref[...])
    coming.store()
    each(weights, "relay")
    each(weights, "finish")
    st.give_rows(dot32(normed, wqkv[...]), qbuf, sem.at[1], qkv_ref)
    coming.finish()


def both_blocks(act, packed, which):
    half = D // 2
    cols = slice(which * half, (which + 1) * half)
    return [dot32(act, packed[cb, :, cols]).astype(BF16) for cb in range(2)]


def layer_kernel(layer, last, seqs, len_ref, o_ref, x_ref, gcross_ref, gmlp_ref, *refs):
    if last:
        (ck, cv, pack_in, ypack_in, xtail_in, wg_r, wu_r, wd_r, hid_ref,
         kbuf, vbuf, wattn, wtail, wdown, qs, os, ubuf, kvsem, asem, wtsem, dsem, sem, sem2, nbuf, zbuf, zs) = refs
    else:
        (gself_ref, ck, cv, pack_in, ypack_in, xtail_in, wg_r, wu_r, wd_r, wq_r, wk_r, wv_r, wo_r, wc_r, wco_r,
         x_out, qkv_ref, pack_ref, tail_ref,
         kbuf, vbuf, wattn, wtail, wdown, qs, os, ubuf, kvsem, asem, wtsem, dsem, sem, sem2,
         rbuf, zbuf, wqkv, qkvbuf, pbuf, tbuf, wsem, nsem, xsem) = refs
    st = Stage()
    rows = o_ref.shape[0]
    attn = Whole(st, (pack_in, ypack_in), wattn, asem)
    tail = weights_of(st, (wg_r, wu_r), layer, wtail, wtsem, xtail_in)
    down = weights_of(st, (wd_r,), layer, wdown, dsem)
    attn.open_local()

    def caches(b):
        return [pltpu.make_async_copy(src.at[layer, b], buf.at[b], kvsem.at[n, b])
                for n, (src, buf) in enumerate(((ck, kbuf), (cv, vbuf)))]

    def fetch_caches(b, carry):
        each(caches(b), "start")
        return carry

    st.greet()
    attn.open_share()
    each(down, "open_cross")
    lax.fori_loop(0, seqs, fetch_caches, 0)
    each(tail, "open_local")
    each(down, "open_local")
    if not last:
        ahead = weights_of(st, (wq_r, wk_r, wv_r), layer + 1, wqkv, wsem)
        coming = NextLayer(st, (wo_r, wc_r, wco_r), (wg_r, wu_r), layer + 1, pack_ref, tail_ref, pbuf, tbuf,
                           nsem, xsem)
        each(ahead, "open_cross")
        each(coming.sends, "start")
        each(ahead, "open_local")
        each(coming.loads, "start")
    attn.finish()
    y = jnp.concatenate(both_blocks(o_ref[...].astype(BF16), wattn, 0), axis=1)
    res = x_ref[...] + y.astype(F32)
    for cb, q in enumerate(both_blocks(rms(res, gcross_ref[...]), wattn, 1)):
        qs[cb] = q.astype(F32)
    each(tail, "open_share")
    each(down, "open_share")
    if not last:
        each(ahead, "open_share")
        coming.store()

    def cross_step(i, carry):
        hmask = head_mask()
        t_id = lax.broadcasted_iota(jnp.int32, (TOKENS * HROWS, kbuf.shape[-1]), 1)
        seqids = [i * SEQ_BLOCK + j for j in range(SEQ_BLOCK)]
        for b in seqids:
            each(caches(b), "wait")
        queries = [spread_query(qs, b, seqs, hmask) for b in seqids]
        scores = [dot32(q, kbuf[b]) for q, b in zip(queries, seqids)]
        parts = [jnp.where(t_id < len_ref[b], sc, NEG) for b, sc in zip(seqids, scores)]
        mix_values(softmax_rows(jnp.concatenate(parts, axis=0)), vbuf, seqids, hmask, os)
        return carry

    lax.fori_loop(0, seqs // SEQ_BLOCK, cross_step, 0)
    each(down, "relay")
    y = jnp.concatenate(both_blocks(os[...].reshape(rows, D).astype(BF16), wattn, 2), axis=1)
    res = res + y.astype(F32)
    if last:
        normed = st.trade_rows(rms(res, gmlp_ref[...]), nbuf, sem.at[0])
    else:
        res = st.trade_rows(res, rbuf, sem.at[0])
        normed = rms(res, gmlp_ref[...])
    each(tail, "finish")
    ff = wtail.shape[1] // 2
    gate = dot32(normed, wtail[:, 0:ff]).astype(BF16).astype(F32)
    up = dot32(normed, wtail[:, ff:2 * ff]).astype(BF16).astype(F32)
    act = st.trade_columns(gate * jax.nn.sigmoid(gate) * up, ubuf, sem2.at[0])
    if not last:
        each(ahead, "relay")
    each(down, "finish")
    z = dot32(act, wdown[...])
    if last:
        st.give_rows(z, zbuf, sem.at[1], zs)
        hid_ref[...] = (res + jnp.concatenate([zs[0], zs[1]], axis=1)).astype(BF16)
    else:
        res = res + st.trade_columns(z, zbuf, sem2.at[1]).astype(F32)
        x_out[...] = res[:rows]
        normed = rms(res, gself_ref[...])
        each(ahead, "finish")
        st.give_rows(dot32(normed, wqkv[...]), qkvbuf, sem.at[1], qkv_ref)
        coming.finish()


def exchange_call(kernel, cid, name, specs, args, outs, scratch, flops):
    spaces = {"s": pltpu.SMEM, "v": pltpu.VMEM, "h": pl.ANY}
    spec = lambda letters: [pl.BlockSpec(memory_space=spaces[x]) for x in letters]
    return pl.pallas_call(
        kernel,
        out_shape=tuple(t for _, t in outs),
        in_specs=spec(specs),
        out_specs=tuple(spec(x for x, _ in outs)),
        scratch_shapes=scratch,
        cost_estimate=pl.CostEstimate(flops=flops, bytes_accessed=8 << 20, transcendentals=0),
        compiler_params=pltpu.CompilerParams(collective_id=cid, has_side_effects=True, vmem_limit_bytes=VMEM_LIMIT),
        name=name,
    )(*args)


def bias_table(dec_bias, cache_len):
    dist = np.arange(cache_len)[::-1]
    far = BUCKET_EDGES[0] - 1 + np.sum(dist[:, None] >= np.array(BUCKET_EDGES)[None, :], axis=1)
    bucket = np.where(dist < BUCKET_EDGES[0], dist, far)
    onehot = (np.arange(dec_bias.shape[0])[:, None] == bucket[None, :]).astype(np.float32)
    padded = jnp.pad(dec_bias, ((0, 0), (0, HROWS - dec_bias.shape[1])))
    return lax.dot_general(padded, jnp.asarray(onehot), (((0,), (0,)), ((), ())),
                           precision=lax.Precision.HIGHEST, preferred_element_type=F32)


def solution(mesh):
    batch_axes = ('dp', 'col', 'row')

    def local_step(h_first, h_second, start_pos, enc_lens, dec_bias, norm_self, norm_cross, norm_mlp,
                   w_query, w_key, w_value, w_out, w_cquery, w_cout, w_gate, w_up, w_down,
                   self_k, self_v, cross_k, cross_v):
        layers, seqs, cache_len = self_k.shape[:3]
        rows = TOKENS * seqs
        half = D // 2
        ffc = w_gate.shape[2]
        depth = 4 * w_query.shape[1]
        fdepth = 4 * w_down.shape[1]

        def flat(cache):
            return jnp.transpose(cache, (0, 1, 3, 4, 2)).reshape(layers, seqs, D, cache.shape[2])

        caches = [flat(a) for a in (self_k, self_v, cross_k, cross_v)]
        table = bias_table(dec_bias, cache_len)
        block = w_query.shape[1]

        vm = lambda shape, dt=BF16: pltpu.VMEM(shape, dt)
        dma = lambda *shape: pltpu.SemaphoreType.DMA(shape)
        rowbuf = lambda width, dt=BF16: vm((2, rows, width), dt)
        colbuf = lambda width: vm((2, 2, rows, width))
        res_t = ("v", jax.ShapeDtypeStruct((rows, D), F32))
        qkv_t = ("v", jax.ShapeDtypeStruct((2, rows, 3 * half), F32))
        pack_t = ("h", jax.ShapeDtypeStruct((2, block, 3 * half), BF16))
        tail_t = ("h", jax.ShapeDtypeStruct((block, 2 * ffc), BF16))
        coming = [vm((block, 3 * half)), vm((block, 2 * ffc))]
        gain = lambda g, l: g[l][None, :]
        across = [(r, (r + 2) % 4) for r in range(4)]
        flip = [(0, 1), (1, 0)]

        hidden = jnp.concatenate([h_first, h_second], axis=0)
        res, qkv, pack, tail_own = exchange_call(
            start_kernel, 0, "start", "vv" + "h" * 8,
            [hidden, gain(norm_self, 0), w_query, w_key, w_value, w_out, w_cquery, w_cout, w_gate, w_up],
            [res_t, qkv_t, pack_t, tail_t],
            [rowbuf(D), vm((depth, 3 * half)), rowbuf(3 * half)] + coming
            + [dma(3, 7), dma(3, 3), dma(3, 2), dma(2, 2)], 3_000_000_000)
        outs = None
        for l in range(layers):
            last = l == layers - 1
            ypack = lax.ppermute(pack, "col", flip)
            xtail = lax.ppermute(tail_own, "row", across)
            k_out, v_out, mixed = self_attention(l, start_pos, qkv, table, caches[0], caches[1], outs)
            outs = (k_out, v_out)
            cache_buf = vm((seqs, D, cross_k.shape[2]))
            scratch = [cache_buf, cache_buf, vm((2, depth, 3 * half)), vm((depth, 2 * ffc)), vm((fdepth, half)),
                       vm((2, rows, half), F32), vm((TOKENS, seqs, D), F32), colbuf(ffc),
                       dma(2, seqs), dma(2, 2, 3), dma(2, 7), dma(1, 7), dma(2, 2), dma(2, 2, 2)]
            args = [enc_lens, mixed.reshape(rows, D), res, gain(norm_cross, l), gain(norm_mlp, l)]
            weights = [caches[2], caches[3], pack, ypack, xtail, w_gate, w_up, w_down]
            if last:
                hid, = exchange_call(
                    functools.partial(layer_kernel, l, True, seqs), 1 + l, "last", "svvvv" + "h" * 8,
                    args + weights, [("v", jax.ShapeDtypeStruct((rows, D), BF16))],
                    scratch + [rowbuf(D), rowbuf(half), vm((2, rows, half), F32)], 20_000_000_000)
            else:
                scratch += [rowbuf(D, F32), colbuf(half), vm((depth, 3 * half)), rowbuf(3 * half)] + coming
                scratch += [dma(3, 7), dma(3, 3), dma(3, 2)]
                res, qkv, pack, tail_own = exchange_call(
                    functools.partial(layer_kernel, l, False, seqs), 1 + l, "layer", "svvvvv" + "h" * 14,
                    args + [gain(norm_self, l + 1)] + weights
                    + [w_query, w_key, w_value, w_out, w_cquery, w_cout],
                    [res_t, qkv_t, pack_t, tail_t], scratch, 20_000_000_000)

        def unflat(cache):
            return jnp.transpose(cache.reshape(layers, seqs, HEADS, HEAD_DIM, cache_len), (0, 1, 4, 2, 3))

        return hid.reshape(TOKENS, seqs, D), unflat(outs[0]), unflat(outs[1])

    row_spec = P(batch_axes, None)
    seq_spec = P(batch_axes)
    weight_spec = P(None, 'row', 'col')
    cache_spec = P(None, batch_axes)
    in_specs = (row_spec, row_spec, seq_spec, seq_spec, P(), P(), P(), P()) + (weight_spec,) * 9 + (cache_spec,) * 4
    out_specs = (P(None, batch_axes), cache_spec, cache_spec)
    return jax.shard_map(local_step, mesh=mesh, in_specs=in_specs, out_specs=out_specs, check_vma=False)
```

```python
import functools

import jax
import jax.numpy as jnp
from jax import lax
from jax.experimental import pallas as pl
from jax.experimental.pallas import tpu as pltpu
from jax.sharding import PartitionSpec as P

NORM_EPS = 1e-6
BUCKET_EDGES = (16, 19, 21, 24, 27, 31, 35, 40, 46, 52, 59, 67, 77, 87, 99, 113)
HEADS = 12
HEAD_DIM = 64
D = HEADS * HEAD_DIM
TOKENS = 2
LANES = 128
HROWS = 16
NEG = -1e30
SEQ_BLOCK = 4
AHEAD = 8
MESH = pl.DeviceIdType.MESH
F32 = jnp.float32
BF16 = jnp.bfloat16
VMEM_LIMIT = 67_043_328


def dot32(a, b):
    return jnp.dot(a, b, preferred_element_type=F32)


def head_mask():
    row = lax.broadcasted_iota(jnp.int32, (HROWS, D), 0)
    col = lax.broadcasted_iota(jnp.int32, (HROWS, D), 1)
    return (col >= row * HEAD_DIM) & (col < (row + 1) * HEAD_DIM)


def spread_query(q_ref, b, seqs, hmask):
    rows = []
    for s in range(TOKENS):
        at = pl.ds(s * seqs + b, 1)
        row = jnp.concatenate([q_ref[0, at, 0:D // 2], q_ref[1, at, 0:D // 2]], axis=1)
        rows.append(jnp.where(hmask, jnp.broadcast_to(row, (HROWS, D)), 0.0))
    return jnp.concatenate(rows, axis=0).astype(BF16)


def softmax_rows(sc):
    top = jnp.max(sc, axis=1, keepdims=True)
    e = jnp.exp(sc - top)
    return (e / jnp.sum(e, axis=1, keepdims=True)).astype(BF16)


def mix_values(probs, values, seqids, hmask, o_ref):
    group = TOKENS * HROWS
    mixes = [lax.dot_general(probs[n * group:(n + 1) * group], values[b], (((1,), (1,)), ((), ())),
                             preferred_element_type=F32) for n, b in enumerate(seqids)]
    for b, mixed in zip(seqids, mixes):
        for s in range(TOKENS):
            part = jnp.where(hmask, mixed[s * HROWS:(s + 1) * HROWS], 0.0)
            row = jnp.sum(part, axis=0, keepdims=True)
            o_ref[s, pl.ds(b, 1), :] = row.astype(BF16).astype(F32)


def self_kernel(layer, seqs, aliased, pos_ref, qkv_ref, tab_ref, k_in, v_in, *rest):
    k_out, v_out, o_ref, kbuf, vbuf, kvt, in_sem, out_sem = rest[2 if aliased else 0:]
    half = D // 2
    cache_len = kbuf.shape[-1]
    sides = ((0, k_in, k_out, kbuf), (1, v_in, v_out, vbuf))

    def loads(b):
        return [pltpu.make_async_copy(src.at[layer, b], buf.at[b], in_sem.at[n, b]) for n, src, _, buf in sides]

    def stores(b):
        return [pltpu.make_async_copy(buf.at[b], dst.at[layer, b], out_sem.at[n, b]) for n, _, dst, buf in sides]

    for b in range(AHEAD):
        for copy in loads(b):
            copy.start()
    for which in range(2):
        for cb in range(2):
            lo = (which + 1) * half
            kvt[which, pl.ds(cb * half, half), :] = qkv_ref[cb, :, lo:lo + half].T.astype(BF16)

    def step(i, carry):
        hmask = head_mask()
        wide = 2 * LANES
        row_id = lax.broadcasted_iota(jnp.int32, (TOKENS * seqs, wide), 0)
        lane_id = lax.broadcasted_iota(jnp.int32, (TOKENS * seqs, wide), 1)
        lane_row = lax.broadcasted_iota(jnp.int32, (D, wide), 1)
        t_id = lax.broadcasted_iota(jnp.int32, (HROWS, cache_len), 1)
        seqids = [i * SEQ_BLOCK + j for j in range(SEQ_BLOCK)]
        for b in seqids:
            ahead = b + AHEAD

            @pl.when(ahead < seqs)
            def _():
                for copy in loads(ahead):
                    copy.start()
        for b in seqids:
            for copy in loads(b):
                copy.wait()
        for b in seqids:
            p = pos_ref[b]
            off = pl.multiple_of(jnp.minimum(p // LANES, cache_len // LANES - 2) * LANES, LANES)
            lane = p - off
            sel = ((row_id == b) & (lane_id == lane)) | ((row_id == seqs + b) & (lane_id == lane + 1))
            sel = jnp.where(sel, 1.0, 0.0).astype(BF16)
            here = (lane_row == lane) | (lane_row == lane + 1)
            for n, _, _, buf in sides:
                ins = dot32(kvt[n], sel)
                old = buf[b, :, pl.ds(off, wide)].astype(F32)
                buf[b, :, pl.ds(off, wide)] = jnp.where(here, ins, old).astype(BF16)
            for copy in stores(b):
                copy.start()
        queries = [spread_query(qkv_ref, b, seqs, hmask) for b in seqids]
        scores = [dot32(q, kbuf[b]) for q, b in zip(queries, seqids)]
        parts = []
        for b, sc in zip(seqids, scores):
            for s in range(TOKENS):
                t = pos_ref[b] + s
                bias = pltpu.roll(tab_ref[...], lax.rem(t + 1, cache_len), 1)
                parts.append(jnp.where(t_id <= t, sc[s * HROWS:(s + 1) * HROWS] + bias, NEG))
        mix_values(softmax_rows(jnp.concatenate(parts, axis=0)), vbuf, seqids, hmask, o_ref)
        return carry

    lax.fori_loop(0, seqs // SEQ_BLOCK, step, 0)
    for b in range(seqs):
        for copy in stores(b):
            copy.wait()


def self_attention(layer, pos, qkv, table, cache_k, cache_v, outs):
    layers, seqs, _, cache_len = cache_k.shape
    vm = pl.BlockSpec(memory_space=pltpu.VMEM)
    hb = pl.BlockSpec(memory_space=pl.ANY)
    in_specs = [pl.BlockSpec(memory_space=pltpu.SMEM), vm, vm, hb, hb]
    args = [pos, qkv, table, cache_k, cache_v]
    aliases = {}
    if outs is not None:
        in_specs += [hb, hb]
        args += list(outs)
        aliases = {5: 0, 6: 1}
    buf = pltpu.VMEM((seqs, D, cache_len), BF16)
    return pl.pallas_call(
        functools.partial(self_kernel, layer, seqs, outs is not None),
        out_shape=(jax.ShapeDtypeStruct(cache_k.shape, BF16), jax.ShapeDtypeStruct(cache_v.shape, BF16),
                   jax.ShapeDtypeStruct((TOKENS, seqs, D), F32)),
        in_specs=in_specs,
        out_specs=[hb, hb, vm],
        scratch_shapes=[buf, buf, pltpu.VMEM((2, D, TOKENS * seqs), BF16),
                        pltpu.SemaphoreType.DMA((2, seqs)), pltpu.SemaphoreType.DMA((2, seqs))],
        input_output_aliases=aliases,
        cost_estimate=pl.CostEstimate(flops=20_000_000_000, bytes_accessed=4 * seqs * D * cache_len * 2,
                                      transcendentals=0),
        compiler_params=pltpu.CompilerParams(vmem_limit_bytes=VMEM_LIMIT),
        name="self_attn",
    )(*args)


def rms(res, gain):
    mean_sq = jnp.mean(res * res, axis=-1, keepdims=True)
    return (res * lax.rsqrt(mean_sq + NORM_EPS) * gain.astype(F32)).astype(BF16)


class Stage:
    def __init__(self):
        dp, self.c, self.r = lax.axis_index("dp"), lax.axis_index("col"), lax.axis_index("row")
        self.across = (self.r + 2) % 4
        core = self.r + 1 - 2 * (self.r % 2)
        self.peer = (dp, 1 - self.c, self.r)
        self.partner = (dp, self.c, core)
        self.xpeer = (dp, self.c, self.across)

    def greet(self):
        barrier = pltpu.get_barrier_semaphore()
        for other in (self.peer, self.partner, self.xpeer):
            pl.semaphore_signal(barrier, inc=1, device_id=other, device_id_type=MESH)
        pl.semaphore_wait(barrier, 3)

    def remote(self, src, dst, send_sem, recv_sem, to):
        return pltpu.make_async_remote_copy(src_ref=src, dst_ref=dst, send_sem=send_sem, recv_sem=recv_sem,
                                            device_id=to, device_id_type=MESH)

    def send(self, src, dst, sems):
        copy = self.remote(src, dst, sems.at[0], sems.at[1], self.peer)
        copy.start()
        return copy

    def trade_rows(self, own, buf, sems):
        buf[0] = own
        self.send(buf.at[0], buf.at[1], sems).wait()
        return jnp.concatenate([buf[0], buf[1]], axis=0)

    def trade_columns(self, mine, buf, sems):
        rows, width = mine.shape[0] // 2, mine.shape[1]
        c = self.c
        buf[c] = mine.astype(BF16).reshape(2, rows, width)
        first = self.send(buf.at[c, 0], buf.at[c, 1], sems.at[0])
        second = self.send(buf.at[c, 1], buf.at[c, 0], sems.at[1])
        first.wait()
        second.wait()
        return jnp.concatenate([buf[0].reshape(2 * rows, width), buf[1].reshape(2 * rows, width)], axis=1)

    def give_rows(self, mine, buf, sems, out_ref):
        rows = mine.shape[0] // 2
        c = self.c
        mine = mine.astype(BF16)
        buf[0] = mine[rows:]
        copy = self.send(buf.at[0], buf.at[1], sems)
        out_ref[c] = mine[:rows].astype(F32)
        copy.wait()
        out_ref[1 - c] = buf[1].astype(F32)


class Weight:
    def __init__(self, st, own, dst, col, sems, crossed=None):
        depth, width = own.shape
        self.st, self.crossed = st, crossed

        def place(owner):
            return dst.at[pl.ds(pl.multiple_of(owner * depth, depth), depth), pl.ds(col, width)]

        mine, theirs = place(st.r), place(st.across)
        self.local = pltpu.make_async_copy(own, mine, sems.at[0])
        self.share = st.remote(own, mine, sems.at[1], sems.at[2], st.partner)
        if crossed is None:
            self.cross = st.remote(own, mine, sems.at[3], sems.at[4], st.xpeer)
            self.pass_on = st.remote(theirs, theirs, sems.at[5], sems.at[6], st.partner)
        else:
            self.cross = pltpu.make_async_copy(crossed, theirs, sems.at[3])
            self.pass_on = st.remote(crossed, theirs, sems.at[5], sems.at[6], st.partner)

    def open_local(self):
        self.local.start()
        if self.crossed is not None:
            self.cross.start()

    def open_cross(self):
        if self.crossed is None:
            self.cross.start()

    def open_share(self):
        self.share.start()
        if self.crossed is not None:
            self.pass_on.start()

    def relay(self):
        if self.crossed is None:
            self.cross.wait_recv()
            self.pass_on.start()

    def finish(self):
        self.local.wait()
        self.share.wait()
        if self.crossed is None:
            self.cross.wait_send()
        else:
            self.cross.wait()
        self.pass_on.wait()


def each(items, name):
    for item in items:
        getattr(item, name)()


def weights_of(st, refs, layer, dst, sems, crossed=None):
    col, found = 0, []
    for n, ref in enumerate(refs):
        width = ref.shape[2]
        given = None if crossed is None else crossed.at[:, pl.ds(col, width)]
        found.append(Weight(st, ref.at[layer], dst, col, sems.at[n], given))
        col += width
    return found


def forward(st, refs, layer, dst, sems):
    col, copies = 0, []
    for n, ref in enumerate(refs):
        width = ref.shape[2]
        copies.append(st.remote(ref.at[layer], dst.at[:, pl.ds(col, width)], sems.at[n, 0], sems.at[n, 1], st.xpeer))
        col += width
    return copies


def collect(refs, layer, dst, sems):
    col, copies = 0, []
    for n, ref in enumerate(refs):
        width = ref.shape[2]
        copies.append(pltpu.make_async_copy(ref.at[layer], dst.at[:, pl.ds(col, width)], sems.at[n]))
        col += width
    return copies


class Whole:
    def __init__(self, st, packs, dst, sems):
        block, half = packs[0].shape[1], D // 2
        self.locals, self.shares = [], []
        for w in range(packs[0].shape[2] // half):
            cols = pl.ds(w * half, half)
            self.locals.append([])
            self.shares.append([])
            for n, (pack, cb) in enumerate(zip(packs, (st.c, 1 - st.c))):
                for m, owner in enumerate((st.r, st.across)):
                    src = pack.at[m, :, cols]
                    place = dst.at[cb, pl.ds(pl.multiple_of(owner * block, block), block), cols]
                    sem = sems.at[w, n, m]
                    self.locals[w].append(pltpu.make_async_copy(src, place, sem.at[0]))
                    self.shares[w].append(st.remote(src, place, sem.at[1], sem.at[2], st.partner))

    def open_local(self):
        for copies in self.locals:
            each(copies, "start")

    def open_share(self):
        for copies in self.shares:
            each(copies, "start")

    def finish(self, w):
        each(self.locals[w], "wait")
        each(self.shares[w], "wait")


class NextLayer:
    def __init__(self, st, attn, mlp, layer, pack_ref, tail_ref, pbuf, tbuf, sems, xsems):
        self.loads = collect(attn, layer, pbuf, sems.at[0]) + collect(mlp, layer, tbuf, sems.at[1])
        self.sends = forward(st, attn, layer, pack_ref.at[1], xsems)
        self.stores = [pltpu.make_async_copy(pbuf, pack_ref.at[0], sems.at[2, 0]),
                       pltpu.make_async_copy(tbuf, tail_ref, sems.at[2, 1])]

    def store(self):
        each(self.loads, "wait")
        each(self.stores, "start")

    def finish(self):
        each(self.stores, "wait")
        each(self.sends, "wait")


def bias_table(bias_ref, tab_ref):
    buckets, length = bias_ref.shape[1], tab_ref.shape[1]
    dist = length - 1 - lax.broadcasted_iota(jnp.int32, (buckets, length), 1)
    far = jnp.full((buckets, length), BUCKET_EDGES[0] - 1, jnp.int32)
    for edge in BUCKET_EDGES:
        far = far + jnp.where(dist >= edge, 1, 0)
    bucket = jnp.where(dist < BUCKET_EDGES[0], dist, far)
    pick = jnp.where(bucket == lax.broadcasted_iota(jnp.int32, (buckets, length), 0), 1.0, 0.0).astype(BF16)
    left = jnp.concatenate([bias_ref[...], jnp.zeros((HROWS - bias_ref.shape[0], buckets), F32)], axis=0)
    total = jnp.zeros((HROWS, length), F32)
    for _ in range(3):
        part = left.astype(BF16)
        total = total + dot32(part, pick)
        left = left - part.astype(F32)
    tab_ref[...] = total


def start_kernel(first_ref, second_ref, gain_ref, bias_ref, wq_r, wk_r, wv_r, wo_r, wc_r, wco_r, wg_r, wu_r,
                 x_ref, qkv_ref, pack_ref, tail_ref, tab_ref, hbuf, wqkv, qbuf, pbuf, tbuf, wsem, nsem, xsem, sem):
    st = Stage()
    weights = weights_of(st, (wq_r, wk_r, wv_r), 0, wqkv, wsem)
    coming = NextLayer(st, (wo_r, wc_r, wco_r), (wg_r, wu_r), 0, pack_ref, tail_ref, pbuf, tbuf, nsem, xsem)
    each(weights, "open_local")
    each(coming.loads, "start")
    st.greet()
    each(weights, "open_cross")
    each(coming.sends, "start")
    each(weights, "open_share")
    hidden = jnp.concatenate([first_ref[...], second_ref[...]], axis=0)
    x_ref[...] = hidden.astype(F32)
    res = st.trade_rows(hidden, hbuf, sem.at[0]).astype(F32)
    normed = rms(res, gain_ref[0:1, :])
    bias_table(bias_ref, tab_ref)
    coming.store()
    each(weights, "relay")
    each(weights, "finish")
    st.give_rows(dot32(normed, wqkv[...]), qbuf, sem.at[1], qkv_ref)
    coming.finish()


def both_blocks(act, packed, which):
    half = D // 2
    cols = slice(which * half, (which + 1) * half)
    return [dot32(act, packed[cb, :, cols]).astype(BF16) for cb in range(2)]


def layer_kernel(layer, last, seqs, len_ref, o_ref, x_ref, gcross_ref, gmlp_ref, *refs):
    if last:
        (ck, cv, pack_in, ypack_in, xtail_in, wg_r, wu_r, wd_r, hid_ref,
         kbuf, vbuf, wattn, wtail, wdown, qs, os, ubuf, kvsem, asem, wtsem, dsem, sem, sem2, rbuf, zbuf, zs) = refs
    else:
        (gself_ref, ck, cv, pack_in, ypack_in, xtail_in, wg_r, wu_r, wd_r, wq_r, wk_r, wv_r, wo_r, wc_r, wco_r,
         x_out, qkv_ref, pack_ref, tail_ref,
         kbuf, vbuf, wattn, wtail, wdown, qs, os, ubuf, kvsem, asem, wtsem, dsem, sem, sem2,
         rbuf, zbuf, wqkv, qkvbuf, pbuf, tbuf, wsem, nsem, xsem) = refs
    st = Stage()
    rows = o_ref.shape[0]
    attn = Whole(st, (pack_in, ypack_in), wattn, asem)
    tail = weights_of(st, (wg_r, wu_r), layer, wtail, wtsem, xtail_in)
    down = weights_of(st, (wd_r,), layer, wdown, dsem)
    attn.open_local()

    def caches(b):
        return [pltpu.make_async_copy(src.at[layer, b], buf.at[b], kvsem.at[n, b])
                for n, (src, buf) in enumerate(((ck, kbuf), (cv, vbuf)))]

    def fetch_caches(b, carry):
        each(caches(b), "start")
        return carry

    st.greet()
    attn.open_share()
    each(down, "open_cross")
    lax.fori_loop(0, seqs, fetch_caches, 0)
    each(tail, "open_local")
    each(down, "open_local")
    if not last:
        ahead = weights_of(st, (wq_r, wk_r, wv_r), layer + 1, wqkv, wsem)
        coming = NextLayer(st, (wo_r, wc_r, wco_r), (wg_r, wu_r), layer + 1, pack_ref, tail_ref, pbuf, tbuf,
                           nsem, xsem)
        each(ahead, "open_cross")
        each(coming.sends, "start")
        each(ahead, "open_local")
        each(coming.loads, "start")
    attn.finish(0)
    y = jnp.concatenate(both_blocks(o_ref[...].astype(BF16), wattn, 0), axis=1)
    res = x_ref[...] + y.astype(F32)
    attn.finish(1)
    for cb, q in enumerate(both_blocks(rms(res, gcross_ref[layer:layer + 1, :]), wattn, 1)):
        qs[cb] = q.astype(F32)
    each(tail, "open_share")
    each(down, "open_share")
    if not last:
        each(ahead, "open_share")
        coming.store()

    def cross_step(i, carry):
        hmask = head_mask()
        t_id = lax.broadcasted_iota(jnp.int32, (TOKENS * HROWS, kbuf.shape[-1]), 1)
        seqids = [i * SEQ_BLOCK + j for j in range(SEQ_BLOCK)]
        for b in seqids:
            each(caches(b), "wait")
        queries = [spread_query(qs, b, seqs, hmask) for b in seqids]
        scores = [dot32(q, kbuf[b]) for q, b in zip(queries, seqids)]
        parts = [jnp.where(t_id < len_ref[b], sc, NEG) for b, sc in zip(seqids, scores)]
        mix_values(softmax_rows(jnp.concatenate(parts, axis=0)), vbuf, seqids, hmask, os)
        return carry

    lax.fori_loop(0, seqs // SEQ_BLOCK, cross_step, 0)
    each(down, "relay")
    attn.finish(2)
    y = jnp.concatenate(both_blocks(os[...].reshape(rows, D).astype(BF16), wattn, 2), axis=1)
    res = res + y.astype(F32)
    gain = gmlp_ref[layer:layer + 1, :]
    ff = wtail.shape[1] // 2

    def gated(normed):
        gate = dot32(normed, wtail[:, 0:ff]).astype(BF16).astype(F32)
        up = dot32(normed, wtail[:, ff:2 * ff]).astype(BF16).astype(F32)
        return (gate * jax.nn.sigmoid(gate) * up).astype(BF16)

    normed = rms(res, gain)
    rbuf[0] = normed if last else res
    moving = st.send(rbuf.at[0], rbuf.at[1], sem.at[0])
    each(tail, "finish")
    ubuf[st.c, 0] = gated(normed)
    moving_own = st.send(ubuf.at[st.c, 0], ubuf.at[st.c, 1], sem2.at[0, 0])
    moving.wait()
    ubuf[st.c, 1] = gated(rbuf[1] if last else rms(rbuf[1], gain))
    moving_other = st.send(ubuf.at[st.c, 1], ubuf.at[st.c, 0], sem2.at[0, 1])
    if not last:
        res = jnp.concatenate([res, rbuf[1]], axis=0)
    moving_own.wait()
    moving_other.wait()
    act = jnp.concatenate([ubuf[0].reshape(2 * rows, ff), ubuf[1].reshape(2 * rows, ff)], axis=1)
    if not last:
        each(ahead, "relay")
    each(down, "finish")
    z = dot32(act, wdown[...])
    if last:
        st.give_rows(z, zbuf, sem.at[1], zs)
        hid_ref[...] = res + jnp.concatenate([zs[0], zs[1]], axis=1)
    else:
        res = res + st.trade_columns(z, zbuf, sem2.at[1]).astype(F32)
        x_out[...] = res[:rows]
        normed = rms(res, gself_ref[layer + 1:layer + 2, :])
        each(ahead, "finish")
        st.give_rows(dot32(normed, wqkv[...]), qkvbuf, sem.at[1], qkv_ref)
        coming.finish()


def exchange_call(kernel, cid, name, specs, args, outs, scratch, flops):
    spaces = {"s": pltpu.SMEM, "v": pltpu.VMEM, "h": pl.ANY}
    spec = lambda letters: [pl.BlockSpec(memory_space=spaces[x]) for x in letters]
    return pl.pallas_call(
        kernel,
        out_shape=tuple(t for _, t in outs),
        in_specs=spec(specs),
        out_specs=tuple(spec(x for x, _ in outs)),
        scratch_shapes=scratch,
        cost_estimate=pl.CostEstimate(flops=flops, bytes_accessed=8 << 20, transcendentals=0),
        compiler_params=pltpu.CompilerParams(collective_id=cid, has_side_effects=True, vmem_limit_bytes=VMEM_LIMIT),
        name=name,
    )(*args)


def solution(mesh):
    batch_axes = ('dp', 'col', 'row')

    def local_step(h_first, h_second, start_pos, enc_lens, dec_bias, norm_self, norm_cross, norm_mlp,
                   w_query, w_key, w_value, w_out, w_cquery, w_cout, w_gate, w_up, w_down,
                   self_k, self_v, cross_k, cross_v):
        layers, seqs, cache_len = self_k.shape[:3]
        rows = TOKENS * seqs
        half = D // 2
        ffc = w_gate.shape[2]
        depth = 4 * w_query.shape[1]
        fdepth = 4 * w_down.shape[1]

        def flat(cache):
            return jnp.transpose(cache, (0, 1, 3, 4, 2)).reshape(layers, seqs, D, cache.shape[2])

        caches = [flat(a) for a in (self_k, self_v, cross_k, cross_v)]
        block = w_query.shape[1]

        vm = lambda shape, dt=BF16: pltpu.VMEM(shape, dt)
        dma = lambda *shape: pltpu.SemaphoreType.DMA(shape)
        rowbuf = lambda width, dt=BF16: vm((2, rows, width), dt)
        colbuf = lambda width: vm((2, 2, rows, width))
        res_t = ("v", jax.ShapeDtypeStruct((rows, D), F32))
        qkv_t = ("v", jax.ShapeDtypeStruct((2, rows, 3 * half), F32))
        pack_t = ("h", jax.ShapeDtypeStruct((2, block, 3 * half), BF16))
        tail_t = ("h", jax.ShapeDtypeStruct((block, 2 * ffc), BF16))
        coming = [vm((block, 3 * half)), vm((block, 2 * ffc))]
        across = [(r, (r + 2) % 4) for r in range(4)]
        flip = [(0, 1), (1, 0)]

        table_t = ("v", jax.ShapeDtypeStruct((HROWS, cache_len), F32))
        res, qkv, pack, tail_own, table = exchange_call(
            start_kernel, 0, "start", "vvvv" + "h" * 8,
            [h_first, h_second, norm_self, dec_bias.T, w_query, w_key, w_value, w_out, w_cquery, w_cout, w_gate, w_up],
            [res_t, qkv_t, pack_t, tail_t, table_t],
            [rowbuf(D), vm((depth, 3 * half)), rowbuf(3 * half)] + coming
            + [dma(3, 7), dma(3, 3), dma(3, 2), dma(2, 2)], 3_000_000_000)
        outs = None
        for l in range(layers):
            last = l == layers - 1
            ypack = lax.ppermute(pack, "col", flip)
            xtail = lax.ppermute(tail_own, "row", across)
            k_out, v_out, mixed = self_attention(l, start_pos, qkv, table, caches[0], caches[1], outs)
            outs = (k_out, v_out)
            cache_buf = vm((seqs, D, cross_k.shape[2]))
            scratch = [cache_buf, cache_buf, vm((2, depth, 3 * half)), vm((depth, 2 * ffc)), vm((fdepth, half)),
                       vm((2, rows, half), F32), vm((TOKENS, seqs, D), F32), colbuf(ffc),
                       dma(2, seqs), dma(3, 2, 2, 3), dma(2, 7), dma(1, 7), dma(2, 2), dma(2, 2, 2)]
            args = [enc_lens, mixed.reshape(rows, D), res, norm_cross, norm_mlp]
            weights = [caches[2], caches[3], pack, ypack, xtail, w_gate, w_up, w_down]
            if last:
                hid, = exchange_call(
                    functools.partial(layer_kernel, l, True, seqs), 1 + l, "last", "svvvv" + "h" * 8,
                    args + weights, [res_t],
                    scratch + [rowbuf(D), rowbuf(half), vm((2, rows, half), F32)], 20_000_000_000)
            else:
                scratch += [rowbuf(D, F32), colbuf(half), vm((depth, 3 * half)), rowbuf(3 * half)] + coming
                scratch += [dma(3, 7), dma(3, 3), dma(3, 2)]
                res, qkv, pack, tail_own = exchange_call(
                    functools.partial(layer_kernel, l, False, seqs), 1 + l, "layer", "svvvvv" + "h" * 14,
                    args + [norm_self] + weights
                    + [w_query, w_key, w_value, w_out, w_cquery, w_cout],
                    [res_t, qkv_t, pack_t, tail_t], scratch, 20_000_000_000)

        def unflat(cache):
            return jnp.transpose(cache.reshape(layers, seqs, HEADS, HEAD_DIM, cache_len), (0, 1, 4, 2, 3))

        return hid.reshape(TOKENS, seqs, D).astype(BF16), unflat(outs[0]), unflat(outs[1])

    row_spec = P(batch_axes, None)
    seq_spec = P(batch_axes)
    weight_spec = P(None, 'row', 'col')
    cache_spec = P(None, batch_axes)
    in_specs = (row_spec, row_spec, seq_spec, seq_spec, P(), P(), P(), P()) + (weight_spec,) * 9 + (cache_spec,) * 4
    out_specs = (P(None, batch_axes), cache_spec, cache_spec)
    return jax.shard_map(local_step, mesh=mesh, in_specs=in_specs, out_specs=out_specs, check_vma=False)
```

```python
import functools

import jax
import jax.numpy as jnp
from jax import lax
from jax.experimental import pallas as pl
from jax.experimental.pallas import tpu as pltpu
from jax.sharding import PartitionSpec as P

NORM_EPS = 1e-6
BUCKET_EDGES = (16, 19, 21, 24, 27, 31, 35, 40, 46, 52, 59, 67, 77, 87, 99, 113)
HEADS = 12
HEAD_DIM = 64
D = HEADS * HEAD_DIM
TOKENS = 2
LANES = 128
HROWS = 16
NEG = -1e30
SEQ_BLOCK = 4
AHEAD = 8
MESH = pl.DeviceIdType.MESH
F32 = jnp.float32
BF16 = jnp.bfloat16
VMEM_LIMIT = 67_043_328


def dot32(a, b):
    return jnp.dot(a, b, preferred_element_type=F32)


def head_mask():
    row = lax.broadcasted_iota(jnp.int32, (HROWS, D), 0)
    col = lax.broadcasted_iota(jnp.int32, (HROWS, D), 1)
    return (col >= row * HEAD_DIM) & (col < (row + 1) * HEAD_DIM)


def spread_query(q_ref, b, seqs, hmask):
    rows = []
    for s in range(TOKENS):
        at = pl.ds(s * seqs + b, 1)
        row = jnp.concatenate([q_ref[0, at, 0:D // 2], q_ref[1, at, 0:D // 2]], axis=1)
        rows.append(jnp.where(hmask, jnp.broadcast_to(row, (HROWS, D)), 0.0))
    return jnp.concatenate(rows, axis=0).astype(BF16)


def softmax_rows(sc):
    top = jnp.max(sc, axis=1, keepdims=True)
    e = jnp.exp(sc - top)
    return (e / jnp.sum(e, axis=1, keepdims=True)).astype(BF16)


def mix_values(probs, values, seqids, hmask, o_ref):
    group = TOKENS * HROWS
    mixes = [lax.dot_general(probs[n * group:(n + 1) * group], values[b], (((1,), (1,)), ((), ())),
                             preferred_element_type=F32) for n, b in enumerate(seqids)]
    for b, mixed in zip(seqids, mixes):
        for s in range(TOKENS):
            part = jnp.where(hmask, mixed[s * HROWS:(s + 1) * HROWS], 0.0)
            row = jnp.sum(part, axis=0, keepdims=True)
            o_ref[s, pl.ds(b, 1), :] = row.astype(BF16).astype(F32)


def self_kernel(layer, seqs, aliased, pos_ref, qkv_ref, tab_ref, k_in, v_in, *rest):
    k_out, v_out, o_ref, kbuf, vbuf, kvt, in_sem, out_sem = rest[2 if aliased else 0:]
    half = D // 2
    cache_len = kbuf.shape[-1]
    sides = ((0, k_in, k_out, kbuf), (1, v_in, v_out, vbuf))

    def loads(b):
        return [pltpu.make_async_copy(src.at[layer, b], buf.at[b], in_sem.at[n, b]) for n, src, _, buf in sides]

    def stores(b):
        return [pltpu.make_async_copy(buf.at[b], dst.at[layer, b], out_sem.at[n, b]) for n, _, dst, buf in sides]

    for b in range(AHEAD):
        for copy in loads(b):
            copy.start()
    for which in range(2):
        for cb in range(2):
            lo = (which + 1) * half
            kvt[which, pl.ds(cb * half, half), :] = qkv_ref[cb, :, lo:lo + half].T.astype(BF16)

    def step(i, carry):
        hmask = head_mask()
        wide = 2 * LANES
        row_id = lax.broadcasted_iota(jnp.int32, (TOKENS * seqs, wide), 0)
        lane_id = lax.broadcasted_iota(jnp.int32, (TOKENS * seqs, wide), 1)
        lane_row = lax.broadcasted_iota(jnp.int32, (D, wide), 1)
        t_id = lax.broadcasted_iota(jnp.int32, (HROWS, cache_len), 1)
        seqids = [i * SEQ_BLOCK + j for j in range(SEQ_BLOCK)]
        for b in seqids:
            ahead = b + AHEAD

            @pl.when(ahead < seqs)
            def _():
                for copy in loads(ahead):
                    copy.start()
        for b in seqids:
            for copy in loads(b):
                copy.wait()
        for b in seqids:
            p = pos_ref[b]
            off = pl.multiple_of(jnp.minimum(p // LANES, cache_len // LANES - 2) * LANES, LANES)
            lane = p - off
            sel = ((row_id == b) & (lane_id == lane)) | ((row_id == seqs + b) & (lane_id == lane + 1))
            sel = jnp.where(sel, 1.0, 0.0).astype(BF16)
            here = (lane_row == lane) | (lane_row == lane + 1)
            for n, _, _, buf in sides:
                ins = dot32(kvt[n], sel)
                old = buf[b, :, pl.ds(off, wide)].astype(F32)
                buf[b, :, pl.ds(off, wide)] = jnp.where(here, ins, old).astype(BF16)
            for copy in stores(b):
                copy.start()
        queries = [spread_query(qkv_ref, b, seqs, hmask) for b in seqids]
        scores = [dot32(q, kbuf[b]) for q, b in zip(queries, seqids)]
        parts = []
        for b, sc in zip(seqids, scores):
            for s in range(TOKENS):
                t = pos_ref[b] + s
                bias = pltpu.roll(tab_ref[...], lax.rem(t + 1, cache_len), 1)
                parts.append(jnp.where(t_id <= t, sc[s * HROWS:(s + 1) * HROWS] + bias, NEG))
        mix_values(softmax_rows(jnp.concatenate(parts, axis=0)), vbuf, seqids, hmask, o_ref)
        return carry

    lax.fori_loop(0, seqs // SEQ_BLOCK, step, 0)
    for b in range(seqs):
        for copy in stores(b):
            copy.wait()


def self_attention(layer, pos, qkv, table, cache_k, cache_v, outs):
    layers, seqs, _, cache_len = cache_k.shape
    vm = pl.BlockSpec(memory_space=pltpu.VMEM)
    hb = pl.BlockSpec(memory_space=pl.ANY)
    in_specs = [pl.BlockSpec(memory_space=pltpu.SMEM), vm, vm, hb, hb]
    args = [pos, qkv, table, cache_k, cache_v]
    aliases = {}
    if outs is not None:
        in_specs += [hb, hb]
        args += list(outs)
        aliases = {5: 0, 6: 1}
    buf = pltpu.VMEM((seqs, D, cache_len), BF16)
    return pl.pallas_call(
        functools.partial(self_kernel, layer, seqs, outs is not None),
        out_shape=(jax.ShapeDtypeStruct(cache_k.shape, BF16), jax.ShapeDtypeStruct(cache_v.shape, BF16),
                   jax.ShapeDtypeStruct((TOKENS, seqs, D), F32)),
        in_specs=in_specs,
        out_specs=[hb, hb, vm],
        scratch_shapes=[buf, buf, pltpu.VMEM((2, D, TOKENS * seqs), BF16),
                        pltpu.SemaphoreType.DMA((2, seqs)), pltpu.SemaphoreType.DMA((2, seqs))],
        input_output_aliases=aliases,
        cost_estimate=pl.CostEstimate(flops=20_000_000_000, bytes_accessed=4 * seqs * D * cache_len * 2,
                                      transcendentals=0),
        compiler_params=pltpu.CompilerParams(vmem_limit_bytes=VMEM_LIMIT),
        name="self_attn",
    )(*args)


def rms(res, gain):
    mean_sq = jnp.mean(res * res, axis=-1, keepdims=True)
    return (res * lax.rsqrt(mean_sq + NORM_EPS) * gain.astype(F32)).astype(BF16)


class Stage:
    def __init__(self):
        dp, self.c, self.r = lax.axis_index("dp"), lax.axis_index("col"), lax.axis_index("row")
        self.across = (self.r + 2) % 4
        core = self.r + 1 - 2 * (self.r % 2)
        self.peer = (dp, 1 - self.c, self.r)
        self.partner = (dp, self.c, core)
        self.xpeer = (dp, self.c, self.across)

    def greet(self):
        barrier = pltpu.get_barrier_semaphore()
        for other in (self.peer, self.partner, self.xpeer):
            pl.semaphore_signal(barrier, inc=1, device_id=other, device_id_type=MESH)
        pl.semaphore_wait(barrier, 3)

    def remote(self, src, dst, send_sem, recv_sem, to):
        return pltpu.make_async_remote_copy(src_ref=src, dst_ref=dst, send_sem=send_sem, recv_sem=recv_sem,
                                            device_id=to, device_id_type=MESH)

    def send(self, src, dst, sems):
        copy = self.remote(src, dst, sems.at[0], sems.at[1], self.peer)
        copy.start()
        return copy

    def trade_rows(self, own, buf, sems):
        buf[0] = own
        self.send(buf.at[0], buf.at[1], sems).wait()
        return jnp.concatenate([buf[0], buf[1]], axis=0)

    def trade_columns(self, mine, buf, sems):
        rows, width = mine.shape[0] // 2, mine.shape[1]
        c = self.c
        buf[c] = mine.astype(BF16).reshape(2, rows, width)
        first = self.send(buf.at[c, 0], buf.at[c, 1], sems.at[0])
        second = self.send(buf.at[c, 1], buf.at[c, 0], sems.at[1])
        first.wait()
        second.wait()
        return jnp.concatenate([buf[0].reshape(2 * rows, width), buf[1].reshape(2 * rows, width)], axis=1)

    def give_rows(self, mine, buf, sems, out_ref):
        rows = mine.shape[0] // 2
        c = self.c
        mine = mine.astype(BF16)
        buf[0] = mine[rows:]
        copy = self.send(buf.at[0], buf.at[1], sems)
        out_ref[c] = mine[:rows].astype(F32)
        copy.wait()
        out_ref[1 - c] = buf[1].astype(F32)


class Weight:
    def __init__(self, st, own, dst, col, sems, crossed=None):
        depth, width = own.shape
        self.st, self.crossed = st, crossed

        def place(owner):
            return dst.at[pl.ds(pl.multiple_of(owner * depth, depth), depth), pl.ds(col, width)]

        mine, theirs = place(st.r), place(st.across)
        self.local = pltpu.make_async_copy(own, mine, sems.at[0])
        self.share = st.remote(own, mine, sems.at[1], sems.at[2], st.partner)
        if crossed is None:
            self.cross = st.remote(own, mine, sems.at[3], sems.at[4], st.xpeer)
            self.pass_on = st.remote(theirs, theirs, sems.at[5], sems.at[6], st.partner)
        else:
            self.cross = pltpu.make_async_copy(crossed, theirs, sems.at[3])
            self.pass_on = st.remote(crossed, theirs, sems.at[5], sems.at[6], st.partner)

    def open_local(self):
        self.local.start()
        if self.crossed is not None:
            self.cross.start()

    def open_cross(self):
        if self.crossed is None:
            self.cross.start()

    def open_share(self):
        self.share.start()
        if self.crossed is not None:
            self.pass_on.start()

    def relay(self):
        if self.crossed is None:
            self.cross.wait_recv()
            self.pass_on.start()

    def finish(self):
        self.local.wait()
        self.share.wait()
        if self.crossed is None:
            self.cross.wait_send()
        else:
            self.cross.wait()
        self.pass_on.wait()


def each(items, name):
    for item in items:
        getattr(item, name)()


def weights_of(st, refs, layer, dst, sems, crossed=None):
    col, found = 0, []
    for n, ref in enumerate(refs):
        width = ref.shape[2]
        given = None if crossed is None else crossed.at[:, pl.ds(col, width)]
        found.append(Weight(st, ref.at[layer], dst, col, sems.at[n], given))
        col += width
    return found


def forward(st, refs, layer, dst, sems):
    col, copies = 0, []
    for n, ref in enumerate(refs):
        width = ref.shape[2]
        copies.append(st.remote(ref.at[layer], dst.at[:, pl.ds(col, width)], sems.at[n, 0], sems.at[n, 1], st.xpeer))
        col += width
    return copies


def collect(refs, layer, dst, sems):
    col, copies = 0, []
    for n, ref in enumerate(refs):
        width = ref.shape[2]
        copies.append(pltpu.make_async_copy(ref.at[layer], dst.at[:, pl.ds(col, width)], sems.at[n]))
        col += width
    return copies


class Second:
    def __init__(self, st, own, crossed, dst, sems):
        depth = own.shape[0]
        self.sends, self.relays = [], []
        for n, (src, owner) in enumerate(((own, st.r), (crossed, st.across))):
            at = pl.ds(pl.multiple_of(owner * depth, depth), depth)
            theirs, mine = dst.at[st.c, at, :], dst.at[1 - st.c, at, :]
            self.sends.append(st.remote(src, theirs, sems.at[n, 0], sems.at[n, 1], st.peer))
            self.relays.append(st.remote(mine, mine, sems.at[n, 2], sems.at[n, 3], st.partner))

    def relay(self):
        for send, relay in zip(self.sends, self.relays):
            send.wait_recv()
            relay.start()

    def finish(self):
        for send, relay in zip(self.sends, self.relays):
            send.wait_send()
            relay.wait()


class NextLayer:
    def __init__(self, st, mid, tail, layer, mid_ref, tail_ref, tbuf, sems, xsems):
        self.loads = collect(tail, layer, tbuf, sems)
        self.sends = forward(st, mid, layer, mid_ref, xsems)
        self.out = pltpu.make_async_copy(tbuf, tail_ref, sems.at[len(tail)])

    def store(self):
        each(self.loads, "wait")
        self.out.start()

    def finish(self):
        self.out.wait()
        each(self.sends, "wait")


def bias_table(bias_ref, tab_ref):
    buckets, length = bias_ref.shape[1], tab_ref.shape[1]
    dist = length - 1 - lax.broadcasted_iota(jnp.int32, (buckets, length), 1)
    far = jnp.full((buckets, length), BUCKET_EDGES[0] - 1, jnp.int32)
    for edge in BUCKET_EDGES:
        far = far + jnp.where(dist >= edge, 1, 0)
    bucket = jnp.where(dist < BUCKET_EDGES[0], dist, far)
    pick = jnp.where(bucket == lax.broadcasted_iota(jnp.int32, (buckets, length), 0), 1.0, 0.0).astype(BF16)
    left = jnp.concatenate([bias_ref[...], jnp.zeros((HROWS - bias_ref.shape[0], buckets), F32)], axis=0)
    total = jnp.zeros((HROWS, length), F32)
    for _ in range(3):
        part = left.astype(BF16)
        total = total + dot32(part, pick)
        left = left - part.astype(F32)
    tab_ref[...] = total


def start_kernel(first_ref, second_ref, gain_ref, bias_ref, wq_r, wk_r, wv_r, wo_r, wc_r, wco_r, wg_r, wu_r,
                 x_ref, qkv_ref, mid_ref, tail_ref, tab_ref, hbuf, wqkv, qbuf, tbuf, wsem, nsem, xsem, sem):
    st = Stage()
    weights = weights_of(st, (wq_r, wk_r, wv_r), 0, wqkv, wsem)
    coming = NextLayer(st, (wo_r, wc_r), (wco_r, wg_r, wu_r), 0, mid_ref, tail_ref, tbuf, nsem, xsem)
    each(weights, "open_local")
    each(coming.loads, "start")
    st.greet()
    each(weights, "open_cross")
    each(coming.sends, "start")
    each(weights, "open_share")
    hidden = jnp.concatenate([first_ref[...], second_ref[...]], axis=0)
    res = st.trade_rows(hidden, hbuf, sem.at[0]).astype(F32)
    x_ref[...] = res
    normed = rms(res, gain_ref[0:1, :])
    bias_table(bias_ref, tab_ref)
    coming.store()
    each(weights, "relay")
    each(weights, "finish")
    st.give_rows(dot32(normed, wqkv[...]), qbuf, sem.at[1], qkv_ref)
    coming.finish()


def layer_kernel(layer, last, seqs, len_ref, o_ref, x_ref, gcross_ref, gmlp_ref, *refs):
    if not last:
        gself_ref, refs = refs[0], refs[1:]
    ck, cv, mid_in, tail_in, wo_r, wc_r, wco_r, wg_r, wu_r, wd_r = refs[:10]
    refs = refs[10:]
    if last:
        hid_ref, refs = refs[0], refs[1:]
    else:
        wq_r, wk_r, wv_r, x_out, qkv_ref, mid_ref, tail_ref = refs[:7]
        refs = refs[7:]
    (kbuf, vbuf, wmid, wco, wtail, wdown, qs, os, obuf, ybuf, qbuf, ubuf,
     kvsem, msem, csem, c2sem, gsem, dsem, sem, sem2, rbuf, zbuf) = refs[:22]
    refs = refs[22:]
    st = Stage()
    rows, half = o_ref.shape[0], D // 2
    ff = wg_r.shape[2]
    co_x, gate_x = tail_in.at[:, pl.ds(0, half)], tail_in.at[:, pl.ds(half, 2 * ff)]
    mid = weights_of(st, (wo_r, wc_r), layer, wmid, msem, mid_in)
    co = weights_of(st, (wco_r,), layer, wco.at[st.c], csem, co_x)
    co_second = Second(st, wco_r.at[layer], co_x, wco, c2sem)
    tail = weights_of(st, (wg_r, wu_r), layer, wtail, gsem, gate_x)
    down = weights_of(st, (wd_r,), layer, wdown, dsem)
    each(mid, "open_local")

    def caches(b):
        return [pltpu.make_async_copy(src.at[layer, b], buf.at[b], kvsem.at[n, b])
                for n, (src, buf) in enumerate(((ck, kbuf), (cv, vbuf)))]

    def fetch_caches(b, carry):
        each(caches(b), "start")
        return carry

    obuf[0] = o_ref[...].astype(BF16)
    st.greet()
    moving = st.send(obuf.at[0], obuf.at[1], sem.at[2])
    each(mid, "open_share")
    co_second.sends[0].start()
    each(down, "open_cross")
    lax.fori_loop(0, seqs, fetch_caches, 0)
    each(co, "open_local")
    each(tail, "open_local")
    each(down, "open_local")
    if not last:
        wqkv, qkvbuf, tbuf, wsem, nsem, xsem = refs
        ahead = weights_of(st, (wq_r, wk_r, wv_r), layer + 1, wqkv, wsem)
        coming = NextLayer(st, (wo_r, wc_r), (wco_r, wg_r, wu_r), layer + 1, mid_ref, tail_ref, tbuf, nsem, xsem)
        each(ahead, "open_cross")
        each(coming.sends, "start")
        each(ahead, "open_local")
        each(coming.loads, "start")
    moving.wait()
    each(mid, "finish")
    mixed = jnp.concatenate([obuf[0], obuf[1]], axis=0)
    y = dot32(mixed, wmid[:, 0:half]).astype(BF16)
    ybuf[st.c] = y.reshape(2, rows, half)
    moving = st.send(ybuf.at[st.c, 1], ybuf.at[st.c, 0], sem2.at[2, 0])
    moving_own = st.send(ybuf.at[st.c, 0], ybuf.at[st.c, 1], sem2.at[2, 1])
    co_second.sends[1].start()
    each(co, "open_share")
    moving.wait()
    moving_own.wait()
    y = jnp.concatenate([ybuf[0].reshape(2 * rows, half), ybuf[1].reshape(2 * rows, half)], axis=1)
    res = x_ref[...] + y.astype(F32)
    st.give_rows(dot32(rms(res, gcross_ref[layer:layer + 1, :]), wmid[:, half:D]), qbuf, sem.at[3], qs)
    co_second.relay()
    each(tail, "open_share")
    each(down, "open_share")
    if not last:
        each(ahead, "open_share")
        coming.store()

    def cross_step(i, carry):
        hmask = head_mask()
        t_id = lax.broadcasted_iota(jnp.int32, (TOKENS * HROWS, kbuf.shape[-1]), 1)
        seqids = [i * SEQ_BLOCK + j for j in range(SEQ_BLOCK)]
        for b in seqids:
            each(caches(b), "wait")
        queries = [spread_query(qs, b, seqs, hmask) for b in seqids]
        scores = [dot32(q, kbuf[b]) for q, b in zip(queries, seqids)]
        parts = [jnp.where(t_id < len_ref[b], sc, NEG) for b, sc in zip(seqids, scores)]
        mix_values(softmax_rows(jnp.concatenate(parts, axis=0)), vbuf, seqids, hmask, os)
        return carry

    lax.fori_loop(0, seqs // SEQ_BLOCK, cross_step, 0)
    each(down, "relay")
    each(co, "finish")
    co_second.finish()
    mixed = os[...].reshape(rows, D).astype(BF16)
    y = jnp.concatenate([dot32(mixed, wco[0]), dot32(mixed, wco[1])], axis=1).astype(BF16)
    rbuf[0] = y
    moving = st.send(rbuf.at[0], rbuf.at[1], sem.at[0])
    gain = gmlp_ref[layer:layer + 1, :]

    def gated(normed):
        gate = dot32(normed, wtail[:, 0:ff]).astype(BF16).astype(F32)
        up = dot32(normed, wtail[:, ff:2 * ff]).astype(BF16).astype(F32)
        return (gate * jax.nn.sigmoid(gate) * up).astype(BF16)

    res_own = res[:rows] + y.astype(F32)
    each(tail, "finish")
    ubuf[st.c, 0] = gated(rms(res_own, gain))
    moving_own = st.send(ubuf.at[st.c, 0], ubuf.at[st.c, 1], sem2.at[0, 0])
    moving.wait()
    res_other = res[rows:] + rbuf[1].astype(F32)
    ubuf[st.c, 1] = gated(rms(res_other, gain))
    moving_other = st.send(ubuf.at[st.c, 1], ubuf.at[st.c, 0], sem2.at[0, 1])
    moving_own.wait()
    moving_other.wait()
    act = jnp.concatenate([ubuf[0].reshape(2 * rows, ff), ubuf[1].reshape(2 * rows, ff)], axis=1)
    if not last:
        each(ahead, "relay")
    each(down, "finish")
    z = dot32(act, wdown[...])
    if last:
        zs, = refs
        st.give_rows(z, zbuf, sem.at[1], zs)
        hid_ref[...] = res_own + jnp.concatenate([zs[0], zs[1]], axis=1)
    else:
        res = jnp.concatenate([res_own, res_other], axis=0) + st.trade_columns(z, zbuf, sem2.at[1]).astype(F32)
        x_out[...] = res
        normed = rms(res, gself_ref[layer + 1:layer + 2, :])
        each(ahead, "finish")
        st.give_rows(dot32(normed, wqkv[...]), qkvbuf, sem.at[1], qkv_ref)
        coming.finish()


def exchange_call(kernel, cid, name, specs, args, outs, scratch, flops):
    spaces = {"s": pltpu.SMEM, "v": pltpu.VMEM, "h": pl.ANY}
    spec = lambda letters: [pl.BlockSpec(memory_space=spaces[x]) for x in letters]
    return pl.pallas_call(
        kernel,
        out_shape=tuple(t for _, t in outs),
        in_specs=spec(specs),
        out_specs=tuple(spec(x for x, _ in outs)),
        scratch_shapes=scratch,
        cost_estimate=pl.CostEstimate(flops=flops, bytes_accessed=8 << 20, transcendentals=0),
        compiler_params=pltpu.CompilerParams(collective_id=cid, has_side_effects=True, vmem_limit_bytes=VMEM_LIMIT),
        name=name,
    )(*args)


def solution(mesh):
    batch_axes = ('dp', 'col', 'row')

    def local_step(h_first, h_second, start_pos, enc_lens, dec_bias, norm_self, norm_cross, norm_mlp,
                   w_query, w_key, w_value, w_out, w_cquery, w_cout, w_gate, w_up, w_down,
                   self_k, self_v, cross_k, cross_v):
        layers, seqs, cache_len = self_k.shape[:3]
        rows = TOKENS * seqs
        half = D // 2
        ffc = w_gate.shape[2]
        depth = 4 * w_query.shape[1]
        fdepth = 4 * w_down.shape[1]

        def flat(cache):
            return jnp.transpose(cache, (0, 1, 3, 4, 2)).reshape(layers, seqs, D, cache.shape[2])

        caches = [flat(a) for a in (self_k, self_v, cross_k, cross_v)]
        block = w_query.shape[1]

        vm = lambda shape, dt=BF16: pltpu.VMEM(shape, dt)
        dma = lambda *shape: pltpu.SemaphoreType.DMA(shape)
        rowbuf = lambda width, dt=BF16: vm((2, rows, width), dt)
        colbuf = lambda width: vm((2, 2, rows, width))
        res_t = ("v", jax.ShapeDtypeStruct((2 * rows, D), F32))
        hid_t = ("v", jax.ShapeDtypeStruct((rows, D), F32))
        qkv_t = ("v", jax.ShapeDtypeStruct((2, rows, 3 * half), F32))
        mid_t = ("h", jax.ShapeDtypeStruct((block, D), BF16))
        tail_t = ("h", jax.ShapeDtypeStruct((block, half + 2 * ffc), BF16))
        coming = [vm((block, half + 2 * ffc))]
        across = [(r, (r + 2) % 4) for r in range(4)]

        table_t = ("v", jax.ShapeDtypeStruct((HROWS, cache_len), F32))
        res, qkv, mid, tail_own, table = exchange_call(
            start_kernel, 0, "start", "vvvv" + "h" * 8,
            [h_first, h_second, norm_self, dec_bias.T, w_query, w_key, w_value, w_out, w_cquery, w_cout, w_gate, w_up],
            [res_t, qkv_t, mid_t, tail_t, table_t],
            [rowbuf(D), vm((depth, 3 * half)), rowbuf(3 * half)] + coming
            + [dma(3, 7), dma(4), dma(2, 2), dma(2, 2)], 3_000_000_000)
        outs = None
        for l in range(layers):
            last = l == layers - 1
            xtail = lax.ppermute(tail_own, "row", across)
            k_out, v_out, mixed = self_attention(l, start_pos, qkv, table, caches[0], caches[1], outs)
            outs = (k_out, v_out)
            cache_buf = vm((seqs, D, cross_k.shape[2]))
            scratch = [cache_buf, cache_buf, vm((depth, D)), vm((2, depth, half)), vm((depth, 2 * ffc)),
                       vm((fdepth, half)), vm((2, rows, half), F32), vm((TOKENS, seqs, D), F32),
                       rowbuf(D), colbuf(half), rowbuf(half), colbuf(ffc),
                       dma(2, seqs), dma(2, 7), dma(1, 7), dma(2, 4), dma(2, 7), dma(1, 7), dma(4, 2), dma(3, 2, 2)]
            args = [enc_lens, mixed.reshape(rows, D), res, norm_cross, norm_mlp]
            weights = [caches[2], caches[3], mid, xtail, w_out, w_cquery, w_cout, w_gate, w_up, w_down]
            if last:
                hid, = exchange_call(
                    functools.partial(layer_kernel, l, True, seqs), 1 + l, "last", "svvvv" + "h" * 10,
                    args + weights, [hid_t],
                    scratch + [rowbuf(D), rowbuf(half), vm((2, rows, half), F32)], 20_000_000_000)
            else:
                scratch += [rowbuf(D), colbuf(half), vm((depth, 3 * half)), rowbuf(3 * half)] + coming
                scratch += [dma(3, 7), dma(4), dma(2, 2)]
                res, qkv, mid, tail_own = exchange_call(
                    functools.partial(layer_kernel, l, False, seqs), 1 + l, "layer", "svvvvv" + "h" * 13,
                    args + [norm_self] + weights + [w_query, w_key, w_value],
                    [res_t, qkv_t, mid_t, tail_t], scratch, 20_000_000_000)

        def unflat(cache):
            return jnp.transpose(cache.reshape(layers, seqs, HEADS, HEAD_DIM, cache_len), (0, 1, 4, 2, 3))

        return hid.reshape(TOKENS, seqs, D).astype(BF16), unflat(outs[0]), unflat(outs[1])

    row_spec = P(batch_axes, None)
    seq_spec = P(batch_axes)
    weight_spec = P(None, 'row', 'col')
    cache_spec = P(None, batch_axes)
    in_specs = (row_spec, row_spec, seq_spec, seq_spec, P(), P(), P(), P()) + (weight_spec,) * 9 + (cache_spec,) * 4
    out_specs = (P(None, batch_axes), cache_spec, cache_spec)
    return jax.shard_map(local_step, mesh=mesh, in_specs=in_specs, out_specs=out_specs, check_vma=False)
```

```python
import functools

import jax
import jax.numpy as jnp
from jax import lax
from jax.experimental import pallas as pl
from jax.experimental.pallas import tpu as pltpu
from jax.sharding import PartitionSpec as P

NORM_EPS = 1e-6
BUCKET_EDGES = (16, 19, 21, 24, 27, 31, 35, 40, 46, 52, 59, 67, 77, 87, 99, 113)
HEADS = 12
HEAD_DIM = 64
D = HEADS * HEAD_DIM
TOKENS = 2
LANES = 128
HROWS = 16
NEG = -1e30
SEQ_BLOCK = 4
AHEAD = 8
MESH = pl.DeviceIdType.MESH
F32 = jnp.float32
BF16 = jnp.bfloat16
VMEM_LIMIT = 67_043_328


def dot32(a, b):
    return jnp.dot(a, b, preferred_element_type=F32)


def head_mask():
    row = lax.broadcasted_iota(jnp.int32, (HROWS, D), 0)
    col = lax.broadcasted_iota(jnp.int32, (HROWS, D), 1)
    return (col >= row * HEAD_DIM) & (col < (row + 1) * HEAD_DIM)


def spread_query(q_ref, b, seqs, hmask):
    rows = []
    for s in range(TOKENS):
        at = pl.ds(s * seqs + b, 1)
        row = jnp.concatenate([q_ref[0, at, 0:D // 2], q_ref[1, at, 0:D // 2]], axis=1)
        rows.append(jnp.where(hmask, jnp.broadcast_to(row, (HROWS, D)), 0.0))
    return jnp.concatenate(rows, axis=0).astype(BF16)


def softmax_rows(sc):
    top = jnp.max(sc, axis=1, keepdims=True)
    e = jnp.exp(sc - top)
    return (e / jnp.sum(e, axis=1, keepdims=True)).astype(BF16)


def mix_values(probs, values, seqids, hmask, o_ref):
    group = TOKENS * HROWS
    mixes = [lax.dot_general(probs[n * group:(n + 1) * group], values[b], (((1,), (1,)), ((), ())),
                             preferred_element_type=F32) for n, b in enumerate(seqids)]
    for b, mixed in zip(seqids, mixes):
        for s in range(TOKENS):
            part = jnp.where(hmask, mixed[s * HROWS:(s + 1) * HROWS], 0.0)
            row = jnp.sum(part, axis=0, keepdims=True)
            o_ref[s, pl.ds(b, 1), :] = row.astype(BF16).astype(F32)


def self_kernel(layer, seqs, aliased, pos_ref, qkv_ref, tab_ref, k_in, v_in, *rest):
    k_out, v_out, o_ref, kbuf, vbuf, kvt, in_sem, out_sem = rest[2 if aliased else 0:]
    half = D // 2
    cache_len = kbuf.shape[-1]
    sides = ((0, k_in, k_out, kbuf), (1, v_in, v_out, vbuf))

    def loads(b):
        return [pltpu.make_async_copy(src.at[layer, b], buf.at[b], in_sem.at[n, b]) for n, src, _, buf in sides]

    def stores(b):
        return [pltpu.make_async_copy(buf.at[b], dst.at[layer, b], out_sem.at[n, b]) for n, _, dst, buf in sides]

    for b in range(AHEAD):
        for copy in loads(b):
            copy.start()
    for which in range(2):
        for cb in range(2):
            lo = (which + 1) * half
            kvt[which, pl.ds(cb * half, half), :] = qkv_ref[cb, :, lo:lo + half].T.astype(BF16)

    def step(i, carry):
        hmask = head_mask()
        wide = 2 * LANES
        row_id = lax.broadcasted_iota(jnp.int32, (TOKENS * seqs, wide), 0)
        lane_id = lax.broadcasted_iota(jnp.int32, (TOKENS * seqs, wide), 1)
        lane_row = lax.broadcasted_iota(jnp.int32, (D, wide), 1)
        t_id = lax.broadcasted_iota(jnp.int32, (HROWS, cache_len), 1)
        seqids = [i * SEQ_BLOCK + j for j in range(SEQ_BLOCK)]
        for b in seqids:
            ahead = b + AHEAD

            @pl.when(ahead < seqs)
            def _():
                for copy in loads(ahead):
                    copy.start()
        for b in seqids:
            for copy in loads(b):
                copy.wait()
        for b in seqids:
            p = pos_ref[b]
            off = pl.multiple_of(jnp.minimum(p // LANES, cache_len // LANES - 2) * LANES, LANES)
            lane = p - off
            sel = ((row_id == b) & (lane_id == lane)) | ((row_id == seqs + b) & (lane_id == lane + 1))
            sel = jnp.where(sel, 1.0, 0.0).astype(BF16)
            here = (lane_row == lane) | (lane_row == lane + 1)
            for n, _, _, buf in sides:
                ins = dot32(kvt[n], sel)
                old = buf[b, :, pl.ds(off, wide)].astype(F32)
                buf[b, :, pl.ds(off, wide)] = jnp.where(here, ins, old).astype(BF16)
            for copy in stores(b):
                copy.start()
        queries = [spread_query(qkv_ref, b, seqs, hmask) for b in seqids]
        scores = [dot32(q, kbuf[b]) for q, b in zip(queries, seqids)]
        parts = []
        for b, sc in zip(seqids, scores):
            for s in range(TOKENS):
                t = pos_ref[b] + s
                bias = pltpu.roll(tab_ref[...], lax.rem(t + 1, cache_len), 1)
                parts.append(jnp.where(t_id <= t, sc[s * HROWS:(s + 1) * HROWS] + bias, NEG))
        mix_values(softmax_rows(jnp.concatenate(parts, axis=0)), vbuf, seqids, hmask, o_ref)
        return carry

    lax.fori_loop(0, seqs // SEQ_BLOCK, step, 0)
    for b in range(seqs):
        for copy in stores(b):
            copy.wait()


def self_attention(layer, pos, qkv, table, cache_k, cache_v, outs):
    layers, seqs, _, cache_len = cache_k.shape
    vm = pl.BlockSpec(memory_space=pltpu.VMEM)
    hb = pl.BlockSpec(memory_space=pl.ANY)
    in_specs = [pl.BlockSpec(memory_space=pltpu.SMEM), vm, vm, hb, hb]
    args = [pos, qkv, table, cache_k, cache_v]
    aliases = {}
    if outs is not None:
        in_specs += [hb, hb]
        args += list(outs)
        aliases = {5: 0, 6: 1}
    buf = pltpu.VMEM((seqs, D, cache_len), BF16)
    return pl.pallas_call(
        functools.partial(self_kernel, layer, seqs, outs is not None),
        out_shape=(jax.ShapeDtypeStruct(cache_k.shape, BF16), jax.ShapeDtypeStruct(cache_v.shape, BF16),
                   jax.ShapeDtypeStruct((TOKENS, seqs, D), F32)),
        in_specs=in_specs,
        out_specs=[hb, hb, vm],
        scratch_shapes=[buf, buf, pltpu.VMEM((2, D, TOKENS * seqs), BF16),
                        pltpu.SemaphoreType.DMA((2, seqs)), pltpu.SemaphoreType.DMA((2, seqs))],
        input_output_aliases=aliases,
        cost_estimate=pl.CostEstimate(flops=20_000_000_000, bytes_accessed=4 * seqs * D * cache_len * 2,
                                      transcendentals=0),
        compiler_params=pltpu.CompilerParams(vmem_limit_bytes=VMEM_LIMIT),
        name="self_attn",
    )(*args)


def rms(res, gain):
    mean_sq = jnp.mean(res * res, axis=-1, keepdims=True)
    return (res * lax.rsqrt(mean_sq + NORM_EPS) * gain.astype(F32)).astype(BF16)


class Stage:
    def __init__(self):
        dp, self.c, self.r = lax.axis_index("dp"), lax.axis_index("col"), lax.axis_index("row")
        self.across = (self.r + 2) % 4
        core = self.r + 1 - 2 * (self.r % 2)
        self.peer = (dp, 1 - self.c, self.r)
        self.partner = (dp, self.c, core)
        self.xpeer = (dp, self.c, self.across)
        self.diagonal = (dp, 1 - self.c, self.across)

    def greet(self):
        barrier = pltpu.get_barrier_semaphore()
        for other in (self.peer, self.partner, self.xpeer, self.diagonal):
            pl.semaphore_signal(barrier, inc=1, device_id=other, device_id_type=MESH)
        pl.semaphore_wait(barrier, 4)

    def remote(self, src, dst, send_sem, recv_sem, to):
        return pltpu.make_async_remote_copy(src_ref=src, dst_ref=dst, send_sem=send_sem, recv_sem=recv_sem,
                                            device_id=to, device_id_type=MESH)

    def send(self, src, dst, sems):
        copy = self.remote(src, dst, sems.at[0], sems.at[1], self.peer)
        copy.start()
        return copy

    def trade_rows(self, own, buf, sems):
        buf[0] = own
        self.send(buf.at[0], buf.at[1], sems).wait()
        return jnp.concatenate([buf[0], buf[1]], axis=0)

    def give_rows(self, mine, buf, sems, out_ref):
        rows = mine.shape[0] // 2
        c = self.c
        mine = mine.astype(BF16)
        buf[0] = mine[rows:]
        copy = self.send(buf.at[0], buf.at[1], sems)
        out_ref[c] = mine[:rows].astype(F32)
        copy.wait()
        out_ref[1 - c] = buf[1].astype(F32)


class Weight:
    def __init__(self, st, own, dst, col, sems, crossed=None):
        depth, width = own.shape
        self.st, self.crossed = st, crossed

        def place(owner):
            return dst.at[pl.ds(pl.multiple_of(owner * depth, depth), depth), pl.ds(col, width)]

        mine, theirs = place(st.r), place(st.across)
        self.local = pltpu.make_async_copy(own, mine, sems.at[0])
        self.share = st.remote(own, mine, sems.at[1], sems.at[2], st.partner)
        if crossed is None:
            self.cross = st.remote(own, mine, sems.at[3], sems.at[4], st.xpeer)
            self.pass_on = st.remote(theirs, theirs, sems.at[5], sems.at[6], st.partner)
        else:
            self.cross = pltpu.make_async_copy(crossed, theirs, sems.at[3])
            self.pass_on = st.remote(crossed, theirs, sems.at[5], sems.at[6], st.partner)

    def open_local(self):
        self.local.start()
        if self.crossed is not None:
            self.cross.start()

    def open_cross(self):
        if self.crossed is None:
            self.cross.start()

    def open_share(self):
        self.share.start()
        if self.crossed is not None:
            self.pass_on.start()

    def relay(self):
        if self.crossed is None:
            self.cross.wait_recv()
            self.pass_on.start()

    def finish(self):
        self.local.wait()
        self.share.wait()
        if self.crossed is None:
            self.cross.wait_send()
        else:
            self.cross.wait()
        self.pass_on.wait()


def each(items, name):
    for item in items:
        getattr(item, name)()


def weights_of(st, refs, layer, dst, sems, crossed=None):
    col, found = 0, []
    for n, ref in enumerate(refs):
        width = ref.shape[2]
        given = None if crossed is None else crossed.at[:, pl.ds(col, width)]
        found.append(Weight(st, ref.at[layer], dst, col, sems.at[n], given))
        col += width
    return found


def forward(st, refs, layer, dst, sems):
    col, copies = 0, []
    for n, ref in enumerate(refs):
        width = ref.shape[2]
        copies.append(st.remote(ref.at[layer], dst.at[:, pl.ds(col, width)], sems.at[n, 0], sems.at[n, 1], st.xpeer))
        col += width
    return copies


def collect(refs, layer, dst, sems):
    col, copies = 0, []
    for n, ref in enumerate(refs):
        width = ref.shape[2]
        copies.append(pltpu.make_async_copy(ref.at[layer], dst.at[:, pl.ds(col, width)], sems.at[n]))
        col += width
    return copies


class Whole:
    def __init__(self, st, packs, dst, sems):
        block, half = packs[0].shape[1], D // 2
        self.locals, self.shares = [], []
        for w in range(packs[0].shape[2] // half):
            cols = pl.ds(w * half, half)
            self.locals.append([])
            self.shares.append([])
            for n, (pack, cb) in enumerate(zip(packs, (st.c, 1 - st.c))):
                for m, owner in enumerate((st.r, st.across)):
                    src = pack.at[m, :, cols]
                    place = dst.at[cb, pl.ds(pl.multiple_of(owner * block, block), block), cols]
                    sem = sems.at[w, n, m]
                    self.locals[w].append(pltpu.make_async_copy(src, place, sem.at[0]))
                    self.shares[w].append(st.remote(src, place, sem.at[1], sem.at[2], st.partner))

    def open_local(self):
        for copies in self.locals:
            each(copies, "start")

    def open_share(self):
        for copies in self.shares:
            each(copies, "start")

    def finish(self, w):
        each(self.locals[w], "wait")
        each(self.shares[w], "wait")


class Down:
    def __init__(self, st, own, dst, sems):
        depth = own.shape[0]
        x, core = st.r // 2, st.r % 2
        at = pl.ds(pl.multiple_of(core * depth, depth), depth)
        self.home = x == st.c
        dp = lax.axis_index("dp")
        place = dst.at[st.c, at, :]
        self.local = pltpu.make_async_copy(own, place, sems.at[0, st.c])
        self.near = st.remote(own, place, sems.at[1, 0], sems.at[0, st.c], (dp, x, st.r))
        self.far = st.remote(own, place, sems.at[1, 1], sems.at[0, st.c], (dp, x, st.across))
        self.arrive, self.relays = [], []
        for cb in range(2):
            got = dst.at[cb, at, :]
            self.arrive.append(st.remote(own, got, sems.at[1, 0], sems.at[0, cb], st.peer))
            self.relays.append(st.remote(got, got, sems.at[2, cb], sems.at[3, cb], st.partner))

    def open(self):
        self.far.start()

        @pl.when(self.home)
        def _():
            self.local.start()

        @pl.when(jnp.logical_not(self.home))
        def _():
            self.near.start()

    def relay(self):
        for arrive, relay in zip(self.arrive, self.relays):
            arrive.wait_recv()
            relay.start()

    def finish(self):
        self.far.wait_send()

        @pl.when(jnp.logical_not(self.home))
        def _():
            self.near.wait_send()
        each(self.relays, "wait")


class NextLayer:
    def __init__(self, st, attn, mlp, layer, pack_ref, tail_ref, pbuf, tbuf, sems, xsems):
        self.loads = collect(attn, layer, pbuf, sems.at[0]) + collect(mlp, layer, tbuf, sems.at[1])
        self.sends = forward(st, attn, layer, pack_ref.at[1], xsems)
        self.stores = [pltpu.make_async_copy(pbuf, pack_ref.at[0], sems.at[2, 0]),
                       pltpu.make_async_copy(tbuf, tail_ref, sems.at[2, 1])]

    def store(self):
        each(self.loads, "wait")
        each(self.stores, "start")

    def finish(self):
        each(self.stores, "wait")
        each(self.sends, "wait")


def bias_table(bias_ref, tab_ref):
    buckets, length = bias_ref.shape[1], tab_ref.shape[1]
    dist = length - 1 - lax.broadcasted_iota(jnp.int32, (buckets, length), 1)
    far = jnp.full((buckets, length), BUCKET_EDGES[0] - 1, jnp.int32)
    for edge in BUCKET_EDGES:
        far = far + jnp.where(dist >= edge, 1, 0)
    bucket = jnp.where(dist < BUCKET_EDGES[0], dist, far)
    pick = jnp.where(bucket == lax.broadcasted_iota(jnp.int32, (buckets, length), 0), 1.0, 0.0).astype(BF16)
    left = jnp.concatenate([bias_ref[...], jnp.zeros((HROWS - bias_ref.shape[0], buckets), F32)], axis=0)
    total = jnp.zeros((HROWS, length), F32)
    for _ in range(3):
        part = left.astype(BF16)
        total = total + dot32(part, pick)
        left = left - part.astype(F32)
    tab_ref[...] = total


def start_kernel(first_ref, second_ref, gain_ref, bias_ref, wq_r, wk_r, wv_r, wo_r, wc_r, wco_r, wg_r, wu_r,
                 x_ref, qkv_ref, pack_ref, tail_ref, tab_ref, hbuf, wqkv, qbuf, pbuf, tbuf, wsem, nsem, xsem, sem):
    st = Stage()
    weights = weights_of(st, (wq_r, wk_r, wv_r), 0, wqkv, wsem)
    coming = NextLayer(st, (wo_r, wc_r, wco_r), (wg_r, wu_r), 0, pack_ref, tail_ref, pbuf, tbuf, nsem, xsem)
    each(weights, "open_local")
    each(coming.loads, "start")
    st.greet()
    each(weights, "open_cross")
    each(coming.sends, "start")
    each(weights, "open_share")
    hidden = jnp.concatenate([first_ref[...], second_ref[...]], axis=0)
    x_ref[...] = hidden.astype(F32)
    res = st.trade_rows(hidden, hbuf, sem.at[0]).astype(F32)
    normed = rms(res, gain_ref[0:1, :])
    bias_table(bias_ref, tab_ref)
    coming.store()
    each(weights, "relay")
    each(weights, "finish")
    st.give_rows(dot32(normed, wqkv[...]), qbuf, sem.at[1], qkv_ref)
    coming.finish()


def both_blocks(act, packed, which):
    half = D // 2
    cols = slice(which * half, (which + 1) * half)
    return [dot32(act, packed[cb, :, cols]).astype(BF16) for cb in range(2)]


def layer_kernel(layer, last, seqs, len_ref, o_ref, x_ref, gcross_ref, gmlp_ref, *refs):
    if last:
        (ck, cv, pack_in, ypack_in, xtail_in, wg_r, wu_r, wd_r, hid_ref,
         kbuf, vbuf, wattn, wtail, wdown, qs, os, nbuf, zbuf, kvsem, asem, wtsem, dsem, sem, sem2) = refs
    else:
        (gself_ref, ck, cv, pack_in, ypack_in, xtail_in, wg_r, wu_r, wd_r, wq_r, wk_r, wv_r, wo_r, wc_r, wco_r,
         x_out, qkv_ref, pack_ref, tail_ref,
         kbuf, vbuf, wattn, wtail, wdown, qs, os, nbuf, zbuf, kvsem, asem, wtsem, dsem, sem, sem2,
         rbuf, wqkv, qkvbuf, pbuf, tbuf, wsem, nsem, xsem) = refs
    st = Stage()
    rows = o_ref.shape[0]
    attn = Whole(st, (pack_in, ypack_in), wattn, asem)
    tail = weights_of(st, (wg_r, wu_r), layer, wtail, wtsem, xtail_in)
    down = Down(st, wd_r.at[layer], wdown, dsem)
    attn.open_local()

    def caches(b):
        return [pltpu.make_async_copy(src.at[layer, b], buf.at[b], kvsem.at[n, b])
                for n, (src, buf) in enumerate(((ck, kbuf), (cv, vbuf)))]

    def fetch_caches(b, carry):
        each(caches(b), "start")
        return carry

    st.greet()
    attn.open_share()
    down.open()
    lax.fori_loop(0, seqs, fetch_caches, 0)
    each(tail, "open_local")
    if not last:
        ahead = weights_of(st, (wq_r, wk_r, wv_r), layer + 1, wqkv, wsem)
        coming = NextLayer(st, (wo_r, wc_r, wco_r), (wg_r, wu_r), layer + 1, pack_ref, tail_ref, pbuf, tbuf,
                           nsem, xsem)
        each(ahead, "open_cross")
        each(coming.sends, "start")
        each(ahead, "open_local")
        each(coming.loads, "start")
    attn.finish(0)
    y = jnp.concatenate(both_blocks(o_ref[...].astype(BF16), wattn, 0), axis=1)
    res = x_ref[...] + y.astype(F32)
    attn.finish(1)
    for cb, q in enumerate(both_blocks(rms(res, gcross_ref[layer:layer + 1, :]), wattn, 1)):
        qs[cb] = q.astype(F32)
    each(tail, "open_share")
    if not last:
        each(ahead, "open_share")
        coming.store()

    def cross_step(i, carry):
        hmask = head_mask()
        t_id = lax.broadcasted_iota(jnp.int32, (TOKENS * HROWS, kbuf.shape[-1]), 1)
        seqids = [i * SEQ_BLOCK + j for j in range(SEQ_BLOCK)]
        for b in seqids:
            each(caches(b), "wait")
        queries = [spread_query(qs, b, seqs, hmask) for b in seqids]
        scores = [dot32(q, kbuf[b]) for q, b in zip(queries, seqids)]
        parts = [jnp.where(t_id < len_ref[b], sc, NEG) for b, sc in zip(seqids, scores)]
        mix_values(softmax_rows(jnp.concatenate(parts, axis=0)), vbuf, seqids, hmask, os)
        return carry

    lax.fori_loop(0, seqs // SEQ_BLOCK, cross_step, 0)
    down.relay()
    attn.finish(2)
    y = jnp.concatenate(both_blocks(os[...].reshape(rows, D).astype(BF16), wattn, 2), axis=1)
    res = res + y.astype(F32)
    gain = gmlp_ref[layer:layer + 1, :]
    ff = wtail.shape[1] // 2

    def gated(normed):
        gate = dot32(normed, wtail[:, 0:ff]).astype(BF16).astype(F32)
        up = dot32(normed, wtail[:, ff:2 * ff]).astype(BF16).astype(F32)
        return (gate * jax.nn.sigmoid(gate) * up).astype(BF16)

    normed = rms(res, gain)
    nbuf[0] = normed
    moving = st.send(nbuf.at[0], nbuf.at[1], sem.at[0])
    if not last:
        rbuf[0] = res
        moving_res = st.send(rbuf.at[0], rbuf.at[1], sem2.at[0, 0])
    each(tail, "finish")
    own_act = gated(normed)
    moving.wait()
    act = jnp.concatenate([own_act, gated(nbuf[1])], axis=0)
    down.finish()
    part = jnp.concatenate([dot32(act, wdown[0]), dot32(act, wdown[1])], axis=1)
    zbuf[0, 0] = part[:rows]
    zbuf[0, 1] = part[rows:]
    moving_z = [st.send(zbuf.at[0, 1], zbuf.at[1, 0], sem2.at[1, 0])]
    if not last:
        moving_z.append(st.send(zbuf.at[0, 0], zbuf.at[1, 1], sem2.at[1, 1]))
        each(ahead, "relay")
        moving_res.wait()
    each(moving_z, "wait")
    if last:
        hid_ref[...] = res + (zbuf[0, 0] + zbuf[1, 0]).astype(BF16).astype(F32)
    else:
        z = (zbuf[0] + zbuf[1]).astype(BF16).astype(F32)
        res = jnp.concatenate([res + z[0], rbuf[1] + z[1]], axis=0)
        x_out[...] = res[:rows]
        normed = rms(res, gself_ref[layer + 1:layer + 2, :])
        each(ahead, "finish")
        st.give_rows(dot32(normed, wqkv[...]), qkvbuf, sem.at[1], qkv_ref)
        coming.finish()


def exchange_call(kernel, cid, name, specs, args, outs, scratch, flops):
    spaces = {"s": pltpu.SMEM, "v": pltpu.VMEM, "h": pl.ANY}
    spec = lambda letters: [pl.BlockSpec(memory_space=spaces[x]) for x in letters]
    return pl.pallas_call(
        kernel,
        out_shape=tuple(t for _, t in outs),
        in_specs=spec(specs),
        out_specs=tuple(spec(x for x, _ in outs)),
        scratch_shapes=scratch,
        cost_estimate=pl.CostEstimate(flops=flops, bytes_accessed=8 << 20, transcendentals=0),
        compiler_params=pltpu.CompilerParams(collective_id=cid, has_side_effects=True, vmem_limit_bytes=VMEM_LIMIT),
        name=name,
    )(*args)


def solution(mesh):
    batch_axes = ('dp', 'col', 'row')

    def local_step(h_first, h_second, start_pos, enc_lens, dec_bias, norm_self, norm_cross, norm_mlp,
                   w_query, w_key, w_value, w_out, w_cquery, w_cout, w_gate, w_up, w_down,
                   self_k, self_v, cross_k, cross_v):
        layers, seqs, cache_len = self_k.shape[:3]
        rows = TOKENS * seqs
        half = D // 2
        ffc = w_gate.shape[2]
        depth = 4 * w_query.shape[1]
        fdepth = 4 * w_down.shape[1]

        def flat(cache):
            return jnp.transpose(cache, (0, 1, 3, 4, 2)).reshape(layers, seqs, D, cache.shape[2])

        caches = [flat(a) for a in (self_k, self_v, cross_k, cross_v)]
        block = w_query.shape[1]

        vm = lambda shape, dt=BF16: pltpu.VMEM(shape, dt)
        dma = lambda *shape: pltpu.SemaphoreType.DMA(shape)
        rowbuf = lambda width, dt=BF16: vm((2, rows, width), dt)
        res_t = ("v", jax.ShapeDtypeStruct((rows, D), F32))
        qkv_t = ("v", jax.ShapeDtypeStruct((2, rows, 3 * half), F32))
        pack_t = ("h", jax.ShapeDtypeStruct((2, block, 3 * half), BF16))
        tail_t = ("h", jax.ShapeDtypeStruct((block, 2 * ffc), BF16))
        coming = [vm((block, 3 * half)), vm((block, 2 * ffc))]
        across = [(r, (r + 2) % 4) for r in range(4)]
        flip = [(0, 1), (1, 0)]

        table_t = ("v", jax.ShapeDtypeStruct((HROWS, cache_len), F32))
        res, qkv, pack, tail_own, table = exchange_call(
            start_kernel, 0, "start", "vvvv" + "h" * 8,
            [h_first, h_second, norm_self, dec_bias.T, w_query, w_key, w_value, w_out, w_cquery, w_cout, w_gate, w_up],
            [res_t, qkv_t, pack_t, tail_t, table_t],
            [rowbuf(D), vm((depth, 3 * half)), rowbuf(3 * half)] + coming
            + [dma(3, 7), dma(3, 3), dma(3, 2), dma(2, 2)], 3_000_000_000)
        outs = None
        for l in range(layers):
            last = l == layers - 1
            ypack = lax.ppermute(pack, "col", flip)
            xtail = lax.ppermute(tail_own, "row", across)
            k_out, v_out, mixed = self_attention(l, start_pos, qkv, table, caches[0], caches[1], outs)
            outs = (k_out, v_out)
            cache_buf = vm((seqs, D, cross_k.shape[2]))
            scratch = [cache_buf, cache_buf, vm((2, depth, 3 * half)), vm((depth, 2 * ffc)), vm((2, fdepth // 2, half)),
                       vm((2, rows, half), F32), vm((TOKENS, seqs, D), F32), rowbuf(D), vm((2, 2, rows, D), F32),
                       dma(2, seqs), dma(3, 2, 2, 3), dma(2, 7), dma(4, 2), dma(2, 2), dma(2, 2, 2)]
            args = [enc_lens, mixed.reshape(rows, D), res, norm_cross, norm_mlp]
            weights = [caches[2], caches[3], pack, ypack, xtail, w_gate, w_up, w_down]
            if last:
                hid, = exchange_call(
                    functools.partial(layer_kernel, l, True, seqs), 1 + l, "last", "svvvv" + "h" * 8,
                    args + weights, [res_t],
                    scratch, 20_000_000_000)
            else:
                scratch += [rowbuf(D, F32), vm((depth, 3 * half)), rowbuf(3 * half)] + coming
                scratch += [dma(3, 7), dma(3, 3), dma(3, 2)]
                res, qkv, pack, tail_own = exchange_call(
                    functools.partial(layer_kernel, l, False, seqs), 1 + l, "layer", "svvvvv" + "h" * 14,
                    args + [norm_self] + weights
                    + [w_query, w_key, w_value, w_out, w_cquery, w_cout],
                    [res_t, qkv_t, pack_t, tail_t], scratch, 20_000_000_000)

        def unflat(cache):
            return jnp.transpose(cache.reshape(layers, seqs, HEADS, HEAD_DIM, cache_len), (0, 1, 4, 2, 3))

        return hid.reshape(TOKENS, seqs, D).astype(BF16), unflat(outs[0]), unflat(outs[1])

    row_spec = P(batch_axes, None)
    seq_spec = P(batch_axes)
    weight_spec = P(None, 'row', 'col')
    cache_spec = P(None, batch_axes)
    in_specs = (row_spec, row_spec, seq_spec, seq_spec, P(), P(), P(), P()) + (weight_spec,) * 9 + (cache_spec,) * 4
    out_specs = (P(None, batch_axes), cache_spec, cache_spec)
    return jax.shard_map(local_step, mesh=mesh, in_specs=in_specs, out_specs=out_specs, check_vma=False)
```

```python
import functools

import jax
import jax.numpy as jnp
from jax import lax
from jax.experimental import pallas as pl
from jax.experimental.pallas import tpu as pltpu
from jax.sharding import PartitionSpec as P

NORM_EPS = 1e-6
BUCKET_EDGES = (16, 19, 21, 24, 27, 31, 35, 40, 46, 52, 59, 67, 77, 87, 99, 113)
HEADS = 12
HEAD_DIM = 64
D = HEADS * HEAD_DIM
TOKENS = 2
LANES = 128
HROWS = 16
NEG = -1e30
SEQ_BLOCK = 4
AHEAD = 8
MESH = pl.DeviceIdType.MESH
F32 = jnp.float32
BF16 = jnp.bfloat16
VMEM_LIMIT = 67_043_328


def dot32(a, b):
    return jnp.dot(a, b, preferred_element_type=F32)


def head_mask():
    row = lax.broadcasted_iota(jnp.int32, (HROWS, D), 0)
    col = lax.broadcasted_iota(jnp.int32, (HROWS, D), 1)
    return (col >= row * HEAD_DIM) & (col < (row + 1) * HEAD_DIM)


def spread_query(q_ref, b, seqs, hmask):
    rows = []
    for s in range(TOKENS):
        at = pl.ds(s * seqs + b, 1)
        row = jnp.concatenate([q_ref[0, at, 0:D // 2], q_ref[1, at, 0:D // 2]], axis=1)
        rows.append(jnp.where(hmask, jnp.broadcast_to(row, (HROWS, D)), 0.0))
    return jnp.concatenate(rows, axis=0).astype(BF16)


def softmax_rows(sc):
    top = jnp.max(sc, axis=1, keepdims=True)
    e = jnp.exp(sc - top)
    return (e / jnp.sum(e, axis=1, keepdims=True)).astype(BF16)


def mix_values(probs, values, seqids, hmask, o_ref):
    group = TOKENS * HROWS
    mixes = [lax.dot_general(probs[n * group:(n + 1) * group], values[b], (((1,), (1,)), ((), ())),
                             preferred_element_type=F32) for n, b in enumerate(seqids)]
    for b, mixed in zip(seqids, mixes):
        for s in range(TOKENS):
            part = jnp.where(hmask, mixed[s * HROWS:(s + 1) * HROWS], 0.0)
            row = jnp.sum(part, axis=0, keepdims=True)
            o_ref[s, pl.ds(b, 1), :] = row.astype(BF16).astype(F32)


def self_kernel(layer, seqs, aliased, pos_ref, qkv_ref, tab_ref, k_in, v_in, *rest):
    k_out, v_out, o_ref, kbuf, vbuf, kvt, in_sem, out_sem = rest[2 if aliased else 0:]
    half = D // 2
    cache_len = kbuf.shape[-1]
    sides = ((0, k_in, k_out, kbuf), (1, v_in, v_out, vbuf))

    def loads(b):
        return [pltpu.make_async_copy(src.at[layer, b], buf.at[b], in_sem.at[n, b]) for n, src, _, buf in sides]

    def stores(b):
        return [pltpu.make_async_copy(buf.at[b], dst.at[layer, b], out_sem.at[n, b]) for n, _, dst, buf in sides]

    for b in range(AHEAD):
        for copy in loads(b):
            copy.start()
    for which in range(2):
        for cb in range(2):
            lo = (which + 1) * half
            kvt[which, pl.ds(cb * half, half), :] = qkv_ref[cb, :, lo:lo + half].T.astype(BF16)

    def step(i, carry):
        hmask = head_mask()
        wide = 2 * LANES
        row_id = lax.broadcasted_iota(jnp.int32, (TOKENS * seqs, wide), 0)
        lane_id = lax.broadcasted_iota(jnp.int32, (TOKENS * seqs, wide), 1)
        lane_row = lax.broadcasted_iota(jnp.int32, (D, wide), 1)
        t_id = lax.broadcasted_iota(jnp.int32, (HROWS, cache_len), 1)
        seqids = [i * SEQ_BLOCK + j for j in range(SEQ_BLOCK)]
        for b in seqids:
            ahead = b + AHEAD

            @pl.when(ahead < seqs)
            def _():
                for copy in loads(ahead):
                    copy.start()
        for b in seqids:
            for copy in loads(b):
                copy.wait()
        for b in seqids:
            p = pos_ref[b]
            off = pl.multiple_of(jnp.minimum(p // LANES, cache_len // LANES - 2) * LANES, LANES)
            lane = p - off
            sel = ((row_id == b) & (lane_id == lane)) | ((row_id == seqs + b) & (lane_id == lane + 1))
            sel = jnp.where(sel, 1.0, 0.0).astype(BF16)
            here = (lane_row == lane) | (lane_row == lane + 1)
            for n, _, _, buf in sides:
                ins = dot32(kvt[n], sel)
                old = buf[b, :, pl.ds(off, wide)].astype(F32)
                buf[b, :, pl.ds(off, wide)] = jnp.where(here, ins, old).astype(BF16)
            for copy in stores(b):
                copy.start()
        queries = [spread_query(qkv_ref, b, seqs, hmask) for b in seqids]
        scores = [dot32(q, kbuf[b]) for q, b in zip(queries, seqids)]
        parts = []
        for b, sc in zip(seqids, scores):
            for s in range(TOKENS):
                t = pos_ref[b] + s
                bias = pltpu.roll(tab_ref[...], lax.rem(t + 1, cache_len), 1)
                parts.append(jnp.where(t_id <= t, sc[s * HROWS:(s + 1) * HROWS] + bias, NEG))
        mix_values(softmax_rows(jnp.concatenate(parts, axis=0)), vbuf, seqids, hmask, o_ref)
        return carry

    lax.fori_loop(0, seqs // SEQ_BLOCK, step, 0)
    for b in range(seqs):
        for copy in stores(b):
            copy.wait()


def self_attention(layer, pos, qkv, table, cache_k, cache_v, outs):
    layers, seqs, _, cache_len = cache_k.shape
    vm = pl.BlockSpec(memory_space=pltpu.VMEM)
    hb = pl.BlockSpec(memory_space=pl.ANY)
    in_specs = [pl.BlockSpec(memory_space=pltpu.SMEM), vm, vm, hb, hb]
    args = [pos, qkv, table, cache_k, cache_v]
    aliases = {}
    if outs is not None:
        in_specs += [hb, hb]
        args += list(outs)
        aliases = {5: 0, 6: 1}
    buf = pltpu.VMEM((seqs, D, cache_len), BF16)
    return pl.pallas_call(
        functools.partial(self_kernel, layer, seqs, outs is not None),
        out_shape=(jax.ShapeDtypeStruct(cache_k.shape, BF16), jax.ShapeDtypeStruct(cache_v.shape, BF16),
                   jax.ShapeDtypeStruct((TOKENS, seqs, D), F32)),
        in_specs=in_specs,
        out_specs=[hb, hb, vm],
        scratch_shapes=[buf, buf, pltpu.VMEM((2, D, TOKENS * seqs), BF16),
                        pltpu.SemaphoreType.DMA((2, seqs)), pltpu.SemaphoreType.DMA((2, seqs))],
        input_output_aliases=aliases,
        cost_estimate=pl.CostEstimate(flops=20_000_000_000, bytes_accessed=4 * seqs * D * cache_len * 2,
                                      transcendentals=0),
        compiler_params=pltpu.CompilerParams(vmem_limit_bytes=VMEM_LIMIT),
        name="self_attn",
    )(*args)


def rms(res, gain):
    mean_sq = jnp.mean(res * res, axis=-1, keepdims=True)
    return (res * lax.rsqrt(mean_sq + NORM_EPS) * gain.astype(F32)).astype(BF16)


class Stage:
    def __init__(self):
        dp, self.c, self.r = lax.axis_index("dp"), lax.axis_index("col"), lax.axis_index("row")
        self.across = (self.r + 2) % 4
        core = self.r + 1 - 2 * (self.r % 2)
        self.peer = (dp, 1 - self.c, self.r)
        self.partner = (dp, self.c, core)
        self.xpeer = (dp, self.c, self.across)
        self.diagonal = (dp, 1 - self.c, self.across)

    def greet(self, *others):
        barrier = pltpu.get_barrier_semaphore()
        for other in others:
            pl.semaphore_signal(barrier, inc=1, device_id=other, device_id_type=MESH)
        pl.semaphore_wait(barrier, len(others))

    def remote(self, src, dst, send_sem, recv_sem, to):
        return pltpu.make_async_remote_copy(src_ref=src, dst_ref=dst, send_sem=send_sem, recv_sem=recv_sem,
                                            device_id=to, device_id_type=MESH)

    def send(self, src, dst, sems):
        copy = self.remote(src, dst, sems.at[0], sems.at[1], self.peer)
        copy.start()
        return copy

    def trade_rows(self, own, buf, sems):
        buf[0] = own
        self.send(buf.at[0], buf.at[1], sems).wait()
        return jnp.concatenate([buf[0], buf[1]], axis=0)

    def give_rows(self, mine, buf, sems, out_ref):
        rows = mine.shape[0] // 2
        c = self.c
        mine = mine.astype(BF16)
        buf[0] = mine[rows:]
        copy = self.send(buf.at[0], buf.at[1], sems)
        out_ref[c] = mine[:rows].astype(F32)
        copy.wait()
        out_ref[1 - c] = buf[1].astype(F32)


class Weight:
    def __init__(self, st, own, dst, col, sems, crossed=None, staged=False):
        depth, width = own.shape
        self.st, self.crossed, self.staged = st, crossed, staged

        def place(owner):
            return dst.at[pl.ds(pl.multiple_of(owner * depth, depth), depth), pl.ds(col, width)]

        mine, theirs = place(st.r), place(st.across)
        self.local = pltpu.make_async_copy(own, mine, sems.at[0])
        own = mine if staged else own
        self.share = st.remote(own, mine, sems.at[1], sems.at[2], st.partner)
        if crossed is None:
            self.cross = st.remote(own, mine, sems.at[3], sems.at[4], st.xpeer)
            self.pass_on = st.remote(theirs, theirs, sems.at[5], sems.at[6], st.partner)
        else:
            self.cross = pltpu.make_async_copy(crossed, theirs, sems.at[3])
            self.pass_on = st.remote(crossed, theirs, sems.at[5], sems.at[6], st.partner)

    def open_local(self):
        self.local.start()
        if self.crossed is not None:
            self.cross.start()

    def open_cross(self):
        if self.staged:
            self.local.wait()
        if self.crossed is None:
            self.cross.start()

    def open_share(self):
        self.share.start()
        if self.crossed is not None:
            self.pass_on.start()

    def relay(self):
        if self.crossed is None:
            self.cross.wait_recv()
            self.pass_on.start()

    def finish(self):
        if not self.staged:
            self.local.wait()
        self.share.wait()
        if self.crossed is None:
            self.cross.wait_send()
        else:
            self.cross.wait()
        self.pass_on.wait()


def each(items, name):
    for item in items:
        getattr(item, name)()


def weights_of(st, refs, layer, dst, sems, crossed=None, staged=False):
    col, found = 0, []
    for n, ref in enumerate(refs):
        width = ref.shape[2]
        given = None if crossed is None else crossed.at[:, pl.ds(col, width)]
        found.append(Weight(st, ref.at[layer], dst, col, sems.at[n], given, staged))
        col += width
    return found


def forward(st, refs, layer, dst, sems):
    col, copies = 0, []
    for n, ref in enumerate(refs):
        width = ref.shape[2]
        copies.append(st.remote(ref.at[layer], dst.at[:, pl.ds(col, width)], sems.at[n, 0], sems.at[n, 1], st.xpeer))
        col += width
    return copies


def collect(refs, layer, dst, sems):
    col, copies = 0, []
    for n, ref in enumerate(refs):
        width = ref.shape[2]
        copies.append(pltpu.make_async_copy(ref.at[layer], dst.at[:, pl.ds(col, width)], sems.at[n]))
        col += width
    return copies


class Whole:
    def __init__(self, st, packs, dst, sems):
        block, half = packs[0].shape[1], D // 2
        self.locals, self.shares = [], []
        for w in range(packs[0].shape[2] // half):
            cols = pl.ds(w * half, half)
            self.locals.append([])
            self.shares.append([])
            for n, (pack, cb) in enumerate(zip(packs, (st.c, 1 - st.c))):
                for m, owner in enumerate((st.r, st.across)):
                    src = pack.at[m, :, cols]
                    place = dst.at[cb, pl.ds(pl.multiple_of(owner * block, block), block), cols]
                    sem = sems.at[w, n, m]
                    self.locals[w].append(pltpu.make_async_copy(src, place, sem.at[0]))
                    self.shares[w].append(st.remote(src, place, sem.at[1], sem.at[2], st.partner))

    def open_local(self):
        for copies in self.locals:
            each(copies, "start")

    def open_share(self):
        for copies in self.shares:
            each(copies, "start")

    def finish(self, w):
        each(self.locals[w], "wait")
        each(self.shares[w], "wait")


class Down:
    def __init__(self, st, own, dst, stage, sems):
        depth = own.shape[0]
        self.load = pltpu.make_async_copy(own, stage, sems.at[4, 0])
        x, core = st.r // 2, st.r % 2
        at = pl.ds(pl.multiple_of(core * depth, depth), depth)
        self.home = x == st.c
        dp = lax.axis_index("dp")
        place = dst.at[st.c, at, :]
        self.local = pltpu.make_async_copy(own, place, sems.at[0, st.c])
        self.near = st.remote(stage, place, sems.at[1, 0], sems.at[0, st.c], (dp, x, st.r))
        self.far = st.remote(stage, place, sems.at[1, 1], sems.at[0, st.c], (dp, x, st.across))
        self.arrive, self.relays = [], []
        for cb in range(2):
            got = dst.at[cb, at, :]
            self.arrive.append(st.remote(stage, got, sems.at[1, 0], sems.at[0, cb], st.peer))
            self.relays.append(st.remote(got, got, sems.at[2, cb], sems.at[3, cb], st.partner))

    def open(self):
        self.load.wait()
        self.far.start()

        @pl.when(self.home)
        def _():
            self.local.start()

        @pl.when(jnp.logical_not(self.home))
        def _():
            self.near.start()

    def relay(self):
        for arrive, relay in zip(self.arrive, self.relays):
            arrive.wait_recv()
            relay.start()

    def finish(self):
        self.far.wait_send()

        @pl.when(jnp.logical_not(self.home))
        def _():
            self.near.wait_send()
        each(self.relays, "wait")


class NextLayer:
    def __init__(self, st, attn, mlp, layer, pack_ref, tail_ref, pbuf, tbuf, sems, xsems):
        self.loads = collect(attn, layer, pbuf, sems.at[0]) + collect(mlp, layer, tbuf, sems.at[1])
        self.sends = forward(st, attn, layer, pack_ref.at[1], xsems)
        self.stores = [pltpu.make_async_copy(pbuf, pack_ref.at[0], sems.at[2, 0]),
                       pltpu.make_async_copy(tbuf, tail_ref, sems.at[2, 1])]

    def store(self):
        each(self.loads, "wait")
        each(self.stores, "start")

    def finish(self):
        each(self.stores, "wait")
        each(self.sends, "wait")


def bias_table(bias_ref, tab_ref):
    buckets, length = bias_ref.shape[1], tab_ref.shape[1]
    dist = length - 1 - lax.broadcasted_iota(jnp.int32, (buckets, length), 1)
    far = jnp.full((buckets, length), BUCKET_EDGES[0] - 1, jnp.int32)
    for edge in BUCKET_EDGES:
        far = far + jnp.where(dist >= edge, 1, 0)
    bucket = jnp.where(dist < BUCKET_EDGES[0], dist, far)
    pick = jnp.where(bucket == lax.broadcasted_iota(jnp.int32, (buckets, length), 0), 1.0, 0.0).astype(BF16)
    left = jnp.concatenate([bias_ref[...], jnp.zeros((HROWS - bias_ref.shape[0], buckets), F32)], axis=0)
    total = jnp.zeros((HROWS, length), F32)
    for _ in range(3):
        part = left.astype(BF16)
        total = total + dot32(part, pick)
        left = left - part.astype(F32)
    tab_ref[...] = total


def start_kernel(first_ref, second_ref, gain_ref, bias_ref, wq_r, wk_r, wv_r, wo_r, wc_r, wco_r, wg_r, wu_r,
                 x_ref, qkv_ref, pack_ref, tail_ref, tab_ref, hbuf, wqkv, qbuf, pbuf, tbuf, wsem, nsem, xsem, sem):
    st = Stage()
    weights = weights_of(st, (wq_r, wk_r, wv_r), 0, wqkv, wsem, staged=True)
    coming = NextLayer(st, (wo_r, wc_r, wco_r), (wg_r, wu_r), 0, pack_ref, tail_ref, pbuf, tbuf, nsem, xsem)
    each(weights, "open_local")
    each(coming.loads, "start")
    st.greet(st.peer, st.partner, st.xpeer)
    each(weights, "open_cross")
    each(coming.sends, "start")
    each(weights, "open_share")
    hidden = jnp.concatenate([first_ref[...], second_ref[...]], axis=0)
    x_ref[...] = hidden.astype(F32)
    res = st.trade_rows(hidden, hbuf, sem.at[0]).astype(F32)
    normed = rms(res, gain_ref[0:1, :])
    bias_table(bias_ref, tab_ref)
    coming.store()
    each(weights, "relay")
    each(weights, "finish")
    st.give_rows(dot32(normed, wqkv[...]), qbuf, sem.at[1], qkv_ref)
    coming.finish()


def both_blocks(act, packed, which):
    half = D // 2
    cols = slice(which * half, (which + 1) * half)
    return [dot32(act, packed[cb, :, cols]).astype(BF16) for cb in range(2)]


def layer_kernel(layer, last, seqs, len_ref, o_ref, x_ref, gcross_ref, gmlp_ref, *refs):
    if last:
        (ck, cv, pack_in, ypack_in, xtail_in, wg_r, wu_r, wd_r, own_ref, zin_ref,
         kbuf, vbuf, wattn, wtail, wdown, dstage, qs, os, nbuf, zbuf, kvsem, asem, wtsem, dsem, sem, sem2, rbuf, osem) = refs
    else:
        (gself_ref, ck, cv, pack_in, ypack_in, xtail_in, wg_r, wu_r, wd_r, wq_r, wk_r, wv_r, wo_r, wc_r, wco_r,
         x_out, qkv_ref, pack_ref, tail_ref,
         kbuf, vbuf, wattn, wtail, wdown, dstage, qs, os, nbuf, zbuf, kvsem, asem, wtsem, dsem, sem, sem2,
         rbuf, wqkv, qkvbuf, pbuf, tbuf, wsem, nsem, xsem) = refs
    st = Stage()
    rows = o_ref.shape[0]
    attn = Whole(st, (pack_in, ypack_in), wattn, asem)
    tail = weights_of(st, (wg_r, wu_r), layer, wtail, wtsem, xtail_in)
    down = Down(st, wd_r.at[layer], wdown, dstage, dsem)
    attn.open_local()

    def caches(b):
        return [pltpu.make_async_copy(src.at[layer, b], buf.at[b], kvsem.at[n, b])
                for n, (src, buf) in enumerate(((ck, kbuf), (cv, vbuf)))]

    def fetch_caches(b, carry):
        each(caches(b), "start")
        return carry

    down.load.start()
    st.greet(st.peer, st.partner, st.xpeer, st.diagonal)
    down.open()
    attn.open_share()
    lax.fori_loop(0, seqs, fetch_caches, 0)
    if not last:
        ahead = weights_of(st, (wq_r, wk_r, wv_r), layer + 1, wqkv, wsem)
        coming = NextLayer(st, (wo_r, wc_r, wco_r), (wg_r, wu_r), layer + 1, pack_ref, tail_ref, pbuf, tbuf,
                           nsem, xsem)
        each(ahead, "open_cross")
        each(coming.sends, "start")
    attn.finish(0)
    y = jnp.concatenate(both_blocks(o_ref[...].astype(BF16), wattn, 0), axis=1)
    res = x_ref[...] + y.astype(F32)
    attn.finish(1)
    for cb, q in enumerate(both_blocks(rms(res, gcross_ref[layer:layer + 1, :]), wattn, 1)):
        qs[cb] = q.astype(F32)
    each(tail, "open_local")
    each(tail, "open_share")
    if not last:
        each(ahead, "open_local")
        each(coming.loads, "start")
        each(ahead, "open_share")

    def cross_step(i, carry):
        hmask = head_mask()
        t_id = lax.broadcasted_iota(jnp.int32, (TOKENS * HROWS, kbuf.shape[-1]), 1)
        seqids = [i * SEQ_BLOCK + j for j in range(SEQ_BLOCK)]
        for b in seqids:
            each(caches(b), "wait")
        queries = [spread_query(qs, b, seqs, hmask) for b in seqids]
        scores = [dot32(q, kbuf[b]) for q, b in zip(queries, seqids)]
        parts = [jnp.where(t_id < len_ref[b], sc, NEG) for b, sc in zip(seqids, scores)]
        mix_values(softmax_rows(jnp.concatenate(parts, axis=0)), vbuf, seqids, hmask, os)
        return carry

    lax.fori_loop(0, seqs // SEQ_BLOCK, cross_step, 0)
    if not last:
        coming.store()
    down.relay()
    attn.finish(2)
    y = jnp.concatenate(both_blocks(os[...].reshape(rows, D).astype(BF16), wattn, 2), axis=1)
    res = res + y.astype(F32)
    gain = gmlp_ref[layer:layer + 1, :]
    ff = wtail.shape[1] // 2

    def gated(normed):
        gate = dot32(normed, wtail[:, 0:ff]).astype(BF16).astype(F32)
        up = dot32(normed, wtail[:, ff:2 * ff]).astype(BF16).astype(F32)
        return (gate * jax.nn.sigmoid(gate) * up).astype(BF16)

    normed = rms(res, gain)
    nbuf[0] = normed
    moving = st.send(nbuf.at[0], nbuf.at[1], sem.at[0])
    if last:
        rbuf[...] = res
        res_out = pltpu.make_async_copy(rbuf, own_ref.at[0], osem.at[0])
        res_out.start()
    else:
        rbuf[0] = res
        moving_res = st.send(rbuf.at[0], rbuf.at[1], sem2.at[0, 0])
    each(tail, "finish")
    own_act = gated(normed)
    moving.wait()
    other_act = gated(nbuf[1])
    down.finish()

    def partial_sum(act):
        return jnp.concatenate([dot32(act, wdown[0]), dot32(act, wdown[1])], axis=1)

    zbuf[0, 1] = partial_sum(other_act)
    moving_z = [st.send(zbuf.at[0, 1], zin_ref if last else zbuf.at[1, 0], sem2.at[1, 0])]
    zbuf[0, 0] = partial_sum(own_act)
    if not last:
        moving_z.append(st.send(zbuf.at[0, 0], zbuf.at[1, 1], sem2.at[1, 1]))
        each(ahead, "relay")
        moving_res.wait()
    if last:
        part_out = pltpu.make_async_copy(zbuf.at[0, 0], own_ref.at[1], osem.at[1])
        part_out.start()
        res_out.wait()
        part_out.wait()
    each(moving_z, "wait")
    if not last:
        z = (zbuf[0] + zbuf[1]).astype(BF16).astype(F32)
        res = jnp.concatenate([res + z[0], rbuf[1] + z[1]], axis=0)
        x_out[...] = res[:rows]
        normed = rms(res, gself_ref[layer + 1:layer + 2, :])
        each(ahead, "finish")
        st.give_rows(dot32(normed, wqkv[...]), qkvbuf, sem.at[1], qkv_ref)
        coming.finish()


def exchange_call(kernel, cid, name, specs, args, outs, scratch, flops):
    spaces = {"s": pltpu.SMEM, "v": pltpu.VMEM, "h": pl.ANY}
    spec = lambda letters: [pl.BlockSpec(memory_space=spaces[x]) for x in letters]
    return pl.pallas_call(
        kernel,
        out_shape=tuple(t for _, t in outs),
        in_specs=spec(specs),
        out_specs=tuple(spec(x for x, _ in outs)),
        scratch_shapes=scratch,
        cost_estimate=pl.CostEstimate(flops=flops, bytes_accessed=8 << 20, transcendentals=0),
        compiler_params=pltpu.CompilerParams(collective_id=cid, has_side_effects=True, vmem_limit_bytes=VMEM_LIMIT),
        name=name,
    )(*args)


def solution(mesh):
    batch_axes = ('dp', 'col', 'row')

    def local_step(h_first, h_second, start_pos, enc_lens, dec_bias, norm_self, norm_cross, norm_mlp,
                   w_query, w_key, w_value, w_out, w_cquery, w_cout, w_gate, w_up, w_down,
                   self_k, self_v, cross_k, cross_v):
        layers, seqs, cache_len = self_k.shape[:3]
        rows = TOKENS * seqs
        half = D // 2
        ffc = w_gate.shape[2]
        depth = 4 * w_query.shape[1]
        fdepth = 4 * w_down.shape[1]

        def flat(cache):
            return jnp.transpose(cache, (0, 1, 3, 4, 2)).reshape(layers, seqs, D, cache.shape[2])

        caches = [flat(a) for a in (self_k, self_v, cross_k, cross_v)]
        block = w_query.shape[1]

        vm = lambda shape, dt=BF16: pltpu.VMEM(shape, dt)
        dma = lambda *shape: pltpu.SemaphoreType.DMA(shape)
        rowbuf = lambda width, dt=BF16: vm((2, rows, width), dt)
        res_t = ("v", jax.ShapeDtypeStruct((rows, D), F32))
        qkv_t = ("v", jax.ShapeDtypeStruct((2, rows, 3 * half), F32))
        pack_t = ("h", jax.ShapeDtypeStruct((2, block, 3 * half), BF16))
        tail_t = ("h", jax.ShapeDtypeStruct((block, 2 * ffc), BF16))
        coming = [vm((block, 3 * half)), vm((block, 2 * ffc))]
        across = [(r, (r + 2) % 4) for r in range(4)]
        flip = [(0, 1), (1, 0)]

        table_t = ("v", jax.ShapeDtypeStruct((HROWS, cache_len), F32))
        res, qkv, pack, tail_own, table = exchange_call(
            start_kernel, 0, "start", "vvvv" + "h" * 8,
            [h_first, h_second, norm_self, dec_bias.T, w_query, w_key, w_value, w_out, w_cquery, w_cout, w_gate, w_up],
            [res_t, qkv_t, pack_t, tail_t, table_t],
            [rowbuf(D), vm((depth, 3 * half)), rowbuf(3 * half)] + coming
            + [dma(3, 7), dma(3, 3), dma(3, 2), dma(2, 2)], 3_000_000_000)
        outs = None
        for l in range(layers):
            last = l == layers - 1
            ypack = lax.ppermute(pack, "col", flip)
            xtail = lax.ppermute(tail_own, "row", across)
            k_out, v_out, mixed = self_attention(l, start_pos, qkv, table, caches[0], caches[1], outs)
            outs = (k_out, v_out)
            cache_buf = vm((seqs, D, cross_k.shape[2]))
            scratch = [cache_buf, cache_buf, vm((2, depth, 3 * half)), vm((depth, 2 * ffc)), vm((2, fdepth // 2, half)), vm((fdepth // 4, half)),
                       vm((2, rows, half), F32), vm((TOKENS, seqs, D), F32), rowbuf(D), vm((2, 2, rows, D), F32),
                       dma(2, seqs), dma(3, 2, 2, 3), dma(2, 7), dma(5, 2), dma(2, 2), dma(2, 2, 2)]
            args = [enc_lens, mixed.reshape(rows, D), res, norm_cross, norm_mlp]
            weights = [caches[2], caches[3], pack, ypack, xtail, w_gate, w_up, w_down]
            if last:
                own, zin = exchange_call(
                    functools.partial(layer_kernel, l, True, seqs), 1 + l, "last", "svvvv" + "h" * 8,
                    args + weights,
                    [("h", jax.ShapeDtypeStruct((2, rows, D), F32)), ("h", jax.ShapeDtypeStruct((rows, D), F32))],
                    scratch + [vm((rows, D), F32), dma(2)], 20_000_000_000)
            else:
                scratch += [rowbuf(D, F32), vm((depth, 3 * half)), rowbuf(3 * half)] + coming
                scratch += [dma(3, 7), dma(3, 3), dma(3, 2)]
                res, qkv, pack, tail_own = exchange_call(
                    functools.partial(layer_kernel, l, False, seqs), 1 + l, "layer", "svvvvv" + "h" * 14,
                    args + [norm_self] + weights
                    + [w_query, w_key, w_value, w_out, w_cquery, w_cout],
                    [res_t, qkv_t, pack_t, tail_t], scratch, 20_000_000_000)

        def unflat(cache):
            return jnp.transpose(cache.reshape(layers, seqs, HEADS, HEAD_DIM, cache_len), (0, 1, 4, 2, 3))

        hid = own[0] + lax.reduce_precision(own[1] + zin, 8, 7)
        return hid.reshape(TOKENS, seqs, D).astype(BF16), unflat(outs[0]), unflat(outs[1])

    row_spec = P(batch_axes, None)
    seq_spec = P(batch_axes)
    weight_spec = P(None, 'row', 'col')
    cache_spec = P(None, batch_axes)
    in_specs = (row_spec, row_spec, seq_spec, seq_spec, P(), P(), P(), P()) + (weight_spec,) * 9 + (cache_spec,) * 4
    out_specs = (P(None, batch_axes), cache_spec, cache_spec)
    return jax.shard_map(local_step, mesh=mesh, in_specs=in_specs, out_specs=out_specs, check_vma=False)
```

```python
import functools

import jax
import jax.numpy as jnp
from jax import lax
from jax.experimental import pallas as pl
from jax.experimental.pallas import tpu as pltpu
from jax.sharding import PartitionSpec as P

NORM_EPS = 1e-6
BUCKET_EDGES = (16, 19, 21, 24, 27, 31, 35, 40, 46, 52, 59, 67, 77, 87, 99, 113)
HEADS = 12
HEAD_DIM = 64
D = HEADS * HEAD_DIM
TOKENS = 2
LANES = 128
HROWS = 16
NEG = -1e30
SEQ_BLOCK = 4
AHEAD = 8
MESH = pl.DeviceIdType.MESH
F32 = jnp.float32
BF16 = jnp.bfloat16
VMEM_LIMIT = 67_043_328


def dot32(a, b):
    return jnp.dot(a, b, preferred_element_type=F32)


def head_mask():
    row = lax.broadcasted_iota(jnp.int32, (HROWS, D), 0)
    col = lax.broadcasted_iota(jnp.int32, (HROWS, D), 1)
    return (col >= row * HEAD_DIM) & (col < (row + 1) * HEAD_DIM)


def spread_query(q_ref, b, seqs, hmask):
    rows = []
    for s in range(TOKENS):
        at = pl.ds(s * seqs + b, 1)
        row = jnp.concatenate([q_ref[0, at, 0:D // 2], q_ref[1, at, 0:D // 2]], axis=1)
        rows.append(jnp.where(hmask, jnp.broadcast_to(row, (HROWS, D)), 0.0))
    return jnp.concatenate(rows, axis=0).astype(BF16)


def softmax_rows(sc):
    top = jnp.max(sc, axis=1, keepdims=True)
    e = jnp.exp(sc - top)
    return (e / jnp.sum(e, axis=1, keepdims=True)).astype(BF16)


def mix_values(probs, values, seqids, hmask, o_ref):
    group = TOKENS * HROWS
    mixes = [lax.dot_general(probs[n * group:(n + 1) * group], values[b], (((1,), (1,)), ((), ())),
                             preferred_element_type=F32) for n, b in enumerate(seqids)]
    for b, mixed in zip(seqids, mixes):
        for s in range(TOKENS):
            part = jnp.where(hmask, mixed[s * HROWS:(s + 1) * HROWS], 0.0)
            row = jnp.sum(part, axis=0, keepdims=True)
            o_ref[s, pl.ds(b, 1), :] = row.astype(BF16).astype(F32)


def self_kernel(layer, seqs, aliased, pos_ref, qkv_ref, tab_ref, k_in, v_in, *rest):
    k_out, v_out, o_ref, kbuf, vbuf, kvt, in_sem, out_sem = rest[2 if aliased else 0:]
    half = D // 2
    cache_len = kbuf.shape[-1]
    sides = ((0, k_in, k_out, kbuf), (1, v_in, v_out, vbuf))

    def loads(b):
        return [pltpu.make_async_copy(src.at[layer, b], buf.at[b], in_sem.at[n, b]) for n, src, _, buf in sides]

    def stores(b):
        return [pltpu.make_async_copy(buf.at[b], dst.at[layer, b], out_sem.at[n, b]) for n, _, dst, buf in sides]

    for b in range(AHEAD):
        for copy in loads(b):
            copy.start()
    for which in range(2):
        for cb in range(2):
            lo = (which + 1) * half
            kvt[which, pl.ds(cb * half, half), :] = qkv_ref[cb, :, lo:lo + half].T.astype(BF16)

    def step(i, carry):
        hmask = head_mask()
        wide = 2 * LANES
        row_id = lax.broadcasted_iota(jnp.int32, (TOKENS * seqs, wide), 0)
        lane_id = lax.broadcasted_iota(jnp.int32, (TOKENS * seqs, wide), 1)
        lane_row = lax.broadcasted_iota(jnp.int32, (D, wide), 1)
        t_id = lax.broadcasted_iota(jnp.int32, (HROWS, cache_len), 1)
        seqids = [i * SEQ_BLOCK + j for j in range(SEQ_BLOCK)]
        for b in seqids:
            ahead = b + AHEAD

            @pl.when(ahead < seqs)
            def _():
                for copy in loads(ahead):
                    copy.start()
        for b in seqids:
            for copy in loads(b):
                copy.wait()
        for b in seqids:
            p = pos_ref[b]
            off = pl.multiple_of(jnp.minimum(p // LANES, cache_len // LANES - 2) * LANES, LANES)
            lane = p - off
            sel = ((row_id == b) & (lane_id == lane)) | ((row_id == seqs + b) & (lane_id == lane + 1))
            sel = jnp.where(sel, 1.0, 0.0).astype(BF16)
            here = (lane_row == lane) | (lane_row == lane + 1)
            for n, _, _, buf in sides:
                ins = dot32(kvt[n], sel)
                at = pl.ds(off, wide)
                buf[b, :, at] = jnp.where(here, ins.astype(BF16), buf[b, :, at])
            for copy in stores(b):
                copy.start()
        queries = [spread_query(qkv_ref, b, seqs, hmask) for b in seqids]
        scores = [dot32(q, kbuf[b]) for q, b in zip(queries, seqids)]
        parts = []
        for b, sc in zip(seqids, scores):
            for s in range(TOKENS):
                t = pos_ref[b] + s
                bias = pltpu.roll(tab_ref[...], lax.rem(t + 1, cache_len), 1)
                parts.append(jnp.where(t_id <= t, sc[s * HROWS:(s + 1) * HROWS] + bias, NEG))
        mix_values(softmax_rows(jnp.concatenate(parts, axis=0)), vbuf, seqids, hmask, o_ref)
        return carry

    lax.fori_loop(0, seqs // SEQ_BLOCK, step, 0)
    for b in range(seqs):
        for copy in stores(b):
            copy.wait()


def self_attention(layer, pos, qkv, table, cache_k, cache_v, outs):
    layers, seqs, _, cache_len = cache_k.shape
    vm = pl.BlockSpec(memory_space=pltpu.VMEM)
    hb = pl.BlockSpec(memory_space=pl.ANY)
    in_specs = [pl.BlockSpec(memory_space=pltpu.SMEM), vm, vm, hb, hb]
    args = [pos, qkv, table, cache_k, cache_v]
    aliases = {}
    if outs is not None:
        in_specs += [hb, hb]
        args += list(outs)
        aliases = {5: 0, 6: 1}
    buf = pltpu.VMEM((seqs, D, cache_len), BF16)
    return pl.pallas_call(
        functools.partial(self_kernel, layer, seqs, outs is not None),
        out_shape=(jax.ShapeDtypeStruct(cache_k.shape, BF16), jax.ShapeDtypeStruct(cache_v.shape, BF16),
                   jax.ShapeDtypeStruct((TOKENS, seqs, D), F32)),
        in_specs=in_specs,
        out_specs=[hb, hb, vm],
        scratch_shapes=[buf, buf, pltpu.VMEM((2, D, TOKENS * seqs), BF16),
                        pltpu.SemaphoreType.DMA((2, seqs)), pltpu.SemaphoreType.DMA((2, seqs))],
        input_output_aliases=aliases,
        cost_estimate=pl.CostEstimate(flops=20_000_000_000, bytes_accessed=4 * seqs * D * cache_len * 2,
                                      transcendentals=0),
        compiler_params=pltpu.CompilerParams(vmem_limit_bytes=VMEM_LIMIT),
        name="self_attn",
    )(*args)


def rms(res, gain):
    mean_sq = jnp.mean(res * res, axis=-1, keepdims=True)
    return (res * lax.rsqrt(mean_sq + NORM_EPS) * gain.astype(F32)).astype(BF16)


class Stage:
    def __init__(self):
        dp, self.c, self.r = lax.axis_index("dp"), lax.axis_index("col"), lax.axis_index("row")
        self.across = (self.r + 2) % 4
        core = self.r + 1 - 2 * (self.r % 2)
        self.peer = (dp, 1 - self.c, self.r)
        self.partner = (dp, self.c, core)
        self.xpeer = (dp, self.c, self.across)
        self.diagonal = (dp, 1 - self.c, self.across)

    def greet(self, *others):
        barrier = pltpu.get_barrier_semaphore()
        for other in others:
            pl.semaphore_signal(barrier, inc=1, device_id=other, device_id_type=MESH)
        pl.semaphore_wait(barrier, len(others))

    def remote(self, src, dst, send_sem, recv_sem, to):
        return pltpu.make_async_remote_copy(src_ref=src, dst_ref=dst, send_sem=send_sem, recv_sem=recv_sem,
                                            device_id=to, device_id_type=MESH)

    def send(self, src, dst, sems):
        copy = self.remote(src, dst, sems.at[0], sems.at[1], self.peer)
        copy.start()
        return copy

    def trade_rows(self, own, buf, sems):
        buf[0] = own
        self.send(buf.at[0], buf.at[1], sems).wait()
        return jnp.concatenate([buf[0], buf[1]], axis=0)

    def give_rows(self, mine, buf, sems, out_ref):
        rows = mine.shape[0] // 2
        c = self.c
        mine = mine.astype(BF16)
        buf[0] = mine[rows:]
        copy = self.send(buf.at[0], buf.at[1], sems)
        out_ref[c] = mine[:rows].astype(F32)
        copy.wait()
        out_ref[1 - c] = buf[1].astype(F32)


class Weight:
    def __init__(self, st, own, dst, col, sems, crossed=None, staged=False):
        depth, width = own.shape
        self.st, self.crossed, self.staged = st, crossed, staged

        def place(owner):
            return dst.at[pl.ds(pl.multiple_of(owner * depth, depth), depth), pl.ds(col, width)]

        mine, theirs = place(st.r), place(st.across)
        self.local = pltpu.make_async_copy(own, mine, sems.at[0])
        own = mine if staged else own
        self.share = st.remote(own, mine, sems.at[1], sems.at[2], st.partner)
        if crossed is None:
            self.cross = st.remote(own, mine, sems.at[3], sems.at[4], st.xpeer)
            self.pass_on = st.remote(theirs, theirs, sems.at[5], sems.at[6], st.partner)
        else:
            self.cross = pltpu.make_async_copy(crossed, theirs, sems.at[3])
            self.pass_on = st.remote(crossed, theirs, sems.at[5], sems.at[6], st.partner)

    def open_local(self):
        self.local.start()
        if self.crossed is not None:
            self.cross.start()

    def open_cross(self):
        if self.staged:
            self.local.wait()
        if self.crossed is None:
            self.cross.start()

    def open_share(self):
        self.share.start()
        if self.crossed is not None:
            self.pass_on.start()

    def relay(self):
        if self.crossed is None:
            self.cross.wait_recv()
            self.pass_on.start()

    def finish(self):
        if not self.staged:
            self.local.wait()
        self.share.wait()
        if self.crossed is None:
            self.cross.wait_send()
        else:
            self.cross.wait()
        self.pass_on.wait()


def each(items, name):
    for item in items:
        getattr(item, name)()


def weights_of(st, refs, layer, dst, sems, crossed=None, staged=False):
    col, found = 0, []
    for n, ref in enumerate(refs):
        width = ref.shape[2]
        given = None if crossed is None else crossed.at[:, pl.ds(col, width)]
        found.append(Weight(st, ref.at[layer], dst, col, sems.at[n], given, staged))
        col += width
    return found


def forward(st, refs, layer, dst, sems):
    col, copies = 0, []
    for n, ref in enumerate(refs):
        width = ref.shape[2]
        copies.append(st.remote(ref.at[layer], dst.at[:, pl.ds(col, width)], sems.at[n, 0], sems.at[n, 1], st.xpeer))
        col += width
    return copies


def collect(refs, layer, dst, sems):
    col, copies = 0, []
    for n, ref in enumerate(refs):
        width = ref.shape[2]
        copies.append(pltpu.make_async_copy(ref.at[layer], dst.at[:, pl.ds(col, width)], sems.at[n]))
        col += width
    return copies


class Whole:
    def __init__(self, st, packs, dst, sems):
        block, half = packs[0].shape[1], D // 2
        self.locals, self.shares = [], []
        for w in range(packs[0].shape[2] // half):
            cols = pl.ds(w * half, half)
            self.locals.append([])
            self.shares.append([])
            for n, (pack, cb) in enumerate(zip(packs, (st.c, 1 - st.c))):
                for m, owner in enumerate((st.r, st.across)):
                    src = pack.at[m, :, cols]
                    place = dst.at[cb, pl.ds(pl.multiple_of(owner * block, block), block), cols]
                    sem = sems.at[w, n, m]
                    self.locals[w].append(pltpu.make_async_copy(src, place, sem.at[0]))
                    self.shares[w].append(st.remote(src, place, sem.at[1], sem.at[2], st.partner))

    def open_local(self):
        for copies in self.locals:
            each(copies, "start")

    def open_share(self):
        for copies in self.shares:
            each(copies, "start")

    def finish(self, w):
        each(self.locals[w], "wait")
        each(self.shares[w], "wait")


class Down:
    def __init__(self, st, own, dst, stage, sems):
        depth = own.shape[0]
        self.load = pltpu.make_async_copy(own, stage, sems.at[4, 0])
        x, core = st.r // 2, st.r % 2
        at = pl.ds(pl.multiple_of(core * depth, depth), depth)
        self.home = x == st.c
        dp = lax.axis_index("dp")
        place = dst.at[st.c, at, :]
        self.local = pltpu.make_async_copy(own, place, sems.at[0, st.c])
        self.near = st.remote(stage, place, sems.at[1, 0], sems.at[0, st.c], (dp, x, st.r))
        self.far = st.remote(stage, place, sems.at[1, 1], sems.at[0, st.c], (dp, x, st.across))
        self.arrive, self.relays = [], []
        for cb in range(2):
            got = dst.at[cb, at, :]
            self.arrive.append(st.remote(stage, got, sems.at[1, 0], sems.at[0, cb], st.peer))
            self.relays.append(st.remote(got, got, sems.at[2, cb], sems.at[3, cb], st.partner))

    def open(self):
        self.load.wait()
        self.far.start()

        @pl.when(self.home)
        def _():
            self.local.start()

        @pl.when(jnp.logical_not(self.home))
        def _():
            self.near.start()

    def relay(self):
        for arrive, relay in zip(self.arrive, self.relays):
            arrive.wait_recv()
            relay.start()

    def finish(self):
        self.far.wait_send()

        @pl.when(jnp.logical_not(self.home))
        def _():
            self.near.wait_send()
        each(self.relays, "wait")


class NextLayer:
    def __init__(self, st, attn, mlp, layer, pack_ref, tail_ref, pbuf, tbuf, sems, xsems):
        self.loads = collect(attn, layer, pbuf, sems.at[0]) + collect(mlp, layer, tbuf, sems.at[1])
        self.sends = forward(st, attn, layer, pack_ref.at[1], xsems)
        self.stores = [pltpu.make_async_copy(pbuf, pack_ref.at[0], sems.at[2, 0]),
                       pltpu.make_async_copy(tbuf, tail_ref, sems.at[2, 1])]

    def store(self):
        each(self.loads, "wait")
        each(self.stores, "start")

    def finish(self):
        each(self.stores, "wait")
        each(self.sends, "wait")


def bias_table(bias_ref, tab_ref):
    buckets, length = bias_ref.shape[1], tab_ref.shape[1]
    dist = length - 1 - lax.broadcasted_iota(jnp.int32, (buckets, length), 1)
    far = jnp.full((buckets, length), BUCKET_EDGES[0] - 1, jnp.int32)
    for edge in BUCKET_EDGES:
        far = far + jnp.where(dist >= edge, 1, 0)
    bucket = jnp.where(dist < BUCKET_EDGES[0], dist, far)
    pick = jnp.where(bucket == lax.broadcasted_iota(jnp.int32, (buckets, length), 0), 1.0, 0.0).astype(BF16)
    left = jnp.concatenate([bias_ref[...], jnp.zeros((HROWS - bias_ref.shape[0], buckets), F32)], axis=0)
    total = jnp.zeros((HROWS, length), F32)
    for _ in range(3):
        part = left.astype(BF16)
        total = total + dot32(part, pick)
        left = left - part.astype(F32)
    tab_ref[...] = total


def start_kernel(first_ref, second_ref, gain_ref, bias_ref, wq_r, wk_r, wv_r, wo_r, wc_r, wco_r, wg_r, wu_r,
                 x_ref, qkv_ref, pack_ref, tail_ref, tab_ref, hbuf, wqkv, qbuf, pbuf, tbuf, wsem, nsem, xsem, sem):
    st = Stage()
    weights = weights_of(st, (wq_r, wk_r, wv_r), 0, wqkv, wsem, staged=True)
    coming = NextLayer(st, (wo_r, wc_r, wco_r), (wg_r, wu_r), 0, pack_ref, tail_ref, pbuf, tbuf, nsem, xsem)
    each(weights, "open_local")
    each(coming.loads, "start")
    st.greet(st.peer, st.partner, st.xpeer)
    each(weights, "open_cross")
    each(coming.sends, "start")
    each(weights, "open_share")
    hidden = jnp.concatenate([first_ref[...], second_ref[...]], axis=0)
    x_ref[...] = hidden.astype(F32)
    res = st.trade_rows(hidden, hbuf, sem.at[0]).astype(F32)
    normed = rms(res, gain_ref[0:1, :])
    bias_table(bias_ref, tab_ref)
    coming.store()
    each(weights, "relay")
    each(weights, "finish")
    st.give_rows(dot32(normed, wqkv[...]), qbuf, sem.at[1], qkv_ref)
    coming.finish()


def both_blocks(act, packed, which):
    half = D // 2
    cols = slice(which * half, (which + 1) * half)
    return [dot32(act, packed[cb, :, cols]).astype(BF16) for cb in range(2)]


def layer_kernel(layer, last, seqs, len_ref, o_ref, x_ref, gcross_ref, gmlp_ref, *refs):
    if last:
        (ck, cv, pack_in, ypack_in, xtail_in, wg_r, wu_r, wd_r, own_ref, zin_ref,
         kbuf, vbuf, wattn, wtail, wdown, dstage, qs, os, nbuf, zbuf, kvsem, asem, wtsem, dsem, sem, sem2, rbuf, osem) = refs
    else:
        (gself_ref, ck, cv, pack_in, ypack_in, xtail_in, wg_r, wu_r, wd_r, wq_r, wk_r, wv_r, wo_r, wc_r, wco_r,
         x_out, qkv_ref, pack_ref, tail_ref,
         kbuf, vbuf, wattn, wtail, wdown, dstage, qs, os, nbuf, zbuf, kvsem, asem, wtsem, dsem, sem, sem2,
         rbuf, wqkv, qkvbuf, pbuf, tbuf, wsem, nsem, xsem) = refs
    st = Stage()
    rows = o_ref.shape[0]
    attn = Whole(st, (pack_in, ypack_in), wattn, asem)
    tail = weights_of(st, (wg_r, wu_r), layer, wtail, wtsem, xtail_in)
    down = Down(st, wd_r.at[layer], wdown, dstage, dsem)
    attn.open_local()

    def caches(b):
        return [pltpu.make_async_copy(src.at[layer, b], buf.at[b], kvsem.at[n, b])
                for n, (src, buf) in enumerate(((ck, kbuf), (cv, vbuf)))]

    def fetch_caches(b, carry):
        each(caches(b), "start")
        return carry

    down.load.start()
    st.greet(st.peer, st.partner, st.xpeer, st.diagonal)
    down.open()
    attn.open_share()
    lax.fori_loop(0, seqs, fetch_caches, 0)
    if not last:
        ahead = weights_of(st, (wq_r, wk_r, wv_r), layer + 1, wqkv, wsem)
        coming = NextLayer(st, (wo_r, wc_r, wco_r), (wg_r, wu_r), layer + 1, pack_ref, tail_ref, pbuf, tbuf,
                           nsem, xsem)
        each(ahead, "open_cross")
        each(coming.sends, "start")
    attn.finish(0)
    y = jnp.concatenate(both_blocks(o_ref[...].astype(BF16), wattn, 0), axis=1)
    res = x_ref[...] + y.astype(F32)
    attn.finish(1)
    for cb, q in enumerate(both_blocks(rms(res, gcross_ref[layer:layer + 1, :]), wattn, 1)):
        qs[cb] = q.astype(F32)
    each(tail, "open_local")
    each(tail, "open_share")
    if not last:
        each(ahead, "open_local")
        each(coming.loads, "start")
        each(ahead, "open_share")

    def cross_step(i, carry):
        hmask = head_mask()
        t_id = lax.broadcasted_iota(jnp.int32, (TOKENS * HROWS, kbuf.shape[-1]), 1)
        seqids = [i * SEQ_BLOCK + j for j in range(SEQ_BLOCK)]
        for b in seqids:
            each(caches(b), "wait")
        queries = [spread_query(qs, b, seqs, hmask) for b in seqids]
        scores = [dot32(q, kbuf[b]) for q, b in zip(queries, seqids)]
        parts = [jnp.where(t_id < len_ref[b], sc, NEG) for b, sc in zip(seqids, scores)]
        mix_values(softmax_rows(jnp.concatenate(parts, axis=0)), vbuf, seqids, hmask, os)
        return carry

    lax.fori_loop(0, seqs // SEQ_BLOCK, cross_step, 0)
    if not last:
        coming.store()
    down.relay()
    attn.finish(2)
    y = jnp.concatenate(both_blocks(os[...].reshape(rows, D).astype(BF16), wattn, 2), axis=1)
    res = res + y.astype(F32)
    gain = gmlp_ref[layer:layer + 1, :]
    ff = wtail.shape[1] // 2

    def gated(normed):
        gate = dot32(normed, wtail[:, 0:ff]).astype(BF16).astype(F32)
        up = dot32(normed, wtail[:, ff:2 * ff]).astype(BF16).astype(F32)
        return (gate * jax.nn.sigmoid(gate) * up).astype(BF16)

    normed = rms(res, gain)
    nbuf[0] = normed
    moving = st.send(nbuf.at[0], nbuf.at[1], sem.at[0])
    if last:
        rbuf[...] = res
        res_out = pltpu.make_async_copy(rbuf, own_ref.at[0], osem.at[0])
        res_out.start()
    else:
        rbuf[0] = res
        moving_res = st.send(rbuf.at[0], rbuf.at[1], sem2.at[0, 0])
    each(tail, "finish")
    own_act = gated(normed)
    moving.wait()
    other_act = gated(nbuf[1])
    down.finish()

    def partial_sum(act):
        return jnp.concatenate([dot32(act, wdown[0]), dot32(act, wdown[1])], axis=1)

    zbuf[0, 1] = partial_sum(other_act)
    moving_z = [st.send(zbuf.at[0, 1], zin_ref if last else zbuf.at[1, 0], sem2.at[1, 0])]
    zbuf[0, 0] = partial_sum(own_act)
    if not last:
        moving_z.append(st.send(zbuf.at[0, 0], zbuf.at[1, 1], sem2.at[1, 1]))
        each(ahead, "relay")
        moving_res.wait()
    if last:
        part_out = pltpu.make_async_copy(zbuf.at[0, 0], own_ref.at[1], osem.at[1])
        part_out.start()
        res_out.wait()
        part_out.wait()
    each(moving_z, "wait")
    if not last:
        z = (zbuf[0] + zbuf[1]).astype(BF16).astype(F32)
        res = jnp.concatenate([res + z[0], rbuf[1] + z[1]], axis=0)
        x_out[...] = res[:rows]
        normed = rms(res, gself_ref[layer + 1:layer + 2, :])
        each(ahead, "finish")
        st.give_rows(dot32(normed, wqkv[...]), qkvbuf, sem.at[1], qkv_ref)
        coming.finish()


def exchange_call(kernel, cid, name, specs, args, outs, scratch, flops):
    spaces = {"s": pltpu.SMEM, "v": pltpu.VMEM, "h": pl.ANY}
    spec = lambda letters: [pl.BlockSpec(memory_space=spaces[x]) for x in letters]
    return pl.pallas_call(
        kernel,
        out_shape=tuple(t for _, t in outs),
        in_specs=spec(specs),
        out_specs=tuple(spec(x for x, _ in outs)),
        scratch_shapes=scratch,
        cost_estimate=pl.CostEstimate(flops=flops, bytes_accessed=8 << 20, transcendentals=0),
        compiler_params=pltpu.CompilerParams(collective_id=cid, has_side_effects=True, vmem_limit_bytes=VMEM_LIMIT),
        name=name,
    )(*args)


def solution(mesh):
    batch_axes = ('dp', 'col', 'row')

    def local_step(h_first, h_second, start_pos, enc_lens, dec_bias, norm_self, norm_cross, norm_mlp,
                   w_query, w_key, w_value, w_out, w_cquery, w_cout, w_gate, w_up, w_down,
                   self_k, self_v, cross_k, cross_v):
        layers, seqs, cache_len = self_k.shape[:3]
        rows = TOKENS * seqs
        half = D // 2
        ffc = w_gate.shape[2]
        depth = 4 * w_query.shape[1]
        fdepth = 4 * w_down.shape[1]

        def flat(cache):
            return jnp.transpose(cache, (0, 1, 3, 4, 2)).reshape(layers, seqs, D, cache.shape[2])

        caches = [flat(a) for a in (self_k, self_v, cross_k, cross_v)]
        block = w_query.shape[1]

        vm = lambda shape, dt=BF16: pltpu.VMEM(shape, dt)
        dma = lambda *shape: pltpu.SemaphoreType.DMA(shape)
        rowbuf = lambda width, dt=BF16: vm((2, rows, width), dt)
        res_t = ("v", jax.ShapeDtypeStruct((rows, D), F32))
        qkv_t = ("v", jax.ShapeDtypeStruct((2, rows, 3 * half), F32))
        pack_t = ("h", jax.ShapeDtypeStruct((2, block, 3 * half), BF16))
        tail_t = ("h", jax.ShapeDtypeStruct((block, 2 * ffc), BF16))
        coming = [vm((block, 3 * half)), vm((block, 2 * ffc))]
        across = [(r, (r + 2) % 4) for r in range(4)]
        flip = [(0, 1), (1, 0)]

        table_t = ("v", jax.ShapeDtypeStruct((HROWS, cache_len), F32))
        res, qkv, pack, tail_own, table = exchange_call(
            start_kernel, 0, "start", "vvvv" + "h" * 8,
            [h_first, h_second, norm_self, dec_bias.T, w_query, w_key, w_value, w_out, w_cquery, w_cout, w_gate, w_up],
            [res_t, qkv_t, pack_t, tail_t, table_t],
            [rowbuf(D), vm((depth, 3 * half)), rowbuf(3 * half)] + coming
            + [dma(3, 7), dma(3, 3), dma(3, 2), dma(2, 2)], 3_000_000_000)
        outs = None
        for l in range(layers):
            last = l == layers - 1
            ypack = lax.ppermute(pack, "col", flip)
            xtail = lax.ppermute(tail_own, "row", across)
            k_out, v_out, mixed = self_attention(l, start_pos, qkv, table, caches[0], caches[1], outs)
            outs = (k_out, v_out)
            cache_buf = vm((seqs, D, cross_k.shape[2]))
            scratch = [cache_buf, cache_buf, vm((2, depth, 3 * half)), vm((depth, 2 * ffc)), vm((2, fdepth // 2, half)), vm((fdepth // 4, half)),
                       vm((2, rows, half), F32), vm((TOKENS, seqs, D), F32), rowbuf(D), vm((2, 2, rows, D), F32),
                       dma(2, seqs), dma(3, 2, 2, 3), dma(2, 7), dma(5, 2), dma(2, 2), dma(2, 2, 2)]
            args = [enc_lens, mixed.reshape(rows, D), res, norm_cross, norm_mlp]
            weights = [caches[2], caches[3], pack, ypack, xtail, w_gate, w_up, w_down]
            if last:
                own, zin = exchange_call(
                    functools.partial(layer_kernel, l, True, seqs), 1 + l, "last", "svvvv" + "h" * 8,
                    args + weights,
                    [("h", jax.ShapeDtypeStruct((2, rows, D), F32)), ("h", jax.ShapeDtypeStruct((rows, D), F32))],
                    scratch + [vm((rows, D), F32), dma(2)], 20_000_000_000)
            else:
                scratch += [rowbuf(D, F32), vm((depth, 3 * half)), rowbuf(3 * half)] + coming
                scratch += [dma(3, 7), dma(3, 3), dma(3, 2)]
                res, qkv, pack, tail_own = exchange_call(
                    functools.partial(layer_kernel, l, False, seqs), 1 + l, "layer", "svvvvv" + "h" * 14,
                    args + [norm_self] + weights
                    + [w_query, w_key, w_value, w_out, w_cquery, w_cout],
                    [res_t, qkv_t, pack_t, tail_t], scratch, 20_000_000_000)

        def unflat(cache):
            return jnp.transpose(cache.reshape(layers, seqs, HEADS, HEAD_DIM, cache_len), (0, 1, 4, 2, 3))

        hid = own[0] + lax.reduce_precision(own[1] + zin, 8, 7)
        return hid.reshape(TOKENS, seqs, D).astype(BF16), unflat(outs[0]), unflat(outs[1])

    row_spec = P(batch_axes, None)
    seq_spec = P(batch_axes)
    weight_spec = P(None, 'row', 'col')
    cache_spec = P(None, batch_axes)
    in_specs = (row_spec, row_spec, seq_spec, seq_spec, P(), P(), P(), P()) + (weight_spec,) * 9 + (cache_spec,) * 4
    out_specs = (P(None, batch_axes), cache_spec, cache_spec)
    return jax.shard_map(local_step, mesh=mesh, in_specs=in_specs, out_specs=out_specs, check_vma=False)
```
